32 devices in a mesh: dp: 8 (over z, x), patch: 4 (over y, core).
Axes of the slice: x: 2, y: 2, z: 4, core: 2. Of those that a mesh axis runs over, the one named last changes fastest.
Arguments:
- query_rows: bfloat16 [8, 512, 576], P('dp', 'patch'), may hold values from -6 to 6
- key_rows: bfloat16 [8, 512, 576], P('dp', 'patch'), may hold values from -6 to 6
- value_rows: bfloat16 [8, 512, 576], P('dp', 'patch'), may hold values from -6 to 6
- out_weight: bfloat16 [576, 1152], replicated, may hold values from -0.25 to 0.25
- target: bfloat16 [8, 512, 1152], P('dp', 'patch'), may hold values from -6 to 6
- lengths: int32 [8], P('dp'), may hold values from 64 to 512
- segments: int32 [8, 512], P('dp', 'patch'), may hold values from 0 to 7, never falling along the last dimension, each value on 1 to 256 neighbouring positions
Outputs:
- query_grad: float32 [8, 512, 576], P('dp', 'patch')
- key_grad: float32 [8, 512, 576], P('dp', 'patch')
- value_grad: float32 [8, 512, 576], P('dp', 'patch')
- weight_grad: float32 [576, 1152], P('patch', 'dp')
- loss: float32 [], replicated
The draws below stay inside these ranges and needn't reach their ends.
All inputs are finite; a program needn't handle non-finite values.
Results may differ from the reference program's by a relative error of at most 0.024.
Values may be sent and summed in bfloat16 or wider, within the bound.
A program may use at most 64 MiB of HBM per device.

```python
import math
import jax
import jax.numpy as jnp
import numpy as np
from jax import lax

WIDTH = 1152
HEADS = 8
HEAD_DIM = 72
TOK_DEV = 128
FEAT = 576
SEQ = 512
SAMPLES = 8


def draw_rows(key, salt, chosen_rows):
    fresh_key = jax.random.fold_in(key, salt)
    sampled = jnp.clip(1.5 * jax.random.normal(fresh_key, (SAMPLES, SEQ, FEAT), jnp.float32), -6.0, 6.0)
    return sampled.astype(jnp.bfloat16)


def draw_query_rows(key, part):
    positions = jnp.arange(SEQ)
    return draw_rows(key, 1, positions % TOK_DEV == 0)


def draw_key_rows(key, part):
    positions = jnp.arange(SEQ)
    return draw_rows(key, 2, positions % TOK_DEV == 0)


def plant(entries, key, low, largest):
    longest = entries.shape.index(max(entries.shape))
    spots = []
    for shift in (0, 1):
        where = [jax.random.randint(jax.random.fold_in(key, axis), (), 0, length) for axis, length in enumerate(entries.shape)]
        where[longest] = (where[longest] + shift) % entries.shape[longest]
        spots.append(tuple(where))
    return entries.at[spots[0]].set(low).at[spots[1]].set(largest)


def steps_of(stream_key, extent, split, least, largest):
    level = 1.0
    for position, shards_of in split:
        heights = jax.random.uniform(jax.random.fold_in(jax.random.fold_in(stream_key, 6), position), (shards_of,), jnp.float32, least / len(split), largest / len(split))
        level = level * jnp.repeat(jnp.exp(heights), extent[position] // shards_of).reshape((-1,) + (1,) * (len(extent) - 1 - position))
    return level


def profile(count, total, most, skew):
    weights = [(1 << 20) // math.isqrt(rank ** skew) + 1 for rank in range(2, count + 1)]
    surplus, counts = total - most - (count - 1), [1] * (count - 1)
    while surplus > 0:
        candidates = [i for i in range(count - 1) if counts[i] < most]
        pool, remaining = sum([weights[i] for i in candidates]), surplus
        for i in candidates:
            more = min(most - counts[i], max(1, remaining * weights[i] // pool), surplus)
            counts[i] = counts[i] + more
            surplus = surplus - more
    return np.array([most] + counts)


def uneven_parts(key, number_of, total, most, skew):
    if number_of == 2:
        one = jax.random.randint(key, (), max(1, total - most), min(most, total - 1) + 1)
        return jnp.stack([one, total - one])
    tallies = jnp.asarray(profile(number_of, total, most, skew), jnp.int32)
    pairs = (number_of - 1) // 2
    donor, sink = tallies[1:1 + 2 * pairs:2], tallies[2:2 + 2 * pairs:2]
    slack = jnp.minimum(donor - 1, most - sink)
    shifted = jax.random.randint(jax.random.fold_in(key, 1), (pairs,), 0, 1 << 20) % (slack + 1)
    tallies = tallies.at[1:1 + 2 * pairs:2].set(donor - shifted).at[2:2 + 2 * pairs:2].set(sink + shifted)
    return tallies[jax.random.permutation(jax.random.fold_in(key, 2), number_of)]


def normal_values(rng, shape, spread, most, split=(), kind=jnp.bfloat16):
    array = spread * jax.random.normal(rng, shape, jnp.float32)
    if split:
        array = array * steps_of(rng, shape, split, -0.22, 0.18)
    return jnp.clip(array, -most, most).astype(kind)


def setup_inputs(seed: int = 0) -> dict:
    arg_keys = jax.random.split(jax.random.key(seed), 8)
    query_rows = draw_query_rows(jax.random.fold_in(arg_keys[7], 71), 0)
    key_rows = draw_key_rows(jax.random.fold_in(arg_keys[7], 71), 0)
    value_rows = normal_values(arg_keys[2], (SAMPLES, SEQ, FEAT), 1.0, 6.0, ((0, 8), (1, 4)))
    out_weight = normal_values(arg_keys[3], (FEAT, WIDTH), FEAT ** -0.5, 0.25)
    target = normal_values(arg_keys[4], (SAMPLES, SEQ, WIDTH), 1.0, 6.0, ((0, 8), (1, 4)))
    lengths = plant(jax.random.randint(arg_keys[5], (SAMPLES,), SEQ // 8, SEQ + 1), jax.random.fold_in(arg_keys[5], 1), SEQ // 8, SEQ).astype(jnp.int32)
    segments = jax.vmap(lambda own: jnp.searchsorted(jnp.cumsum(uneven_parts(own, 8, SEQ, SEQ // 2, 2)), jnp.arange(SEQ), side="right"))(jax.random.split(arg_keys[6], SAMPLES)).reshape((SAMPLES, SEQ)).astype(jnp.int32)
    return {"query_rows": query_rows, "key_rows": key_rows, "value_rows": value_rows, "out_weight": out_weight, "target": target, "lengths": lengths, "segments": segments}


NEG_LARGE = -1e+30

def widen(value):
    return lax.optimization_barrier(value).astype(jnp.float32)

def one_sample(packed, out_weight):
    query_rows, key_rows, value_rows, target_rows, length, segment_row = packed
    score_scale = 1.0 / math.sqrt(HEAD_DIM)
    query_heads = query_rows.astype(jnp.float32).reshape(SEQ, HEADS, HEAD_DIM)
    key_heads = key_rows.astype(jnp.float32).reshape(SEQ, HEADS, HEAD_DIM)
    value_heads = value_rows.astype(jnp.float32).reshape(SEQ, HEADS, HEAD_DIM)
    live = lax.iota(jnp.int32, SEQ) < length
    group = jnp.where(live, segment_row, -1)
    allowed = (group[:, None] == group[None, :])[None, :, :]
    scores = jnp.einsum('qhe,khe->hqk', query_heads, key_heads) * score_scale
    masked = jnp.where(allowed, scores, NEG_LARGE)
    row_max = lax.optimization_barrier(jnp.max(masked, axis=2))
    probs = jnp.where(allowed, jnp.exp(masked - row_max[:, :, None]), 0.0)
    denom = lax.optimization_barrier(jnp.sum(probs, axis=2))
    weights = widen(probs.astype(jnp.bfloat16))
    accum = jnp.einsum('hqk,khe->qhe', weights, value_heads)
    attn = (accum / denom.T[:, :, None]).reshape(SEQ, FEAT).astype(jnp.bfloat16)
    log_norm = row_max + jnp.log(denom)
    output = jnp.dot(attn, out_weight, preferred_element_type=jnp.float32)
    error = jnp.where(live[:, None], output - target_rows.astype(jnp.float32), 0.0)
    grad_out = (2.0 * error).astype(jnp.bfloat16)
    attn_wide = widen(attn)
    grad_wide = widen(grad_out)
    weight_part = jnp.einsum('tf,td->fd', attn_wide, grad_wide)
    grad_attn = jnp.einsum('td,fd->tf', grad_wide, out_weight.astype(jnp.float32)).astype(jnp.bfloat16)
    grad_attn_wide = widen(grad_attn)
    delta = lax.optimization_barrier(jnp.sum((grad_attn_wide * attn_wide).reshape(SEQ, HEADS, HEAD_DIM), axis=2)).T
    back_probs = jnp.where(allowed, jnp.exp(masked - log_norm[:, :, None]), 0.0)
    grad_heads = grad_attn_wide.reshape(SEQ, HEADS, HEAD_DIM)
    dprobs = jnp.einsum('qhe,khe->hqk', grad_heads, value_heads)
    dscores = widen((back_probs * (dprobs - delta[:, :, None])).astype(jnp.bfloat16))
    query_raw = jnp.einsum('hqk,khe->qhe', dscores, key_heads) * score_scale
    key_raw = jnp.einsum('hqk,qhe->khe', dscores, query_heads) * score_scale
    back_weights = widen(back_probs.astype(jnp.bfloat16))
    value_raw = jnp.einsum('hqk,qhe->khe', back_weights, grad_heads)
    return (query_raw.reshape(SEQ, FEAT), key_raw.reshape(SEQ, FEAT), value_raw.reshape(SEQ, FEAT), weight_part, jnp.sum(error * error))

def reference(query_rows, key_rows, value_rows, out_weight, target, lengths, segments):

    def per_sample(packed):
        return one_sample(packed, out_weight)
    results = lax.map(per_sample, (query_rows, key_rows, value_rows, target, lengths, segments))
    count = jnp.sum(lengths).astype(jnp.float32)
    ratio = jnp.float32(SAMPLES * SEQ) / count
    query_grad = ratio * results[0]
    key_grad = ratio * results[1]
    value_grad = ratio * results[2]
    weight_grad = lax.optimization_barrier(jnp.sum(results[3], axis=0)) * (ratio / SEQ)
    loss = jnp.sum(results[4]) / (count * WIDTH)
    return (query_grad, key_grad, value_grad, weight_grad, loss)
```

```python
import functools
import math

import jax
import jax.numpy as jnp
from jax import lax
from jax.experimental import pallas as pl
from jax.experimental.pallas import tpu as pltpu
from jax.sharding import PartitionSpec as P

MESH = pl.DeviceIdType.MESH
WIDTH = 1152
HEADS = 8
HEAD_DIM = 72
FEAT = 576
PAIRS = HEADS // 2
PAIR_ROWS = 2 * HEAD_DIM
STAT_ROWS = 16
AUG_ROWS = PAIR_ROWS + STAT_ROWS
LANES = 128
NEG_LARGE = -1e30
F32 = jnp.float32
BF16 = jnp.bfloat16
KEY, VALUE, QUERY = range(3)


def nt(left, right):
    return lax.dot_general(left, right, (((1,), (1,)), ((), ())), preferred_element_type=F32)


def nn(left, right):
    return lax.dot_general(left, right, (((1,), (0,)), ((), ())), preferred_element_type=F32)


def tn(left, right):
    return lax.dot_general(left, right, (((0,), (0,)), ((), ())), preferred_element_type=F32)


def pad16(size):
    return -(-size // 16) * 16


def unit_layout(members, groups):
    share, features = WIDTH // groups, FEAT // members
    main = features // LANES * LANES
    rest = features - main
    main_rows = pad16(share) if main else 0
    tiles = -(-share // LANES)
    return share, features, main, rest, main_rows, tiles, main_rows + tiles * pad16(rest)


def kernel(
    members,
    groups,
    len_ref,
    seg_hbm,
    q_hbm,
    k_hbm,
    v_hbm,
    w_hbm,
    t_hbm,
    dq_ref,
    dk_ref,
    dv_ref,
    dw_ref,
    sum_ref,
    w_ref,
    t_ref,
    seg_row_ref,
    wt_ref,
    acc_ref,
    dout_ref,
    kvq_ref,
    g_ref,
    seg_own,
    seg_all,
    stat_ref,
    bias_ref,
    prob_ref,
    at_ref,
    dt_own,
    dt_all,
    u_own,
    y_all,
    z_own,
    z_all,
    tile_own,
    tile_all,
    sum_own,
    sum_all,
    load_sem,
    far_sem,
    near_sem,
    kvq_send,
    g_far,
    g_near,
    g_send,
    at_send,
    at_recv,
    dt_send,
    dt_recv,
    y_send,
    y_recv,
    z_send,
    z_recv,
    small_send,
    small_recv,
):
    rows = q_hbm.shape[1]
    chips = members // 2
    outer = groups // 2
    mine = outer // 2
    half = mine // 2
    share, features, main, rest, main_rows, tiles, unit_rows = unit_layout(members, groups)
    rest_rows = pad16(rest)
    me = lax.axis_index("patch")
    dp = lax.axis_index("dp")
    chip, core = me // 2, me % 2
    step_a, step_b = dp // 2, dp % 2
    partner = chip * 2 + 1 - core
    across = step_a * 2 + 1 - step_b
    slot = step_b * 2 + core

    def patch_peer(shift):
        return lax.rem(me + shift, members)

    def dp_peer(shift):
        return lax.rem(dp + shift, groups)

    def far(shift):
        return lax.rem(chip + shift, chips)

    def outer_peer(shift):
        return lax.rem(step_a + shift, outer)

    loads = [
        pltpu.make_async_copy(k_hbm, kvq_ref.at[KEY, me], load_sem.at[0]),
        pltpu.make_async_copy(v_hbm, kvq_ref.at[VALUE, me], load_sem.at[1]),
        pltpu.make_async_copy(seg_hbm, seg_row_ref, load_sem.at[2]),
        pltpu.make_async_copy(q_hbm, kvq_ref.at[QUERY, me], load_sem.at[3]),
        pltpu.make_async_copy(w_hbm, w_ref, load_sem.at[4]),
        pltpu.make_async_copy(t_hbm, t_ref, load_sem.at[5]),
    ]
    for load in loads:
        load.start()

    barrier = pltpu.get_barrier_semaphore()

    def greet(dp_index, patch_index):
        pl.semaphore_signal(barrier, inc=1, device_id=(dp_index, patch_index), device_id_type=MESH)

    for shift in range(1, members):
        greet(dp, patch_peer(shift))
    for shift in range(1, groups):
        greet(dp_peer(shift), me)
    greet(across, partner)
    for shift in range(1, outer):
        greet(outer_peer(shift) * 2 + step_b, partner)
    greeted = members - 1 + groups - 1 + 1 + outer - 1

    def copy(src, dst, send, recv, device):
        return pltpu.make_async_remote_copy(
            src_ref=src, dst_ref=dst, send_sem=send, recv_sem=recv, device_id=device, device_id_type=MESH
        )

    def received(ref, recv):
        copy(ref, ref, small_send.at[0], recv, (dp, partner)).wait_recv()

    def sent(ref, send):
        copy(ref, ref, send, small_recv.at[0], (dp, partner)).wait_send()

    def rows_of(pair):
        return pl.ds(PAIR_ROWS * pair, PAIR_ROWS)

    def kvq_part(array, owner, pair):
        if array == QUERY:
            return kvq_ref.at[array, owner]
        return kvq_ref.at[array, owner, rows_of(pair)]

    def kvq_index(array, pair):
        return 2 * PAIRS if array == QUERY else PAIRS * array + pair

    def spread(part, index, send, away, near):
        for shift in range(1, chips):
            copy(part, part, send, away.at[index], (dp, far(shift) * 2 + core)).start()
        copy(part, part, send, near.at[index], (dp, partner)).start()

    def relay_parts(part_at, span_at, index, send, away, near):
        received(part_at(far(1) * 2 + core) if chips == 2 else span_at(chips - 1), away.at[index])
        for shift in range(1, chips):
            part = part_at(far(shift) * 2 + core)
            copy(part, part, send, near.at[index], (dp, partner)).start()

    def kvq_span(array, pair, count):
        if array == QUERY:
            return kvq_ref.at[array, pl.ds(0, count)]
        return kvq_ref.at[array, pl.ds(0, count), rows_of(pair)]

    def kvq_spread(array, pair=0):
        spread(kvq_part(array, me, pair), kvq_index(array, pair), kvq_send.at[0], far_sem, near_sem)

    def kvq_relay(array, pair=0):
        relay_parts(
            lambda owner: kvq_part(array, owner, pair),
            lambda count: kvq_span(array, pair, count),
            kvq_index(array, pair),
            kvq_send.at[0],
            far_sem,
            near_sem,
        )

    def kvq_finish(array, pair=0):
        received(kvq_span(array, pair, chips), near_sem.at[kvq_index(array, pair)])

    def g_spread(pair):
        spread(g_ref.at[me, pair], pair, g_send.at[0], g_far, g_near)

    def g_relay(pair):
        relay_parts(
            lambda owner: g_ref.at[owner, pair],
            lambda count: g_ref.at[pl.ds(0, count), pair],
            pair,
            g_send.at[0],
            g_far,
            g_near,
        )

    def g_finish(pair):
        received(g_ref.at[pl.ds(0, chips), pair], g_near.at[pair])

    def small(index, own_ref, everyone):
        for shift in range(1, members):
            copy(own_ref, everyone.at[me], small_send.at[index], small_recv.at[index], (dp, patch_peer(shift))).start()

    loads[2].wait()
    seg_own[...] = jnp.broadcast_to(seg_row_ref[...], seg_own.shape)
    for load in (loads[0], loads[1], loads[3]):
        load.wait()
    pl.semaphore_wait(barrier, greeted)
    small(0, seg_own, seg_all)
    for pair in range(PAIRS):
        kvq_spread(KEY, pair)
        kvq_spread(VALUE, pair)
    kvq_spread(QUERY)
    seg_all[me] = seg_own[...]

    upper = lax.broadcasted_iota(jnp.int32, (PAIR_ROWS, 1), 0) < HEAD_DIM
    masks = [upper.astype(F32).astype(BF16), jnp.logical_not(upper).astype(F32).astype(BF16)]

    def stacked(value):
        return jnp.concatenate([value * masks[0], value * masks[1]], axis=1)

    def merged(value):
        return jnp.concatenate([value[:HEAD_DIM, :rows], value[HEAD_DIM:, rows:]], axis=0)

    def own(array, pair):
        return kvq_ref[array, me, PAIR_ROWS * pair : PAIR_ROWS * (pair + 1), :]

    def whole(array, pair):
        low = PAIR_ROWS * pair
        return jnp.concatenate([kvq_ref[array, j, low : low + PAIR_ROWS, :] for j in range(members)], axis=1)

    stat_row = lax.broadcasted_iota(jnp.int32, (STAT_ROWS, 2 * rows), 0)
    stat_side = (lax.broadcasted_iota(jnp.int32, (STAT_ROWS, 2 * rows), 1) >= rows).astype(jnp.int32)

    def picker(base):
        low = base + 3 * stat_side
        return jnp.where((stat_row >= low) & (stat_row < low + 3), -1.0, 0.0).astype(BF16)

    norm_picker, delta_picker = picker(0), picker(6)

    loads[5].wait()
    acc_ref[...] = -(t_ref[...].astype(F32).T)
    loads[4].wait()
    for pair in range(PAIRS):
        wt_ref[pair] = w_ref[PAIR_ROWS * pair : PAIR_ROWS * (pair + 1), :].astype(F32).T.astype(BF16)
    u_own[:, :, main_rows:, :] = jnp.zeros((mine, members, unit_rows - main_rows, LANES), BF16)

    length = len_ref[0]
    lane_position = lax.broadcasted_iota(jnp.int32, (1, rows), 1)
    own_live = me * rows + lane_position < length
    own_group = jnp.where(own_live, seg_own[0:1], -1).astype(F32)
    received(seg_all.at[pl.ds(0, members - 1)], small_recv.at[0])
    for j in range(members):
        group = jnp.where(j * rows + lane_position < length, seg_all[j][0:1], -1).astype(F32)
        group = jnp.broadcast_to(group, (rows, rows)).T
        bias_ref[j * rows : (j + 1) * rows, :] = jnp.where(group == own_group, 0.0, NEG_LARGE)

    log_scale = math.log2(math.e) / math.sqrt(HEAD_DIM)
    score_scale = 1.0 / math.sqrt(HEAD_DIM)

    def biased(scores):
        bias = bias_ref[...]
        return scores * log_scale + jnp.concatenate([bias, bias], axis=1)

    denoms = []
    kvq_relay(KEY, 0)
    for pair in range(PAIRS):
        kvq_finish(KEY, pair)
        kvq_relay(VALUE, pair)
        scores = biased(tn(whole(KEY, pair), stacked(own(QUERY, pair))))
        row_max = jnp.max(scores, axis=0, keepdims=True)
        probs = jnp.exp2(scores - row_max)
        denom = jnp.sum(probs, axis=0, keepdims=True)
        prob_ref[pair] = probs
        log_norm = (row_max + jnp.log2(denom)) * (1.0 / log_scale)
        for side in (0, 1):
            head = 2 * pair + side
            stat_ref[head : head + 1, :] = log_norm[:, side * rows : (side + 1) * rows]
        denoms.append(denom)
        if pair + 1 < PAIRS:
            kvq_relay(KEY, pair + 1)
        kvq_finish(VALUE, pair)
        accum = nn(whole(VALUE, pair), probs.astype(BF16))
        attn_pair = merged(accum / denom).astype(BF16)
        at_ref[slot, PAIR_ROWS * pair : PAIR_ROWS * (pair + 1), :] = attn_pair
        part = at_ref.at[slot, rows_of(pair)]
        copy(part, part, at_send.at[0], at_recv.at[0], (across, me)).start()
        copy(part, part, at_send.at[0], at_recv.at[1], (dp, partner)).start()
        acc_ref[...] += nn(wt_ref[pair], attn_pair)

    error = jnp.where(own_live, acc_ref[...], 0.0)
    dout = (2.0 * error).astype(BF16)
    dout_ref[...] = dout
    for z in range(outer):
        for side in (0, 1):
            low = (z * 2 + side) * share
            dt_own[side, z] = dout[low : low + share]
    for chunk in (0, 1):
        for side, to in ((1 - step_b, core), (1 - step_b, 1 - core), (step_b, 1 - core)):
            copy(
                dt_own.at[side, pl.ds(to * mine + chunk * half, half)],
                dt_all.at[pl.ds(chunk * half, half), slot],
                dt_send.at[0],
                dt_recv.at[chunk],
                (step_a * 2 + side, chip * 2 + to),
            ).start()
    for i in range(mine):
        dt_all[i, slot] = dt_own[step_b, core * mine + i]

    def terms(value):
        first = value.astype(BF16).astype(F32)
        second = (value - first).astype(BF16).astype(F32)
        return [first, second, value - first - second]

    for pair in range(PAIRS):
        grad = nn(w_ref[PAIR_ROWS * pair : PAIR_ROWS * (pair + 1), :], dout_ref[...]).astype(BF16)
        g_ref[me, pair, :PAIR_ROWS, :] = grad
        product = grad.astype(F32) * at_ref[slot, PAIR_ROWS * pair : PAIR_ROWS * (pair + 1), :].astype(F32)
        lines = []
        for side in (0, 1):
            lines += terms(stat_ref[2 * pair + side : 2 * pair + side + 1, :])
        for side in (0, 1):
            head = 2 * pair + side
            delta = jnp.sum(product[HEAD_DIM * side : HEAD_DIM * (side + 1)], axis=0, keepdims=True)
            stat_ref[HEADS + head : HEADS + head + 1, :] = delta
            lines += terms(delta)
        lines.append(jnp.zeros((STAT_ROWS - 12, rows), F32))
        g_ref[me, pair, PAIR_ROWS:, :] = jnp.concatenate(lines, axis=0).astype(BF16)
        g_spread(pair)

    loss_part = jnp.sum(jnp.sum(error * error, axis=0, keepdims=True), axis=1, keepdims=True)
    tile_own[...] = jnp.broadcast_to(loss_part, tile_own.shape)
    small(1, tile_own, tile_all)
    tile_all[me] = tile_own[...]

    def query_pass(pair):
        low = HEADS + 2 * pair
        delta = jnp.concatenate([stat_ref[low : low + 1, :], stat_ref[low + 1 : low + 2, :]], axis=1)
        grad = g_ref[me, pair, :PAIR_ROWS, :]
        dprobs = tn(whole(VALUE, pair), stacked(grad))
        dscores = prob_ref[pair] * (1.0 / denoms[pair]) * (dprobs - delta)
        value = nn(whole(KEY, pair), dscores.astype(BF16))
        dq_ref[PAIR_ROWS * pair : PAIR_ROWS * (pair + 1), :] = merged(value) * score_scale

    def key_pass(pair):
        g_finish(pair)
        queries = whole(QUERY, pair)
        grads = jnp.concatenate([g_ref[j, pair] for j in range(members)], axis=1)
        stats = grads[PAIR_ROWS:]
        scores = tn(
            jnp.concatenate([queries, stats], axis=0),
            jnp.concatenate([stacked(own(KEY, pair)), norm_picker], axis=0),
        )
        probs = jnp.exp2(biased(scores))
        dv_ref[PAIR_ROWS * pair : PAIR_ROWS * (pair + 1), :] = merged(nn(grads[:PAIR_ROWS], probs.astype(BF16)))
        dprobs = tn(grads, jnp.concatenate([stacked(own(VALUE, pair)), delta_picker], axis=0))
        dscores = (probs * dprobs).astype(BF16)
        dk_ref[PAIR_ROWS * pair : PAIR_ROWS * (pair + 1), :] = merged(nn(queries, dscores)) * score_scale

    def weight_part(chunk):
        received(dt_all.at[pl.ds(chunk * half, half), pl.ds(0, 3)], dt_recv.at[chunk])
        attn = jnp.concatenate([at_ref[s] for s in range(4)], axis=1)
        if main:
            attn_main = jnp.concatenate([attn[p * features : p * features + main] for p in range(members)], axis=0)
            attn_rest = jnp.concatenate([attn[p * features + main : (p + 1) * features] for p in range(members)], axis=0)
        else:
            attn_rest = attn
        for i in range(chunk * half, (chunk + 1) * half):
            grads = jnp.concatenate([dt_all[i, s] for s in range(4)], axis=1)
            if main:
                part_main = nt(grads, attn_main).astype(BF16)
            part_rest = nt(attn_rest, grads)
            for p in range(members):
                if main:
                    u_own[i, p, :share, :] = part_main[:, p * main : (p + 1) * main]
                for t in range(tiles):
                    wide = min(share - t * LANES, LANES)
                    piece = part_rest[p * rest : (p + 1) * rest, t * LANES : t * LANES + wide].astype(BF16)
                    low = main_rows + t * rest_rows
                    u_own[i, p, low : low + rest, :wide] = piece
            for to in (0, 1):
                for shift in range(1, chips):
                    copy(
                        u_own.at[i, far(shift) * 2 + to],
                        y_all.at[i, to, chip],
                        y_send.at[0],
                        y_recv.at[i, to],
                        (dp, far(shift) * 2 + core),
                    ).start()

    def weight_sum(i, to):
        received(y_all.at[i, to, pl.ds(0, chips - 1)], y_recv.at[i, to])
        value = u_own[i, chip * 2 + to].astype(F32)
        for shift in range(1, chips):
            value = value + y_all[i, to, far(shift)].astype(F32)
        z_own[i, to] = value.astype(BF16)
        target = core * mine + i
        stays = jnp.logical_and(target == step_a, core == to)

        @pl.when(stays)
        def _():
            z_all[step_a] = z_own[i, to]

        @pl.when(jnp.logical_not(stays))
        def _():
            copy(
                z_own.at[i, to],
                z_all.at[step_a],
                z_send.at[0],
                z_recv.at[0],
                (target * 2 + step_b, chip * 2 + to),
            ).start()

    kvq_relay(QUERY)
    received(at_ref.at[0], at_recv.at[0])
    part = at_ref.at[(1 - step_b) * 2 + core]
    copy(part, part, at_send.at[0], at_recv.at[1], (dp, partner)).start()
    query_pass(0)
    g_relay(0)
    query_pass(1)
    g_relay(1)
    received(at_ref.at[pl.ds(0, 2)], at_recv.at[1])
    weight_part(0)
    g_relay(2)
    query_pass(2)
    weight_part(1)
    g_relay(3)

    received(tile_all.at[pl.ds(0, members - 1)], small_recv.at[1])
    pack_loss = tile_all[0]
    for j in range(1, members):
        pack_loss = pack_loss + tile_all[j]
    tile_lane = lax.broadcasted_iota(jnp.int32, pack_loss.shape, 1)
    sum_own[...] = jnp.where(tile_lane == 0, pack_loss, length.astype(F32))
    for shift in range(1, groups):
        copy(sum_own, sum_all.at[dp], small_send.at[2], small_recv.at[2], (dp_peer(shift), me)).start()
    sum_all[dp] = sum_own[...]

    query_pass(3)
    kvq_finish(QUERY)
    key_pass(0)
    units = [(i, to) for i in range(mine) for to in (0, 1)]
    quarter = len(units) // 4
    for i, to in units[: 2 * quarter]:
        weight_sum(i, to)
    key_pass(1)
    for i, to in units[2 * quarter : 3 * quarter]:
        weight_sum(i, to)
    key_pass(2)
    for i, to in units[3 * quarter :]:
        weight_sum(i, to)
    key_pass(3)

    received(sum_all.at[pl.ds(0, groups - 1)], small_recv.at[2])
    totals = sum_all[0]
    for j in range(1, groups):
        totals = totals + sum_all[j]
    sum_ref[...] = totals

    sent(kvq_ref.at[:, pl.ds(0, members - 1)], kvq_send.at[0])
    sent(g_ref.at[pl.ds(0, members - 1)], g_send.at[0])
    sent(at_ref.at[pl.ds(0, 3)], at_send.at[0])
    sent(dt_all.at[:, pl.ds(0, 3)], dt_send.at[0])
    sent(y_all.at[:, :, pl.ds(0, chips - 1)], y_send.at[0])
    sent(seg_all.at[pl.ds(0, members - 1)], small_send.at[0])
    sent(tile_all.at[pl.ds(0, members - 1)], small_send.at[1])
    sent(sum_all.at[pl.ds(0, groups - 1)], small_send.at[2])

    collects = core == step_a // mine

    @pl.when(collects)
    def _():
        sent(z_all.at[pl.ds(0, outer - 1)], z_send.at[0])
        received(z_all.at[pl.ds(0, outer - 1)], z_recv.at[0])

    @pl.when(jnp.logical_not(collects))
    def _():
        sent(z_all, z_send.at[0])
        received(z_all, z_recv.at[0])

    summed = z_all[0].astype(F32)
    for j in range(1, outer):
        summed = summed + z_all[j].astype(F32)
    if main:
        dw_ref[:main, :] = summed[:share].T
    for t in range(tiles):
        wide = min(share - t * LANES, LANES)
        low = main_rows + t * rest_rows
        dw_ref[main:, t * LANES : t * LANES + wide] = summed[low : low + rest, :wide]


def scale_kernel(slots, total, sum_ref, dq_ref, dk_ref, dv_ref, dw_ref, query_ref, key_ref, value_ref, weight_ref, loss_ref):
    count = sum_ref[0:1, 1:2]
    ratio = slots / count
    query_ref[...] = dq_ref[...] * ratio
    key_ref[...] = dk_ref[...] * ratio
    value_ref[...] = dv_ref[...] * ratio
    weight_ref[...] = dw_ref[...] * (ratio / total)
    loss_ref[...] = sum_ref[0:1, 0:1] / (count * WIDTH)


def solution(mesh):
    members, groups = mesh.shape["patch"], mesh.shape["dp"]

    def local(query_rows, key_rows, value_rows, out_weight, target, lengths, segments):
        rows = query_rows.shape[1]
        total = rows * members
        chips = members // 2
        outer = groups // 2
        mine = outer // 2
        share, features, main, rest, main_rows, tiles, unit_rows = unit_layout(members, groups)
        vmem = pl.BlockSpec(memory_space=pltpu.VMEM)
        hbm = pl.BlockSpec(memory_space=pltpu.HBM)
        dma = pltpu.SemaphoreType.DMA
        operands = (
            segments,
            query_rows[0].T,
            key_rows[0].T,
            value_rows[0].T,
            out_weight,
            target[0],
        )
        outs = pl.pallas_call(
            functools.partial(kernel, members, groups),
            out_shape=(
                jax.ShapeDtypeStruct((FEAT, rows), F32),
                jax.ShapeDtypeStruct((FEAT, rows), F32),
                jax.ShapeDtypeStruct((FEAT, rows), F32),
                jax.ShapeDtypeStruct((features, share), F32),
                jax.ShapeDtypeStruct((8, 128), F32),
            ),
            in_specs=[pl.BlockSpec(memory_space=pltpu.SMEM)] + [hbm] * 6,
            out_specs=(vmem,) * 5,
            scratch_shapes=[
                pltpu.VMEM((FEAT, WIDTH), BF16),
                pltpu.VMEM((rows, WIDTH), BF16),
                pltpu.VMEM((1, rows), jnp.int32),
                pltpu.VMEM((PAIRS, WIDTH, PAIR_ROWS), BF16),
                pltpu.VMEM((WIDTH, rows), F32),
                pltpu.VMEM((WIDTH, rows), BF16),
                pltpu.VMEM((3, members, FEAT, rows), BF16),
                pltpu.VMEM((members, PAIRS, AUG_ROWS, rows), BF16),
                pltpu.VMEM((8, rows), jnp.int32),
                pltpu.VMEM((members, 8, rows), jnp.int32),
                pltpu.VMEM((2 * HEADS, rows), F32),
                pltpu.VMEM((total, rows), F32),
                pltpu.VMEM((PAIRS, total, 2 * rows), F32),
                pltpu.VMEM((4, FEAT, rows), BF16),
                pltpu.VMEM((2, outer, share, rows), BF16),
                pltpu.VMEM((mine, 4, share, rows), BF16),
                pltpu.VMEM((mine, members, unit_rows, LANES), BF16),
                pltpu.VMEM((mine, 2, chips, unit_rows, LANES), BF16),
                pltpu.VMEM((mine, 2, unit_rows, LANES), BF16),
                pltpu.VMEM((outer, unit_rows, LANES), BF16),
                pltpu.VMEM((8, 128), F32),
                pltpu.VMEM((members, 8, 128), F32),
                pltpu.VMEM((8, 128), F32),
                pltpu.VMEM((groups, 8, 128), F32),
                dma((6,)),
                dma((2 * PAIRS + 1,)),
                dma((2 * PAIRS + 1,)),
                dma((1,)),
                dma((PAIRS,)),
                dma((PAIRS,)),
                dma((1,)),
                dma((1,)),
                dma((2,)),
                dma((1,)),
                dma((2,)),
                dma((1,)),
                dma((mine, 2)),
                dma((1,)),
                dma((1,)),
                dma((3,)),
                dma((3,)),
            ],
            compiler_params=pltpu.CompilerParams(collective_id=0, has_side_effects=True, vmem_limit_bytes=48000000),
            name="sublayer",
        )(lengths, *[pltpu.with_memory_space_constraint(operand, pltpu.HBM) for operand in operands])
        final = pl.pallas_call(
            functools.partial(scale_kernel, groups * total, total),
            out_shape=(
                jax.ShapeDtypeStruct((FEAT, rows), F32),
                jax.ShapeDtypeStruct((FEAT, rows), F32),
                jax.ShapeDtypeStruct((FEAT, rows), F32),
                jax.ShapeDtypeStruct((features, share), F32),
                jax.ShapeDtypeStruct((1, 1), F32),
            ),
            in_specs=[vmem] * 5,
            out_specs=(vmem,) * 5,
            compiler_params=pltpu.CompilerParams(vmem_limit_bytes=8000000),
            name="scale",
        )(outs[4], *outs[:4])
        return (final[0].T[None], final[1].T[None], final[2].T[None], final[3], final[4].reshape(()))

    placed = (
        P("dp", "patch", None),
        P("dp", "patch", None),
        P("dp", "patch", None),
        P(),
        P("dp", "patch", None),
        P("dp"),
        P("dp", "patch"),
    )
    return jax.shard_map(
        local,
        mesh=mesh,
        in_specs=placed,
        out_specs=(
            P("dp", "patch", None),
            P("dp", "patch", None),
            P("dp", "patch", None),
            P("patch", "dp"),
            P(),
        ),
        check_vma=False,
    )
```

```python
import functools
import math

import jax
import jax.numpy as jnp
from jax import lax
from jax.experimental import pallas as pl
from jax.experimental.pallas import tpu as pltpu
from jax.sharding import PartitionSpec as P

MESH = pl.DeviceIdType.MESH
WIDTH = 1152
HEADS = 8
HEAD_DIM = 72
FEAT = 576
PAIRS = HEADS // 2
PAIR_ROWS = 2 * HEAD_DIM
STAT_ROWS = 16
AUG_ROWS = PAIR_ROWS + STAT_ROWS
LANES = 128
NEG_LARGE = -1e30
F32 = jnp.float32
BF16 = jnp.bfloat16
KEY, VALUE, QUERY = range(3)


def nt(left, right):
    return lax.dot_general(left, right, (((1,), (1,)), ((), ())), preferred_element_type=F32)


def nn(left, right):
    return lax.dot_general(left, right, (((1,), (0,)), ((), ())), preferred_element_type=F32)


def tn(left, right):
    return lax.dot_general(left, right, (((0,), (0,)), ((), ())), preferred_element_type=F32)


def pad16(size):
    return -(-size // 16) * 16


def unit_layout(members, groups):
    share, features = WIDTH // groups, FEAT // members
    main = features // LANES * LANES
    rest = features - main
    main_rows = pad16(share) if main else 0
    tiles = -(-share // LANES)
    return share, features, main, rest, main_rows, tiles, main_rows + tiles * pad16(rest)


def kernel(
    members,
    groups,
    len_ref,
    seg_hbm,
    q_hbm,
    k_hbm,
    v_hbm,
    w_hbm,
    t_hbm,
    dq_ref,
    dk_ref,
    dv_ref,
    dw_ref,
    sum_ref,
    w_ref,
    t_ref,
    wt_ref,
    acc_ref,
    dout_ref,
    kvq_ref,
    g_ref,
    seg_own,
    seg_all,
    stat_ref,
    bias_ref,
    prob_ref,
    at_ref,
    dt_own,
    dt_all,
    u_own,
    y_all,
    z_own,
    z_all,
    tile_own,
    tile_all,
    pair_own,
    pair_all,
    sum_own,
    sum_all,
    load_sem,
    far_sem,
    near_sem,
    kvq_send,
    g_far,
    g_near,
    g_send,
    at_send,
    at_recv,
    dt_send,
    dt_recv,
    y_send,
    y_recv,
    z_send,
    z_recv,
    small_send,
    small_recv,
    wave_sem,
):
    rows = q_hbm.shape[1]
    chips = members // 2
    outer = groups // 2
    mine = outer // 2
    half = mine // 2
    share, features, main, rest, main_rows, tiles, unit_rows = unit_layout(members, groups)
    rest_rows = pad16(rest)
    me = lax.axis_index("patch")
    dp = lax.axis_index("dp")
    chip, core = me // 2, me % 2
    step_a, step_b = dp // 2, dp % 2
    partner = chip * 2 + 1 - core
    across = step_a * 2 + 1 - step_b
    slot = step_b * 2 + core

    def patch_peer(shift):
        return lax.rem(me + shift, members)

    def far(shift):
        return lax.rem(chip + shift, chips)

    def outer_peer(shift):
        return lax.rem(step_a + shift, outer)

    loads = [
        pltpu.make_async_copy(k_hbm, kvq_ref.at[KEY, me], load_sem.at[0]),
        pltpu.make_async_copy(v_hbm, kvq_ref.at[VALUE, me], load_sem.at[1]),
        pltpu.make_async_copy(seg_hbm, seg_own, load_sem.at[2]),
        pltpu.make_async_copy(q_hbm, kvq_ref.at[QUERY, me], load_sem.at[3]),
        pltpu.make_async_copy(w_hbm, w_ref, load_sem.at[4]),
        pltpu.make_async_copy(t_hbm, t_ref, load_sem.at[5]),
    ]
    for load in loads:
        load.start()

    barrier = pltpu.get_barrier_semaphore()

    def greet(dp_index, patch_index):
        pl.semaphore_signal(barrier, inc=1, device_id=(dp_index, patch_index), device_id_type=MESH)

    for shift in range(1, members):
        greet(dp, patch_peer(shift))
    for to in (me, partner):
        greet(across, to)

        @pl.when(step_a > 0)
        def _():
            greet(dp - 2, to)

        @pl.when(step_a < outer - 1)
        def _():
            greet(dp + 2, to)

    edges = (step_a == 0).astype(jnp.int32) + (step_a == outer - 1).astype(jnp.int32)
    greeted = members - 1 + 2 + 2 * (2 - edges)

    def token(device, side):
        pl.semaphore_signal(wave_sem.at[side], inc=1, device_id=(device, me), device_id_type=MESH)

    def wave_start():
        @pl.when(step_a > 0)
        def _():
            token(dp - 2, 1)

        @pl.when(step_a < outer - 1)
        def _():
            token(dp + 2, 0)

    def wave_wait():
        @pl.when(step_a > 0)
        def _():
            pl.semaphore_wait(wave_sem.at[0], 1)

        @pl.when(step_a < outer - 1)
        def _():
            pl.semaphore_wait(wave_sem.at[1], 1)

    def copy(src, dst, send, recv, device):
        return pltpu.make_async_remote_copy(
            src_ref=src, dst_ref=dst, send_sem=send, recv_sem=recv, device_id=device, device_id_type=MESH
        )

    def received(ref, recv):
        copy(ref, ref, small_send.at[0], recv, (dp, partner)).wait_recv()

    def sent(ref, send):
        copy(ref, ref, send, small_recv.at[0], (dp, partner)).wait_send()

    def rows_of(pair):
        return pl.ds(PAIR_ROWS * pair, PAIR_ROWS)

    def kvq_part(array, owner, pair):
        if array == QUERY:
            return kvq_ref.at[array, owner]
        return kvq_ref.at[array, owner, rows_of(pair)]

    def kvq_index(array, pair):
        return 2 * PAIRS if array == QUERY else PAIRS * array + pair

    def spread(part, index, send, away, near):
        for shift in range(1, chips):
            copy(part, part, send, away.at[index], (dp, far(shift) * 2 + core)).start()
        copy(part, part, send, near.at[index], (dp, partner)).start()

    def relay_parts(part_at, span_at, index, send, away, near):
        received(part_at(far(1) * 2 + core) if chips == 2 else span_at(chips - 1), away.at[index])
        for shift in range(1, chips):
            part = part_at(far(shift) * 2 + core)
            copy(part, part, send, near.at[index], (dp, partner)).start()

    def kvq_span(array, pair, count):
        if array == QUERY:
            return kvq_ref.at[array, pl.ds(0, count)]
        return kvq_ref.at[array, pl.ds(0, count), rows_of(pair)]

    def kvq_spread(array, pair=0):
        spread(kvq_part(array, me, pair), kvq_index(array, pair), kvq_send.at[0], far_sem, near_sem)

    def kvq_relay(array, pair=0):
        relay_parts(
            lambda owner: kvq_part(array, owner, pair),
            lambda count: kvq_span(array, pair, count),
            kvq_index(array, pair),
            kvq_send.at[0],
            far_sem,
            near_sem,
        )

    def kvq_finish(array, pair=0):
        received(kvq_span(array, pair, chips), near_sem.at[kvq_index(array, pair)])

    def g_spread(pair):
        spread(g_ref.at[me, pair], pair, g_send.at[0], g_far, g_near)

    def g_relay(pair):
        relay_parts(
            lambda owner: g_ref.at[owner, pair],
            lambda count: g_ref.at[pl.ds(0, count), pair],
            pair,
            g_send.at[0],
            g_far,
            g_near,
        )

    def g_finish(pair):
        received(g_ref.at[pl.ds(0, chips), pair], g_near.at[pair])

    def small(index, own_ref, everyone):
        for shift in range(1, members):
            copy(own_ref, everyone.at[me], small_send.at[index], small_recv.at[index], (dp, patch_peer(shift))).start()

    for load in (loads[2], loads[0], loads[1], loads[3]):
        load.wait()
    pl.semaphore_wait(barrier, greeted)
    small(0, seg_own, seg_all)
    for pair in range(PAIRS):
        kvq_spread(KEY, pair)
        kvq_spread(VALUE, pair)
    kvq_spread(QUERY)
    wave_start()
    seg_all[me] = seg_own[...]

    upper = lax.broadcasted_iota(jnp.int32, (PAIR_ROWS, 1), 0) < HEAD_DIM
    masks = [upper.astype(F32).astype(BF16), jnp.logical_not(upper).astype(F32).astype(BF16)]

    def stacked(value):
        return jnp.concatenate([value * masks[0], value * masks[1]], axis=1)

    def merged(value):
        return jnp.concatenate([value[:HEAD_DIM, :rows], value[HEAD_DIM:, rows:]], axis=0)

    def own(array, pair):
        return kvq_ref[array, me, PAIR_ROWS * pair : PAIR_ROWS * (pair + 1), :]

    def whole(array, pair):
        low = PAIR_ROWS * pair
        return jnp.concatenate([kvq_ref[array, j, low : low + PAIR_ROWS, :] for j in range(members)], axis=1)

    stat_row = lax.broadcasted_iota(jnp.int32, (STAT_ROWS, 2 * rows), 0)
    stat_side = (lax.broadcasted_iota(jnp.int32, (STAT_ROWS, 2 * rows), 1) >= rows).astype(jnp.int32)

    def picker(base):
        low = base + 3 * stat_side
        return jnp.where((stat_row >= low) & (stat_row < low + 3), -1.0, 0.0).astype(BF16)

    norm_picker, delta_picker = picker(0), picker(6)

    loads[5].wait()
    acc_ref[...] = -(t_ref[...].astype(F32).T)
    loads[4].wait()
    for pair in range(PAIRS):
        wt_ref[pair] = w_ref[PAIR_ROWS * pair : PAIR_ROWS * (pair + 1), :].astype(F32).T.astype(BF16)
    u_own[:, :, main_rows:, :] = jnp.zeros((mine, members, unit_rows - main_rows, LANES), BF16)

    length = len_ref[0]
    lane_position = lax.broadcasted_iota(jnp.int32, (1, rows), 1)
    own_live = me * rows + lane_position < length
    own_group = jnp.where(own_live, seg_own[...], -1).astype(F32)
    received(seg_all.at[pl.ds(0, members - 1)], small_recv.at[0])
    for j in range(members):
        group = jnp.where(j * rows + lane_position < length, seg_all[j], -1).astype(F32)
        group = jnp.broadcast_to(group, (rows, rows)).T
        bias_ref[j * rows : (j + 1) * rows, :] = jnp.where(group == own_group, 0.0, NEG_LARGE)

    log_scale = math.log2(math.e) / math.sqrt(HEAD_DIM)
    score_scale = 1.0 / math.sqrt(HEAD_DIM)

    def biased(scores):
        bias = bias_ref[...]
        return scores * log_scale + jnp.concatenate([bias, bias], axis=1)

    denoms = []
    kvq_relay(KEY, 0)
    for pair in range(PAIRS):
        kvq_finish(KEY, pair)
        kvq_relay(VALUE, pair)
        scores = biased(tn(whole(KEY, pair), stacked(own(QUERY, pair))))
        row_max = jnp.max(scores, axis=0, keepdims=True)
        probs = jnp.exp2(scores - row_max)
        denom = jnp.sum(probs, axis=0, keepdims=True)
        prob_ref[pair] = probs
        log_norm = (row_max + jnp.log2(denom)) * (1.0 / log_scale)
        for side in (0, 1):
            head = 2 * pair + side
            stat_ref[head : head + 1, :] = log_norm[:, side * rows : (side + 1) * rows]
        denoms.append(denom)
        if pair + 1 < PAIRS:
            kvq_relay(KEY, pair + 1)
        kvq_finish(VALUE, pair)
        accum = nn(whole(VALUE, pair), probs.astype(BF16))
        attn_pair = merged(accum / denom).astype(BF16)
        at_ref[slot, PAIR_ROWS * pair : PAIR_ROWS * (pair + 1), :] = attn_pair
        part = at_ref.at[slot, rows_of(pair)]
        copy(part, part, at_send.at[0], at_recv.at[0], (across, me)).start()
        copy(part, part, at_send.at[0], at_recv.at[1], (dp, partner)).start()
        acc_ref[...] += nn(wt_ref[pair], attn_pair)
        if pair == 2 and outer > 2:
            wave_wait()
            if outer > 3:
                wave_start()

    error = jnp.where(own_live, acc_ref[...], 0.0)
    dout = (2.0 * error).astype(BF16)
    dout_ref[...] = dout
    for z in range(outer):
        for side in (0, 1):
            low = (z * 2 + side) * share
            dt_own[side, z] = dout[low : low + share]
    for chunk in (0, 1):
        for side, to in ((1 - step_b, core), (1 - step_b, 1 - core), (step_b, 1 - core)):
            copy(
                dt_own.at[side, pl.ds(to * mine + chunk * half, half)],
                dt_all.at[pl.ds(chunk * half, half), slot],
                dt_send.at[0],
                dt_recv.at[chunk],
                (step_a * 2 + side, chip * 2 + to),
            ).start()
    for i in range(mine):
        dt_all[i, slot] = dt_own[step_b, core * mine + i]

    def terms(value):
        first = value.astype(BF16).astype(F32)
        second = (value - first).astype(BF16).astype(F32)
        return [first, second, value - first - second]

    for pair in range(PAIRS):
        grad = nn(w_ref[PAIR_ROWS * pair : PAIR_ROWS * (pair + 1), :], dout_ref[...]).astype(BF16)
        g_ref[me, pair, :PAIR_ROWS, :] = grad
        product = grad.astype(F32) * at_ref[slot, PAIR_ROWS * pair : PAIR_ROWS * (pair + 1), :].astype(F32)
        lines = []
        for side in (0, 1):
            lines += terms(stat_ref[2 * pair + side : 2 * pair + side + 1, :])
        for side in (0, 1):
            head = 2 * pair + side
            delta = jnp.sum(product[HEAD_DIM * side : HEAD_DIM * (side + 1)], axis=0, keepdims=True)
            stat_ref[HEADS + head : HEADS + head + 1, :] = delta
            lines += terms(delta)
        lines.append(jnp.zeros((STAT_ROWS - 12, rows), F32))
        g_ref[me, pair, PAIR_ROWS:, :] = jnp.concatenate(lines, axis=0).astype(BF16)
        g_spread(pair)

    loss_part = jnp.sum(jnp.sum(error * error, axis=0, keepdims=True), axis=1, keepdims=True)
    tile_own[...] = jnp.broadcast_to(loss_part, tile_own.shape)
    small(1, tile_own, tile_all)
    tile_all[me] = tile_own[...]

    def query_pass(pair):
        low = HEADS + 2 * pair
        delta = jnp.concatenate([stat_ref[low : low + 1, :], stat_ref[low + 1 : low + 2, :]], axis=1)
        grad = g_ref[me, pair, :PAIR_ROWS, :]
        dprobs = tn(whole(VALUE, pair), stacked(grad))
        dscores = prob_ref[pair] * (1.0 / denoms[pair]) * (dprobs - delta)
        value = nn(whole(KEY, pair), dscores.astype(BF16))
        dq_ref[PAIR_ROWS * pair : PAIR_ROWS * (pair + 1), :] = merged(value) * score_scale

    def key_pass(pair):
        g_finish(pair)
        queries = whole(QUERY, pair)
        grads = jnp.concatenate([g_ref[j, pair] for j in range(members)], axis=1)
        stats = grads[PAIR_ROWS:]
        scores = tn(
            jnp.concatenate([queries, stats], axis=0),
            jnp.concatenate([stacked(own(KEY, pair)), norm_picker], axis=0),
        )
        probs = jnp.exp2(biased(scores))
        dv_ref[PAIR_ROWS * pair : PAIR_ROWS * (pair + 1), :] = merged(nn(grads[:PAIR_ROWS], probs.astype(BF16)))
        dprobs = tn(grads, jnp.concatenate([stacked(own(VALUE, pair)), delta_picker], axis=0))
        dscores = (probs * dprobs).astype(BF16)
        dk_ref[PAIR_ROWS * pair : PAIR_ROWS * (pair + 1), :] = merged(nn(queries, dscores)) * score_scale

    def weight_part(chunk):
        received(dt_all.at[pl.ds(chunk * half, half), pl.ds(0, 3)], dt_recv.at[chunk])
        attn = jnp.concatenate([at_ref[s] for s in range(4)], axis=1)
        if main:
            attn_main = jnp.concatenate([attn[p * features : p * features + main] for p in range(members)], axis=0)
            attn_rest = jnp.concatenate([attn[p * features + main : (p + 1) * features] for p in range(members)], axis=0)
        else:
            attn_rest = attn
        for i in range(chunk * half, (chunk + 1) * half):
            grads = jnp.concatenate([dt_all[i, s] for s in range(4)], axis=1)
            if main:
                part_main = nt(grads, attn_main).astype(BF16)
            part_rest = nt(attn_rest, grads)
            for p in range(members):
                if main:
                    u_own[i, p, :share, :] = part_main[:, p * main : (p + 1) * main]
                for t in range(tiles):
                    wide = min(share - t * LANES, LANES)
                    piece = part_rest[p * rest : (p + 1) * rest, t * LANES : t * LANES + wide].astype(BF16)
                    low = main_rows + t * rest_rows
                    u_own[i, p, low : low + rest, :wide] = piece
            for to in (0, 1):
                for shift in range(1, chips):
                    copy(
                        u_own.at[i, far(shift) * 2 + to],
                        y_all.at[i, to, chip],
                        y_send.at[0],
                        y_recv.at[i, to],
                        (dp, far(shift) * 2 + core),
                    ).start()

    def weight_sum(i, to):
        received(y_all.at[i, to, pl.ds(0, chips - 1)], y_recv.at[i, to])
        value = u_own[i, chip * 2 + to].astype(F32)
        for shift in range(1, chips):
            value = value + y_all[i, to, far(shift)].astype(F32)
        z_own[i, to] = value.astype(BF16)
        target = core * mine + i
        stays = jnp.logical_and(target == step_a, core == to)

        @pl.when(stays)
        def _():
            z_all[step_a] = z_own[i, to]

        @pl.when(jnp.logical_not(stays))
        def _():
            copy(
                z_own.at[i, to],
                z_all.at[step_a],
                z_send.at[0],
                z_recv.at[0],
                (target * 2 + step_b, chip * 2 + to),
            ).start()

    for hops in range(4, outer + 1):
        wave_wait()
        if hops < outer:
            wave_start()
    kvq_relay(QUERY)
    received(at_ref.at[0], at_recv.at[0])
    part = at_ref.at[(1 - step_b) * 2 + core]
    copy(part, part, at_send.at[0], at_recv.at[1], (dp, partner)).start()
    query_pass(0)
    g_relay(0)
    query_pass(1)
    g_relay(1)
    received(at_ref.at[pl.ds(0, 2)], at_recv.at[1])
    weight_part(0)
    g_relay(2)
    query_pass(2)
    weight_part(1)
    g_relay(3)

    received(tile_all.at[pl.ds(0, members - 1)], small_recv.at[1])
    pack_loss = tile_all[0]
    for j in range(1, members):
        pack_loss = pack_loss + tile_all[j]
    tile_lane = lax.broadcasted_iota(jnp.int32, pack_loss.shape, 1)
    pair_own[...] = jnp.where(tile_lane == 0, pack_loss, length.astype(F32))
    copy(pair_own, pair_all, small_send.at[3], small_recv.at[3], (across, me)).start()

    query_pass(3)
    kvq_finish(QUERY)
    key_pass(0)
    units = [(i, to) for i in range(mine) for to in (0, 1)]
    quarter = len(units) // 4
    for i, to in units[: 2 * quarter]:
        weight_sum(i, to)
    received(pair_all, small_recv.at[3])
    sum_own[...] = pair_own[...] + pair_all[...]
    for shift in range(1, outer):
        to = outer_peer(shift) * 2 + step_b
        copy(sum_own, sum_all.at[step_a], small_send.at[2], small_recv.at[2], (to, me)).start()
    sum_all[step_a] = sum_own[...]
    key_pass(1)
    for i, to in units[2 * quarter : 3 * quarter]:
        weight_sum(i, to)
    key_pass(2)
    for i, to in units[3 * quarter :]:
        weight_sum(i, to)
    key_pass(3)

    received(sum_all.at[pl.ds(0, outer - 1)], small_recv.at[2])
    totals = sum_all[0]
    for j in range(1, outer):
        totals = totals + sum_all[j]
    sum_ref[...] = totals

    sent(kvq_ref.at[:, pl.ds(0, members - 1)], kvq_send.at[0])
    sent(g_ref.at[pl.ds(0, members - 1)], g_send.at[0])
    sent(at_ref.at[pl.ds(0, 3)], at_send.at[0])
    sent(dt_all.at[:, pl.ds(0, 3)], dt_send.at[0])
    sent(y_all.at[:, :, pl.ds(0, chips - 1)], y_send.at[0])
    sent(seg_all.at[pl.ds(0, members - 1)], small_send.at[0])
    sent(tile_all.at[pl.ds(0, members - 1)], small_send.at[1])
    sent(sum_all.at[pl.ds(0, outer - 1)], small_send.at[2])
    sent(pair_all, small_send.at[3])

    collects = core == step_a // mine

    @pl.when(collects)
    def _():
        sent(z_all.at[pl.ds(0, outer - 1)], z_send.at[0])
        received(z_all.at[pl.ds(0, outer - 1)], z_recv.at[0])

    @pl.when(jnp.logical_not(collects))
    def _():
        sent(z_all, z_send.at[0])
        received(z_all, z_recv.at[0])

    summed = z_all[0].astype(F32)
    for j in range(1, outer):
        summed = summed + z_all[j].astype(F32)
    if main:
        dw_ref[:main, :] = summed[:share].T
    for t in range(tiles):
        wide = min(share - t * LANES, LANES)
        low = main_rows + t * rest_rows
        dw_ref[main:, t * LANES : t * LANES + wide] = summed[low : low + rest, :wide]


def scale_kernel(slots, total, sum_ref, dq_ref, dk_ref, dv_ref, dw_ref, query_ref, key_ref, value_ref, weight_ref, loss_ref):
    count = sum_ref[0:1, 1:2]
    ratio = slots / count
    query_ref[...] = dq_ref[...] * ratio
    key_ref[...] = dk_ref[...] * ratio
    value_ref[...] = dv_ref[...] * ratio
    weight_ref[...] = dw_ref[...] * (ratio / total)
    loss_ref[...] = sum_ref[0:1, 0:1] / (count * WIDTH)


def solution(mesh):
    members, groups = mesh.shape["patch"], mesh.shape["dp"]

    def local(query_rows, key_rows, value_rows, out_weight, target, lengths, segments):
        rows = query_rows.shape[1]
        total = rows * members
        chips = members // 2
        outer = groups // 2
        mine = outer // 2
        share, features, main, rest, main_rows, tiles, unit_rows = unit_layout(members, groups)
        vmem = pl.BlockSpec(memory_space=pltpu.VMEM)
        hbm = pl.BlockSpec(memory_space=pltpu.HBM)
        dma = pltpu.SemaphoreType.DMA
        operands = (
            segments,
            query_rows[0].T,
            key_rows[0].T,
            value_rows[0].T,
            out_weight,
            target[0],
        )
        outs = pl.pallas_call(
            functools.partial(kernel, members, groups),
            out_shape=(
                jax.ShapeDtypeStruct((FEAT, rows), F32),
                jax.ShapeDtypeStruct((FEAT, rows), F32),
                jax.ShapeDtypeStruct((FEAT, rows), F32),
                jax.ShapeDtypeStruct((features, share), F32),
                jax.ShapeDtypeStruct((8, 128), F32),
            ),
            in_specs=[pl.BlockSpec(memory_space=pltpu.SMEM)] + [hbm] * 6,
            out_specs=(vmem,) * 5,
            scratch_shapes=[
                pltpu.VMEM((FEAT, WIDTH), BF16),
                pltpu.VMEM((rows, WIDTH), BF16),
                pltpu.VMEM((PAIRS, WIDTH, PAIR_ROWS), BF16),
                pltpu.VMEM((WIDTH, rows), F32),
                pltpu.VMEM((WIDTH, rows), BF16),
                pltpu.VMEM((3, members, FEAT, rows), BF16),
                pltpu.VMEM((members, PAIRS, AUG_ROWS, rows), BF16),
                pltpu.VMEM((1, rows), jnp.int32),
                pltpu.VMEM((members, 1, rows), jnp.int32),
                pltpu.VMEM((2 * HEADS, rows), F32),
                pltpu.VMEM((total, rows), F32),
                pltpu.VMEM((PAIRS, total, 2 * rows), F32),
                pltpu.VMEM((4, FEAT, rows), BF16),
                pltpu.VMEM((2, outer, share, rows), BF16),
                pltpu.VMEM((mine, 4, share, rows), BF16),
                pltpu.VMEM((mine, members, unit_rows, LANES), BF16),
                pltpu.VMEM((mine, 2, chips, unit_rows, LANES), BF16),
                pltpu.VMEM((mine, 2, unit_rows, LANES), BF16),
                pltpu.VMEM((outer, unit_rows, LANES), BF16),
                pltpu.VMEM((8, 128), F32),
                pltpu.VMEM((members, 8, 128), F32),
                pltpu.VMEM((8, 128), F32),
                pltpu.VMEM((8, 128), F32),
                pltpu.VMEM((8, 128), F32),
                pltpu.VMEM((outer, 8, 128), F32),
                dma((6,)),
                dma((2 * PAIRS + 1,)),
                dma((2 * PAIRS + 1,)),
                dma((1,)),
                dma((PAIRS,)),
                dma((PAIRS,)),
                dma((1,)),
                dma((1,)),
                dma((2,)),
                dma((1,)),
                dma((2,)),
                dma((1,)),
                dma((mine, 2)),
                dma((1,)),
                dma((1,)),
                dma((4,)),
                dma((4,)),
                pltpu.SemaphoreType.REGULAR((2,)),
            ],
            compiler_params=pltpu.CompilerParams(collective_id=0, has_side_effects=True, vmem_limit_bytes=48000000),
            name="sublayer",
        )(lengths, *[pltpu.with_memory_space_constraint(operand, pltpu.HBM) for operand in operands])
        final = pl.pallas_call(
            functools.partial(scale_kernel, groups * total, total),
            out_shape=(
                jax.ShapeDtypeStruct((FEAT, rows), F32),
                jax.ShapeDtypeStruct((FEAT, rows), F32),
                jax.ShapeDtypeStruct((FEAT, rows), F32),
                jax.ShapeDtypeStruct((features, share), F32),
                jax.ShapeDtypeStruct((1, 1), F32),
            ),
            in_specs=[vmem] * 5,
            out_specs=(vmem,) * 5,
            compiler_params=pltpu.CompilerParams(vmem_limit_bytes=8000000),
            name="scale",
        )(outs[4], *outs[:4])
        return (final[0].T[None], final[1].T[None], final[2].T[None], final[3], final[4].reshape(()))

    placed = (
        P("dp", "patch", None),
        P("dp", "patch", None),
        P("dp", "patch", None),
        P(),
        P("dp", "patch", None),
        P("dp"),
        P("dp", "patch"),
    )
    return jax.shard_map(
        local,
        mesh=mesh,
        in_specs=placed,
        out_specs=(
            P("dp", "patch", None),
            P("dp", "patch", None),
            P("dp", "patch", None),
            P("patch", "dp"),
            P(),
        ),
        check_vma=False,
    )
```

```python
import functools
import math

import jax
import jax.numpy as jnp
from jax import lax
from jax.experimental import pallas as pl
from jax.experimental.pallas import tpu as pltpu
from jax.sharding import PartitionSpec as P

MESH = pl.DeviceIdType.MESH
WIDTH = 1152
HEADS = 8
HEAD_DIM = 72
FEAT = 576
PAIRS = HEADS // 2
PAIR_ROWS = 2 * HEAD_DIM
STAT_ROWS = 16
AUG_ROWS = PAIR_ROWS + STAT_ROWS
LANES = 128
NEG_LARGE = -1e30
F32 = jnp.float32
BF16 = jnp.bfloat16
KEY, VALUE, QUERY = range(3)


def nt(left, right):
    return lax.dot_general(left, right, (((1,), (1,)), ((), ())), preferred_element_type=F32)


def nn(left, right):
    return lax.dot_general(left, right, (((1,), (0,)), ((), ())), preferred_element_type=F32)


def tn(left, right):
    return lax.dot_general(left, right, (((0,), (0,)), ((), ())), preferred_element_type=F32)


def pad16(size):
    return -(-size // 16) * 16


def unit_layout(members, groups):
    share, features = WIDTH // groups, FEAT // members
    main = features // LANES * LANES
    rest = features - main
    main_rows = pad16(share) if main else 0
    tiles = -(-share // LANES)
    return share, features, main, rest, main_rows, tiles, main_rows + tiles * pad16(rest)


def kernel(
    members,
    groups,
    len_ref,
    seg_hbm,
    q_hbm,
    k_hbm,
    v_hbm,
    w_hbm,
    t_hbm,
    dq_ref,
    dk_ref,
    dv_ref,
    dw_ref,
    sum_ref,
    w_ref,
    t_ref,
    wt_ref,
    acc_ref,
    dout_ref,
    kvq_ref,
    g_ref,
    seg_own,
    seg_all,
    stat_ref,
    bias_ref,
    prob_ref,
    at_ref,
    tt_own,
    tt_all,
    other_ref,
    u_own,
    y_all,
    z_own,
    z_all,
    tile_own,
    tile_all,
    pair_own,
    pair_all,
    sum_own,
    sum_all,
    load_sem,
    far_sem,
    near_sem,
    kvq_send,
    g_far,
    g_near,
    g_send,
    at_send,
    at_recv,
    tt_send,
    tt_recv,
    y_send,
    y_recv,
    z_send,
    z_recv,
    small_send,
    small_recv,
    wave_sem,
):
    rows = q_hbm.shape[1]
    chips = members // 2
    outer = groups // 2
    mine = outer // 2
    share, features, main, rest, main_rows, tiles, unit_rows = unit_layout(members, groups)
    rest_rows = pad16(rest)
    me = lax.axis_index("patch")
    dp = lax.axis_index("dp")
    chip, core = me // 2, me % 2
    step_a, step_b = dp // 2, dp % 2
    partner = chip * 2 + 1 - core
    across = step_a * 2 + 1 - step_b
    slot = step_b * 2 + core
    job = (core + chip) % 2

    def patch_peer(shift):
        return lax.rem(me + shift, members)

    def far(shift):
        return lax.rem(chip + shift, chips)

    def outer_peer(shift):
        return lax.rem(step_a + shift, outer)

    loads = [
        pltpu.make_async_copy(k_hbm, kvq_ref.at[KEY, me], load_sem.at[0]),
        pltpu.make_async_copy(v_hbm, kvq_ref.at[VALUE, me], load_sem.at[1]),
        pltpu.make_async_copy(seg_hbm, seg_own, load_sem.at[2]),
        pltpu.make_async_copy(q_hbm, kvq_ref.at[QUERY, me], load_sem.at[3]),
        pltpu.make_async_copy(w_hbm, w_ref, load_sem.at[4]),
        pltpu.make_async_copy(t_hbm, t_ref, load_sem.at[5]),
    ]
    for load in loads:
        load.start()

    barrier = pltpu.get_barrier_semaphore()

    def greet(dp_index, patch_index):
        pl.semaphore_signal(barrier, inc=1, device_id=(dp_index, patch_index), device_id_type=MESH)

    for shift in range(1, members):
        greet(dp, patch_peer(shift))
    for to in (me, partner):
        greet(across, to)

        @pl.when(step_a > 0)
        def _():
            greet(dp - 2, to)

        @pl.when(step_a < outer - 1)
        def _():
            greet(dp + 2, to)

    edges = (step_a == 0).astype(jnp.int32) + (step_a == outer - 1).astype(jnp.int32)
    greeted = members - 1 + 2 + 2 * (2 - edges)

    def token(device, side):
        pl.semaphore_signal(wave_sem.at[side], inc=1, device_id=(device, me), device_id_type=MESH)

    def wave_start():
        @pl.when(step_a > 0)
        def _():
            token(dp - 2, 1)

        @pl.when(step_a < outer - 1)
        def _():
            token(dp + 2, 0)

    def wave_wait():
        @pl.when(step_a > 0)
        def _():
            pl.semaphore_wait(wave_sem.at[0], 1)

        @pl.when(step_a < outer - 1)
        def _():
            pl.semaphore_wait(wave_sem.at[1], 1)

    def copy(src, dst, send, recv, device):
        return pltpu.make_async_remote_copy(
            src_ref=src, dst_ref=dst, send_sem=send, recv_sem=recv, device_id=device, device_id_type=MESH
        )

    def received(ref, recv):
        copy(ref, ref, small_send.at[0], recv, (dp, partner)).wait_recv()

    def sent(ref, send):
        copy(ref, ref, send, small_recv.at[0], (dp, partner)).wait_send()

    def rows_of(pair):
        return pl.ds(PAIR_ROWS * pair, PAIR_ROWS)

    def kvq_part(array, owner, pair):
        if array == QUERY:
            return kvq_ref.at[array, owner]
        return kvq_ref.at[array, owner, rows_of(pair)]

    def kvq_index(array, pair):
        return 2 * PAIRS if array == QUERY else PAIRS * array + pair

    def spread(part, index, send, away, near):
        for shift in range(1, chips):
            copy(part, part, send, away.at[index], (dp, far(shift) * 2 + 1 - core)).start()
        copy(part, part, send, near.at[index], (dp, partner)).start()

    def relay_parts(part_at, span_at, index, send, away, near):
        received(part_at(far(1) * 2 + 1 - core) if chips == 2 else span_at(chips - 1), away.at[index])
        for shift in range(1, chips):
            part = part_at(far(shift) * 2 + 1 - core)
            copy(part, part, send, near.at[index], (dp, partner)).start()

    def kvq_span(array, pair, count):
        if array == QUERY:
            return kvq_ref.at[array, pl.ds(0, count)]
        return kvq_ref.at[array, pl.ds(0, count), rows_of(pair)]

    def kvq_spread(array, pair=0):
        spread(kvq_part(array, me, pair), kvq_index(array, pair), kvq_send.at[0], far_sem, near_sem)

    def kvq_relay(array, pair=0):
        relay_parts(
            lambda owner: kvq_part(array, owner, pair),
            lambda count: kvq_span(array, pair, count),
            kvq_index(array, pair),
            kvq_send.at[0],
            far_sem,
            near_sem,
        )

    def kvq_finish(array, pair=0):
        received(kvq_span(array, pair, chips), near_sem.at[kvq_index(array, pair)])

    def g_spread(pair):
        spread(g_ref.at[me, pair], pair, g_send.at[0], g_far, g_near)

    def g_relay(pair):
        relay_parts(
            lambda owner: g_ref.at[owner, pair],
            lambda count: g_ref.at[pl.ds(0, count), pair],
            pair,
            g_send.at[0],
            g_far,
            g_near,
        )

    def g_finish(pair):
        received(g_ref.at[pl.ds(0, chips), pair], g_near.at[pair])

    def small(index, own_ref, everyone):
        for shift in range(1, members):
            copy(own_ref, everyone.at[me], small_send.at[index], small_recv.at[index], (dp, patch_peer(shift))).start()

    for load in (loads[2], loads[0], loads[1], loads[3]):
        load.wait()
    pl.semaphore_wait(barrier, greeted)
    small(0, seg_own, seg_all)
    for pair in range(PAIRS):
        kvq_spread(KEY, pair)
        kvq_spread(VALUE, pair)
    kvq_spread(QUERY)
    wave_start()
    seg_all[me] = seg_own[...]

    upper = lax.broadcasted_iota(jnp.int32, (PAIR_ROWS, 1), 0) < HEAD_DIM
    masks = [upper.astype(F32).astype(BF16), jnp.logical_not(upper).astype(F32).astype(BF16)]

    def stacked(value):
        return jnp.concatenate([value * masks[0], value * masks[1]], axis=1)

    def merged(value):
        return jnp.concatenate([value[:HEAD_DIM, :rows], value[HEAD_DIM:, rows:]], axis=0)

    def own(array, pair):
        return kvq_ref[array, me, PAIR_ROWS * pair : PAIR_ROWS * (pair + 1), :]

    def whole(array, pair):
        low = PAIR_ROWS * pair
        return jnp.concatenate([kvq_ref[array, j, low : low + PAIR_ROWS, :] for j in range(members)], axis=1)

    stat_row = lax.broadcasted_iota(jnp.int32, (STAT_ROWS, 2 * rows), 0)
    stat_side = (lax.broadcasted_iota(jnp.int32, (STAT_ROWS, 2 * rows), 1) >= rows).astype(jnp.int32)

    def picker(base):
        low = base + 3 * stat_side
        return jnp.where((stat_row >= low) & (stat_row < low + 3), -1.0, 0.0).astype(BF16)

    norm_picker, delta_picker = picker(0), picker(6)

    loads[5].wait()
    target = t_ref[...].astype(F32).T
    acc_ref[...] = -target
    for z in range(outer):
        for side in (0, 1):
            low = (z * 2 + side) * share
            tt_own[side, z] = target[low : low + share].astype(BF16)
    peers = ((1 - step_b, core), (1 - step_b, 1 - core), (step_b, 1 - core))
    for side, to in peers:
        copy(
            tt_own.at[side, pl.ds((to + chip) % 2 * mine, mine)],
            tt_all.at[slot],
            tt_send.at[0],
            tt_recv.at[0],
            (step_a * 2 + side, chip * 2 + to),
        ).start()
    for i in range(mine):
        tt_all[slot, i] = tt_own[step_b, job * mine + i]
    loads[4].wait()
    for pair in range(PAIRS):
        turned = w_ref[PAIR_ROWS * pair : PAIR_ROWS * (pair + 1), :].astype(F32).T
        for block in range(groups):
            wt_ref[pair, block] = turned[block * share : (block + 1) * share].astype(BF16)
    u_own[:, :, main_rows:, :] = jnp.zeros((mine, members, unit_rows - main_rows, LANES), BF16)

    length = len_ref[0]
    lane_position = lax.broadcasted_iota(jnp.int32, (1, rows), 1)
    own_live = me * rows + lane_position < length
    own_group = jnp.where(own_live, seg_own[...], -1).astype(F32)
    received(seg_all.at[pl.ds(0, members - 1)], small_recv.at[0])
    for j in range(members):
        group = jnp.where(j * rows + lane_position < length, seg_all[j], -1).astype(F32)
        group = jnp.broadcast_to(group, (rows, rows)).T
        bias_ref[j * rows : (j + 1) * rows, :] = jnp.where(group == own_group, 0.0, NEG_LARGE)

    log_scale = math.log2(math.e) / math.sqrt(HEAD_DIM)
    score_scale = 1.0 / math.sqrt(HEAD_DIM)

    def biased(scores):
        bias = bias_ref[...]
        return scores * log_scale + jnp.concatenate([bias, bias], axis=1)

    denoms = []
    kvq_relay(KEY, 0)
    for pair in range(PAIRS):
        kvq_finish(KEY, pair)
        kvq_relay(VALUE, pair)
        scores = biased(tn(whole(KEY, pair), stacked(own(QUERY, pair))))
        row_max = jnp.max(scores, axis=0, keepdims=True)
        probs = jnp.exp2(scores - row_max)
        denom = jnp.sum(probs, axis=0, keepdims=True)
        prob_ref[pair] = probs
        log_norm = (row_max + jnp.log2(denom)) * (1.0 / log_scale)
        for side in (0, 1):
            head = 2 * pair + side
            stat_ref[head : head + 1, :] = log_norm[:, side * rows : (side + 1) * rows]
        denoms.append(denom)
        if pair + 1 < PAIRS:
            kvq_relay(KEY, pair + 1)
        kvq_finish(VALUE, pair)
        accum = nn(whole(VALUE, pair), probs.astype(BF16))
        attn_pair = jnp.where(own_live, merged(accum / denom), 0.0).astype(BF16)
        at_ref[slot, PAIR_ROWS * pair : PAIR_ROWS * (pair + 1), :] = attn_pair
        part = at_ref.at[slot, rows_of(pair)]
        for side, to in peers:
            arrival = at_recv.at[pair // (PAIRS - 1)]
            copy(part, part, at_send.at[0], arrival, (step_a * 2 + side, chip * 2 + to)).start()
        if share % 16 == 0:
            acc_ref[...] += nn(wt_ref[pair].reshape(WIDTH, PAIR_ROWS), attn_pair)
        else:
            for block in range(groups):
                acc_ref[block * share : (block + 1) * share, :] += nn(wt_ref[pair, block], attn_pair)
        if pair == 2 and outer > 2:
            wave_wait()
            if outer > 3:
                wave_start()

    error = jnp.where(own_live, acc_ref[...], 0.0)
    dout = (2.0 * error).astype(BF16)
    dout_ref[...] = dout
    loss_part = jnp.sum(jnp.sum(error * error, axis=0, keepdims=True), axis=1, keepdims=True)
    tile_own[...] = jnp.broadcast_to(loss_part, tile_own.shape)
    small(1, tile_own, tile_all)
    tile_all[me] = tile_own[...]

    def terms(value):
        first = value.astype(BF16).astype(F32)
        second = (value - first).astype(BF16).astype(F32)
        return [first, second, value - first - second]

    for pair in range(PAIRS):
        grad = nn(w_ref[PAIR_ROWS * pair : PAIR_ROWS * (pair + 1), :], dout_ref[...]).astype(BF16)
        g_ref[me, pair, :PAIR_ROWS, :] = grad
        product = grad.astype(F32) * at_ref[slot, PAIR_ROWS * pair : PAIR_ROWS * (pair + 1), :].astype(F32)
        lines = []
        for side in (0, 1):
            lines += terms(stat_ref[2 * pair + side : 2 * pair + side + 1, :])
        for side in (0, 1):
            head = 2 * pair + side
            delta = jnp.sum(product[HEAD_DIM * side : HEAD_DIM * (side + 1)], axis=0, keepdims=True)
            stat_ref[HEADS + head : HEADS + head + 1, :] = delta
            lines += terms(delta)
        lines.append(jnp.zeros((STAT_ROWS - 12, rows), F32))
        g_ref[me, pair, PAIR_ROWS:, :] = jnp.concatenate(lines, axis=0).astype(BF16)
        g_spread(pair)

    def query_pass(pair):
        low = HEADS + 2 * pair
        delta = jnp.concatenate([stat_ref[low : low + 1, :], stat_ref[low + 1 : low + 2, :]], axis=1)
        grad = g_ref[me, pair, :PAIR_ROWS, :]
        dprobs = tn(whole(VALUE, pair), stacked(grad))
        dscores = prob_ref[pair] * (1.0 / denoms[pair]) * (dprobs - delta)
        value = nn(whole(KEY, pair), dscores.astype(BF16))
        dq_ref[PAIR_ROWS * pair : PAIR_ROWS * (pair + 1), :] = merged(value) * score_scale

    def key_pass(pair):
        g_finish(pair)
        queries = whole(QUERY, pair)
        grads = jnp.concatenate([g_ref[j, pair] for j in range(members)], axis=1)
        stats = grads[PAIR_ROWS:]
        scores = tn(
            jnp.concatenate([queries, stats], axis=0),
            jnp.concatenate([stacked(own(KEY, pair)), norm_picker], axis=0),
        )
        probs = jnp.exp2(biased(scores))
        dv_ref[PAIR_ROWS * pair : PAIR_ROWS * (pair + 1), :] = merged(nn(grads[:PAIR_ROWS], probs.astype(BF16)))
        dprobs = tn(grads, jnp.concatenate([stacked(own(VALUE, pair)), delta_picker], axis=0))
        dscores = (probs * dprobs).astype(BF16)
        dk_ref[PAIR_ROWS * pair : PAIR_ROWS * (pair + 1), :] = merged(nn(queries, dscores)) * score_scale

    def attention(pair):
        low = PAIR_ROWS * pair
        return jnp.concatenate([at_ref[s, low : low + PAIR_ROWS, :] for s in range(4)], axis=1)

    def weight_start():
        received(tt_all.at[pl.ds(0, 3)], tt_recv.at[0])
        received(at_ref.at[pl.ds(0, 3), pl.ds(0, FEAT - PAIR_ROWS)], at_recv.at[0])
        for i in range(mine):
            block = (job * mine + i) * 2 + step_b
            value = -jnp.concatenate([tt_all[s, i].astype(F32) for s in range(4)], axis=1)
            for pair in range(PAIRS - 1):
                value = value + nn(wt_ref[pair, block], attention(pair))
            other_ref[i] = value

    def weight_part():
        received(at_ref.at[pl.ds(0, 3), rows_of(PAIRS - 1)], at_recv.at[1])
        attn = jnp.concatenate([at_ref[s] for s in range(4)], axis=1)
        if main:
            attn_main = jnp.concatenate([attn[p * features : p * features + main] for p in range(members)], axis=0)
            attn_rest = jnp.concatenate([attn[p * features + main : (p + 1) * features] for p in range(members)], axis=0)
        else:
            attn_rest = attn
        for i in range(mine):
            block = (job * mine + i) * 2 + step_b
            value = other_ref[i] + nn(wt_ref[PAIRS - 1, block], attention(PAIRS - 1))
            grads = (2.0 * value).astype(BF16)
            if main:
                part_main = nt(grads, attn_main).astype(BF16)
            part_rest = nt(attn_rest, grads)
            for p in range(members):
                if main:
                    u_own[i, p, :share, :] = part_main[:, p * main : (p + 1) * main]
                for t in range(tiles):
                    wide = min(share - t * LANES, LANES)
                    piece = part_rest[p * rest : (p + 1) * rest, t * LANES : t * LANES + wide].astype(BF16)
                    low = main_rows + t * rest_rows
                    u_own[i, p, low : low + rest, :wide] = piece
            for to in (0, 1):
                for shift in range(1, chips):
                    away = far(shift)
                    copy(
                        u_own.at[i, away * 2 + to],
                        y_all.at[i, to, chip],
                        y_send.at[0],
                        y_recv.at[i, to],
                        (dp, away * 2 + (job + away) % 2),
                    ).start()

    def weight_sum(i, to):
        received(y_all.at[i, to, pl.ds(0, chips - 1)], y_recv.at[i, to])
        value = u_own[i, chip * 2 + to].astype(F32)
        for shift in range(1, chips):
            value = value + y_all[i, to, far(shift)].astype(F32)
        z_own[i, to] = value.astype(BF16)
        owner = job * mine + i
        stays = jnp.logical_and(owner == step_a, core == to)

        @pl.when(stays)
        def _():
            z_all[step_a] = z_own[i, to]

        @pl.when(jnp.logical_not(stays))
        def _():
            copy(
                z_own.at[i, to],
                z_all.at[step_a],
                z_send.at[0],
                z_recv.at[0],
                (owner * 2 + step_b, chip * 2 + to),
            ).start()

    for hops in range(4, outer + 1):
        wave_wait()
        if hops < outer:
            wave_start()
    kvq_relay(QUERY)
    query_pass(0)
    weight_start()
    g_relay(0)
    query_pass(1)
    g_relay(1)
    received(tile_all.at[pl.ds(0, members - 1)], small_recv.at[1])
    pack_loss = tile_all[0]
    for j in range(1, members):
        pack_loss = pack_loss + tile_all[j]
    tile_lane = lax.broadcasted_iota(jnp.int32, pack_loss.shape, 1)
    pair_own[...] = jnp.where(tile_lane == 0, pack_loss, length.astype(F32))
    copy(pair_own, pair_all, small_send.at[3], small_recv.at[3], (across, me)).start()
    weight_part()
    g_relay(2)
    query_pass(2)
    g_relay(3)
    query_pass(3)
    received(pair_all, small_recv.at[3])
    sum_own[...] = pair_own[...] + pair_all[...]
    for shift in range(1, outer):
        to = outer_peer(shift) * 2 + step_b
        copy(sum_own, sum_all.at[step_a], small_send.at[2], small_recv.at[2], (to, me)).start()
    sum_all[step_a] = sum_own[...]
    kvq_finish(QUERY)
    key_pass(0)
    units = [(i, to) for i in range(mine) for to in (0, 1)]
    quarter = len(units) // 4
    for i, to in units[: 2 * quarter]:
        weight_sum(i, to)
    key_pass(1)
    for i, to in units[2 * quarter : 3 * quarter]:
        weight_sum(i, to)
    key_pass(2)
    for i, to in units[3 * quarter :]:
        weight_sum(i, to)
    key_pass(3)

    received(sum_all.at[pl.ds(0, outer - 1)], small_recv.at[2])
    totals = sum_all[0]
    for j in range(1, outer):
        totals = totals + sum_all[j]
    sum_ref[...] = totals

    sent(kvq_ref.at[:, pl.ds(0, members - 1)], kvq_send.at[0])
    sent(g_ref.at[pl.ds(0, members - 1)], g_send.at[0])
    sent(at_ref.at[pl.ds(0, 3)], at_send.at[0])
    sent(tt_all.at[pl.ds(0, 3)], tt_send.at[0])
    sent(y_all.at[:, :, pl.ds(0, chips - 1)], y_send.at[0])
    sent(seg_all.at[pl.ds(0, members - 1)], small_send.at[0])
    sent(tile_all.at[pl.ds(0, members - 1)], small_send.at[1])
    sent(sum_all.at[pl.ds(0, outer - 1)], small_send.at[2])
    sent(pair_all, small_send.at[3])

    collects = job == step_a // mine

    @pl.when(collects)
    def _():
        sent(z_all.at[pl.ds(0, outer - 1)], z_send.at[0])
        received(z_all.at[pl.ds(0, outer - 1)], z_recv.at[0])

    @pl.when(jnp.logical_not(collects))
    def _():
        sent(z_all, z_send.at[0])
        received(z_all, z_recv.at[0])

    summed = z_all[0].astype(F32)
    for j in range(1, outer):
        summed = summed + z_all[j].astype(F32)
    if main:
        dw_ref[:main, :] = summed[:share].T
    for t in range(tiles):
        wide = min(share - t * LANES, LANES)
        low = main_rows + t * rest_rows
        dw_ref[main:, t * LANES : t * LANES + wide] = summed[low : low + rest, :wide]


def scale_kernel(slots, total, sum_ref, dq_ref, dk_ref, dv_ref, dw_ref, query_ref, key_ref, value_ref, weight_ref, loss_ref):
    count = sum_ref[0:1, 1:2]
    ratio = slots / count
    query_ref[...] = dq_ref[...] * ratio
    key_ref[...] = dk_ref[...] * ratio
    value_ref[...] = dv_ref[...] * ratio
    weight_ref[...] = dw_ref[...] * (ratio / total)
    loss_ref[...] = sum_ref[0:1, 0:1] / (count * WIDTH)


def solution(mesh):
    members, groups = mesh.shape["patch"], mesh.shape["dp"]

    def local(query_rows, key_rows, value_rows, out_weight, target, lengths, segments):
        rows = query_rows.shape[1]
        total = rows * members
        chips = members // 2
        outer = groups // 2
        mine = outer // 2
        share, features, main, rest, main_rows, tiles, unit_rows = unit_layout(members, groups)
        vmem = pl.BlockSpec(memory_space=pltpu.VMEM)
        hbm = pl.BlockSpec(memory_space=pltpu.HBM)
        dma = pltpu.SemaphoreType.DMA
        operands = (
            segments,
            query_rows[0].T,
            key_rows[0].T,
            value_rows[0].T,
            out_weight,
            target[0],
        )
        outs = pl.pallas_call(
            functools.partial(kernel, members, groups),
            out_shape=(
                jax.ShapeDtypeStruct((FEAT, rows), F32),
                jax.ShapeDtypeStruct((FEAT, rows), F32),
                jax.ShapeDtypeStruct((FEAT, rows), F32),
                jax.ShapeDtypeStruct((features, share), F32),
                jax.ShapeDtypeStruct((8, 128), F32),
            ),
            in_specs=[pl.BlockSpec(memory_space=pltpu.SMEM)] + [hbm] * 6,
            out_specs=(vmem,) * 5,
            scratch_shapes=[
                pltpu.VMEM((FEAT, WIDTH), BF16),
                pltpu.VMEM((rows, WIDTH), BF16),
                pltpu.VMEM((PAIRS, groups, share, PAIR_ROWS), BF16),
                pltpu.VMEM((WIDTH, rows), F32),
                pltpu.VMEM((WIDTH, rows), BF16),
                pltpu.VMEM((3, members, FEAT, rows), BF16),
                pltpu.VMEM((members, PAIRS, AUG_ROWS, rows), BF16),
                pltpu.VMEM((1, rows), jnp.int32),
                pltpu.VMEM((members, 1, rows), jnp.int32),
                pltpu.VMEM((2 * HEADS, rows), F32),
                pltpu.VMEM((total, rows), F32),
                pltpu.VMEM((PAIRS, total, 2 * rows), F32),
                pltpu.VMEM((4, FEAT, rows), BF16),
                pltpu.VMEM((2, outer, share, rows), BF16),
                pltpu.VMEM((4, mine, share, rows), BF16),
                pltpu.VMEM((mine, share, 4 * rows), F32),
                pltpu.VMEM((mine, members, unit_rows, LANES), BF16),
                pltpu.VMEM((mine, 2, chips, unit_rows, LANES), BF16),
                pltpu.VMEM((mine, 2, unit_rows, LANES), BF16),
                pltpu.VMEM((outer, unit_rows, LANES), BF16),
                pltpu.VMEM((8, 128), F32),
                pltpu.VMEM((members, 8, 128), F32),
                pltpu.VMEM((8, 128), F32),
                pltpu.VMEM((8, 128), F32),
                pltpu.VMEM((8, 128), F32),
                pltpu.VMEM((outer, 8, 128), F32),
                dma((6,)),
                dma((2 * PAIRS + 1,)),
                dma((2 * PAIRS + 1,)),
                dma((1,)),
                dma((PAIRS,)),
                dma((PAIRS,)),
                dma((1,)),
                dma((1,)),
                dma((2,)),
                dma((1,)),
                dma((1,)),
                dma((1,)),
                dma((mine, 2)),
                dma((1,)),
                dma((1,)),
                dma((4,)),
                dma((4,)),
                pltpu.SemaphoreType.REGULAR((2,)),
            ],
            compiler_params=pltpu.CompilerParams(collective_id=0, has_side_effects=True, vmem_limit_bytes=48000000),
            name="sublayer",
        )(lengths, *[pltpu.with_memory_space_constraint(operand, pltpu.HBM) for operand in operands])
        final = pl.pallas_call(
            functools.partial(scale_kernel, groups * total, total),
            out_shape=(
                jax.ShapeDtypeStruct((FEAT, rows), F32),
                jax.ShapeDtypeStruct((FEAT, rows), F32),
                jax.ShapeDtypeStruct((FEAT, rows), F32),
                jax.ShapeDtypeStruct((features, share), F32),
                jax.ShapeDtypeStruct((1, 1), F32),
            ),
            in_specs=[vmem] * 5,
            out_specs=(vmem,) * 5,
            compiler_params=pltpu.CompilerParams(vmem_limit_bytes=8000000),
            name="scale",
        )(outs[4], *outs[:4])
        return (final[0].T[None], final[1].T[None], final[2].T[None], final[3], final[4].reshape(()))

    placed = (
        P("dp", "patch", None),
        P("dp", "patch", None),
        P("dp", "patch", None),
        P(),
        P("dp", "patch", None),
        P("dp"),
        P("dp", "patch"),
    )
    return jax.shard_map(
        local,
        mesh=mesh,
        in_specs=placed,
        out_specs=(
            P("dp", "patch", None),
            P("dp", "patch", None),
            P("dp", "patch", None),
            P("patch", "dp"),
            P(),
        ),
        check_vma=False,
    )
```

```python
import functools
import math

import jax
import jax.numpy as jnp
from jax import lax
from jax.experimental import pallas as pl
from jax.experimental.pallas import tpu as pltpu
from jax.sharding import PartitionSpec as P

MESH = pl.DeviceIdType.MESH
WIDTH = 1152
HEADS = 8
HEAD_DIM = 72
FEAT = 576
PAIRS = HEADS // 2
PAIR_ROWS = 2 * HEAD_DIM
STAT_ROWS = 16
AUG_ROWS = PAIR_ROWS + STAT_ROWS
LANES = 128
NEG_LARGE = -1e30
F32 = jnp.float32
BF16 = jnp.bfloat16
KEY, VALUE, QUERY = range(3)


def nt(left, right):
    return lax.dot_general(left, right, (((1,), (1,)), ((), ())), preferred_element_type=F32)


def nn(left, right):
    return lax.dot_general(left, right, (((1,), (0,)), ((), ())), preferred_element_type=F32)


def tn(left, right):
    return lax.dot_general(left, right, (((0,), (0,)), ((), ())), preferred_element_type=F32)


def pad16(size):
    return -(-size // 16) * 16


def unit_layout(members, groups):
    share, features = WIDTH // groups, FEAT // members
    main = features // LANES * LANES
    rest = features - main
    main_rows = pad16(share) if main else 0
    tiles = -(-share // LANES)
    return share, features, main, rest, main_rows, tiles, main_rows + tiles * pad16(rest)


def kernel(
    members,
    groups,
    len_ref,
    seg_hbm,
    q_hbm,
    k_hbm,
    v_hbm,
    w_hbm,
    t_hbm,
    dq_ref,
    dk_ref,
    dv_ref,
    dw_ref,
    sum_ref,
    w_ref,
    t_ref,
    wt_ref,
    acc_ref,
    dout_ref,
    kvq_ref,
    g_ref,
    seg_own,
    seg_all,
    stat_ref,
    bias_ref,
    prob_ref,
    at_ref,
    tt_own,
    tt_all,
    other_ref,
    u_own,
    y_all,
    z_own,
    z_all,
    tile_own,
    tile_all,
    pair_own,
    pair_all,
    sum_own,
    sum_all,
    load_sem,
    far_sem,
    near_sem,
    kvq_send,
    g_far,
    g_near,
    g_send,
    at_send,
    at_recv,
    tt_send,
    tt_recv,
    y_send,
    y_recv,
    z_send,
    z_recv,
    small_send,
    small_recv,
    wave_sem,
):
    rows = q_hbm.shape[1]
    chips = members // 2
    outer = groups // 2
    mine = outer // 2
    share, features, main, rest, main_rows, tiles, unit_rows = unit_layout(members, groups)
    rest_rows = pad16(rest)
    me = lax.axis_index("patch")
    dp = lax.axis_index("dp")
    chip, core = me // 2, me % 2
    step_a, step_b = dp // 2, dp % 2
    partner = chip * 2 + 1 - core
    across = step_a * 2 + 1 - step_b
    slot = step_b * 2 + core
    job = (core + chip) % 2

    def patch_peer(shift):
        return lax.rem(me + shift, members)

    def far(shift):
        return lax.rem(chip + shift, chips)

    def outer_peer(shift):
        return lax.rem(step_a + shift, outer)

    loads = [
        pltpu.make_async_copy(k_hbm, kvq_ref.at[KEY, me], load_sem.at[0]),
        pltpu.make_async_copy(v_hbm, kvq_ref.at[VALUE, me], load_sem.at[1]),
        pltpu.make_async_copy(seg_hbm, seg_own, load_sem.at[2]),
        pltpu.make_async_copy(q_hbm, kvq_ref.at[QUERY, me], load_sem.at[3]),
        pltpu.make_async_copy(w_hbm, w_ref, load_sem.at[4]),
        pltpu.make_async_copy(t_hbm, t_ref, load_sem.at[5]),
    ]
    for load in loads:
        load.start()

    barrier = pltpu.get_barrier_semaphore()

    def greet(dp_index, patch_index):
        pl.semaphore_signal(barrier, inc=1, device_id=(dp_index, patch_index), device_id_type=MESH)

    for shift in range(1, members):
        greet(dp, patch_peer(shift))
    for to in (me, partner):
        greet(across, to)

        @pl.when(step_a > 0)
        def _():
            greet(dp - 2, to)

        @pl.when(step_a < outer - 1)
        def _():
            greet(dp + 2, to)

    edges = (step_a == 0).astype(jnp.int32) + (step_a == outer - 1).astype(jnp.int32)
    greeted = members - 1 + 2 + 2 * (2 - edges)

    def token(device, side):
        pl.semaphore_signal(wave_sem.at[side], inc=1, device_id=(device, me), device_id_type=MESH)

    def wave_start():
        @pl.when(step_a > 0)
        def _():
            token(dp - 2, 1)

        @pl.when(step_a < outer - 1)
        def _():
            token(dp + 2, 0)

    def wave_wait():
        @pl.when(step_a > 0)
        def _():
            pl.semaphore_wait(wave_sem.at[0], 1)

        @pl.when(step_a < outer - 1)
        def _():
            pl.semaphore_wait(wave_sem.at[1], 1)

    def copy(src, dst, send, recv, device):
        return pltpu.make_async_remote_copy(
            src_ref=src, dst_ref=dst, send_sem=send, recv_sem=recv, device_id=device, device_id_type=MESH
        )

    def received(ref, recv):
        copy(ref, ref, small_send.at[0], recv, (dp, partner)).wait_recv()

    def sent(ref, send):
        copy(ref, ref, send, small_recv.at[0], (dp, partner)).wait_send()

    def rows_of(pair):
        return pl.ds(PAIR_ROWS * pair, PAIR_ROWS)

    def kvq_part(array, owner, pair):
        if array == QUERY:
            return kvq_ref.at[array, owner]
        return kvq_ref.at[array, owner, rows_of(pair)]

    def kvq_index(array, pair):
        return 2 * PAIRS if array == QUERY else PAIRS * array + pair

    def spread(part, index, send, away, near):
        for shift in range(1, chips):
            copy(part, part, send, away.at[index], (dp, far(shift) * 2 + 1 - core)).start()
        copy(part, part, send, near.at[index], (dp, partner)).start()

    def relay_parts(part_at, span_at, index, send, away, near):
        received(part_at(far(1) * 2 + 1 - core) if chips == 2 else span_at(chips - 1), away.at[index])
        for shift in range(1, chips):
            part = part_at(far(shift) * 2 + 1 - core)
            copy(part, part, send, near.at[index], (dp, partner)).start()

    def kvq_span(array, pair, count):
        if array == QUERY:
            return kvq_ref.at[array, pl.ds(0, count)]
        return kvq_ref.at[array, pl.ds(0, count), rows_of(pair)]

    def kvq_spread(array, pair=0):
        spread(kvq_part(array, me, pair), kvq_index(array, pair), kvq_send.at[0], far_sem, near_sem)

    def kvq_relay(array, pair=0):
        relay_parts(
            lambda owner: kvq_part(array, owner, pair),
            lambda count: kvq_span(array, pair, count),
            kvq_index(array, pair),
            kvq_send.at[0],
            far_sem,
            near_sem,
        )

    def kvq_finish(array, pair=0):
        received(kvq_span(array, pair, chips), near_sem.at[kvq_index(array, pair)])

    def g_spread(pair):
        spread(g_ref.at[me, pair], pair, g_send.at[0], g_far, g_near)

    def g_relay(pair):
        relay_parts(
            lambda owner: g_ref.at[owner, pair],
            lambda count: g_ref.at[pl.ds(0, count), pair],
            pair,
            g_send.at[0],
            g_far,
            g_near,
        )

    def g_finish(pair):
        received(g_ref.at[pl.ds(0, chips), pair], g_near.at[pair])

    def small(index, own_ref, everyone):
        for shift in range(1, members):
            copy(own_ref, everyone.at[me], small_send.at[index], small_recv.at[index], (dp, patch_peer(shift))).start()

    for load in (loads[2], loads[0], loads[1], loads[3]):
        load.wait()
    pl.semaphore_wait(barrier, greeted)
    small(0, seg_own, seg_all)
    for pair in range(PAIRS):
        kvq_spread(KEY, pair)
        kvq_spread(VALUE, pair)
    kvq_spread(QUERY)
    wave_start()
    seg_all[me] = seg_own[...]

    upper = lax.broadcasted_iota(jnp.int32, (PAIR_ROWS, 1), 0) < HEAD_DIM
    masks = [upper.astype(F32).astype(BF16), jnp.logical_not(upper).astype(F32).astype(BF16)]

    def stacked(value):
        return jnp.concatenate([value * masks[0], value * masks[1]], axis=1)

    def merged(value):
        return jnp.concatenate([value[:HEAD_DIM, :rows], value[HEAD_DIM:, rows:]], axis=0)

    def own(array, pair):
        return kvq_ref[array, me, PAIR_ROWS * pair : PAIR_ROWS * (pair + 1), :]

    def whole(array, pair):
        low = PAIR_ROWS * pair
        return jnp.concatenate([kvq_ref[array, j, low : low + PAIR_ROWS, :] for j in range(members)], axis=1)

    stat_row = lax.broadcasted_iota(jnp.int32, (STAT_ROWS, 2 * rows), 0)
    stat_side = (lax.broadcasted_iota(jnp.int32, (STAT_ROWS, 2 * rows), 1) >= rows).astype(jnp.int32)

    def picker(base):
        low = base + 3 * stat_side
        return jnp.where((stat_row >= low) & (stat_row < low + 3), -1.0, 0.0).astype(BF16)

    norm_picker, delta_picker = picker(0), picker(6)

    loads[5].wait()
    target = t_ref[...].astype(F32).T
    acc_ref[...] = -target
    for z in range(outer):
        for side in (0, 1):
            low = (z * 2 + side) * share
            tt_own[side, z] = target[low : low + share].astype(BF16)
    peers = ((1 - step_b, core), (1 - step_b, 1 - core), (step_b, 1 - core))
    for side, to in peers:
        copy(
            tt_own.at[side, pl.ds((to + chip) % 2 * mine, mine)],
            tt_all.at[slot],
            tt_send.at[0],
            tt_recv.at[0],
            (step_a * 2 + side, chip * 2 + to),
        ).start()
    for i in range(mine):
        tt_all[slot, i] = tt_own[step_b, job * mine + i]
    loads[4].wait()
    for pair in range(PAIRS):
        turned = w_ref[PAIR_ROWS * pair : PAIR_ROWS * (pair + 1), :].astype(F32).T
        for block in range(groups):
            wt_ref[pair, block] = turned[block * share : (block + 1) * share].astype(BF16)
    u_own[:, :, main_rows:, :] = jnp.zeros((mine, members, unit_rows - main_rows, LANES), BF16)

    length = len_ref[0]
    lane_position = lax.broadcasted_iota(jnp.int32, (1, rows), 1)
    own_live = me * rows + lane_position < length
    own_group = jnp.where(own_live, seg_own[...], -1).astype(F32)
    kvq_relay(KEY, 0)
    received(seg_all.at[pl.ds(0, members - 1)], small_recv.at[0])
    for j in range(members):
        group = jnp.where(j * rows + lane_position < length, seg_all[j], -1).astype(F32)
        group = jnp.broadcast_to(group, (rows, rows)).T
        bias_ref[j * rows : (j + 1) * rows, :] = jnp.where(group == own_group, 0.0, NEG_LARGE)

    log_scale = math.log2(math.e) / math.sqrt(HEAD_DIM)
    score_scale = 1.0 / math.sqrt(HEAD_DIM)

    def biased(scores):
        bias = bias_ref[...]
        return scores * log_scale + jnp.concatenate([bias, bias], axis=1)

    def projected(pair):
        attn_pair = at_ref[slot, PAIR_ROWS * pair : PAIR_ROWS * (pair + 1), :]
        if share % 16 == 0:
            return nn(wt_ref[pair].reshape(WIDTH, PAIR_ROWS), attn_pair)
        return jnp.concatenate([nn(wt_ref[pair, block], attn_pair) for block in range(groups)], axis=0)

    inverses = []
    for pair in range(PAIRS):
        kvq_finish(KEY, pair)
        kvq_relay(VALUE, pair)
        scores = biased(tn(whole(KEY, pair), stacked(own(QUERY, pair))))
        row_max = jnp.max(scores, axis=0, keepdims=True)
        probs = jnp.exp2(scores - row_max)
        denom = jnp.sum(probs, axis=0, keepdims=True)
        prob_ref[pair] = probs
        log_norm = (row_max + jnp.log2(denom)) * (1.0 / log_scale)
        for side in (0, 1):
            head = 2 * pair + side
            stat_ref[head : head + 1, :] = log_norm[:, side * rows : (side + 1) * rows]
        inverse = 1.0 / denom
        inverses.append(inverse)
        if pair + 1 < PAIRS:
            kvq_relay(KEY, pair + 1)
        if pair:
            acc_ref[...] += projected(pair - 1)
        kvq_finish(VALUE, pair)
        accum = nn(whole(VALUE, pair), probs.astype(BF16)) * inverse
        attn_pair = jnp.where(own_live, merged(accum), 0.0).astype(BF16)
        at_ref[slot, PAIR_ROWS * pair : PAIR_ROWS * (pair + 1), :] = attn_pair
        part = at_ref.at[slot, rows_of(pair)]
        for side, to in peers:
            arrival = at_recv.at[pair // (PAIRS - 1)]
            copy(part, part, at_send.at[0], arrival, (step_a * 2 + side, chip * 2 + to)).start()
        if pair == 1 and outer > 2:
            wave_wait()
            if outer > 3:
                wave_start()

    error = jnp.where(own_live, acc_ref[...] + projected(PAIRS - 1), 0.0)
    dout = (2.0 * error).astype(BF16)
    dout_ref[...] = dout
    loss_part = jnp.sum(jnp.sum(error * error, axis=0, keepdims=True), axis=1, keepdims=True)
    tile_own[...] = jnp.broadcast_to(loss_part, tile_own.shape)
    small(1, tile_own, tile_all)
    tile_all[me] = tile_own[...]

    def terms(value):
        first = value.astype(BF16).astype(F32)
        second = (value - first).astype(BF16).astype(F32)
        return [first, second, value - first - second]

    for pair in range(PAIRS):
        grad = nn(w_ref[PAIR_ROWS * pair : PAIR_ROWS * (pair + 1), :], dout_ref[...]).astype(BF16)
        g_ref[me, pair, :PAIR_ROWS, :] = grad
        product = grad.astype(F32) * at_ref[slot, PAIR_ROWS * pair : PAIR_ROWS * (pair + 1), :].astype(F32)
        lines = []
        for side in (0, 1):
            lines += terms(stat_ref[2 * pair + side : 2 * pair + side + 1, :])
        for side in (0, 1):
            head = 2 * pair + side
            delta = jnp.sum(product[HEAD_DIM * side : HEAD_DIM * (side + 1)], axis=0, keepdims=True)
            stat_ref[HEADS + head : HEADS + head + 1, :] = delta
            lines += terms(delta)
        lines.append(jnp.zeros((STAT_ROWS - 12, rows), F32))
        g_ref[me, pair, PAIR_ROWS:, :] = jnp.concatenate(lines, axis=0).astype(BF16)
        g_spread(pair)

    def query_pass(pair):
        low = HEADS + 2 * pair
        delta = jnp.concatenate([stat_ref[low : low + 1, :], stat_ref[low + 1 : low + 2, :]], axis=1)
        grad = g_ref[me, pair, :PAIR_ROWS, :]
        dprobs = tn(whole(VALUE, pair), stacked(grad))
        dscores = prob_ref[pair] * inverses[pair] * (dprobs - delta)
        value = nn(whole(KEY, pair), dscores.astype(BF16))
        dq_ref[PAIR_ROWS * pair : PAIR_ROWS * (pair + 1), :] = merged(value) * score_scale

    def key_pass(pair):
        g_finish(pair)
        queries = whole(QUERY, pair)
        grads = jnp.concatenate([g_ref[j, pair] for j in range(members)], axis=1)
        stats = grads[PAIR_ROWS:]
        scores = tn(
            jnp.concatenate([queries, stats], axis=0),
            jnp.concatenate([stacked(own(KEY, pair)), norm_picker], axis=0),
        )
        probs = jnp.exp2(biased(scores))
        dv_ref[PAIR_ROWS * pair : PAIR_ROWS * (pair + 1), :] = merged(nn(grads[:PAIR_ROWS], probs.astype(BF16)))
        dprobs = tn(grads, jnp.concatenate([stacked(own(VALUE, pair)), delta_picker], axis=0))
        dscores = (probs * dprobs).astype(BF16)
        dk_ref[PAIR_ROWS * pair : PAIR_ROWS * (pair + 1), :] = merged(nn(queries, dscores)) * score_scale

    def attention(pair):
        low = PAIR_ROWS * pair
        return jnp.concatenate([at_ref[s, low : low + PAIR_ROWS, :] for s in range(4)], axis=1)

    def weight_start():
        received(tt_all.at[pl.ds(0, 3)], tt_recv.at[0])
        received(at_ref.at[pl.ds(0, 3), pl.ds(0, FEAT - PAIR_ROWS)], at_recv.at[0])
        for i in range(mine):
            block = (job * mine + i) * 2 + step_b
            value = -jnp.concatenate([tt_all[s, i].astype(F32) for s in range(4)], axis=1)
            for pair in range(PAIRS - 1):
                value = value + nn(wt_ref[pair, block], attention(pair))
            other_ref[i] = value

    def weight_blocks(away, blocks, grads, attn, span):
        if main:
            attn_main = jnp.concatenate([attn[p * features : p * features + main] for p in range(span)], axis=0)
            attn_rest = jnp.concatenate([attn[p * features + main : (p + 1) * features] for p in range(span)], axis=0)
            part_main = nt(grads, attn_main).astype(BF16)
        else:
            attn_rest = attn
        part_rest = nt(attn_rest, grads)
        for place, i in enumerate(blocks):
            for p in range(span):
                if main:
                    u_own[i, away + p, :share, :] = part_main[place * share : (place + 1) * share, p * main : (p + 1) * main]
                for t in range(tiles):
                    wide = min(share - t * LANES, LANES)
                    first = place * share + t * LANES
                    low = main_rows + t * rest_rows
                    piece = part_rest[p * rest : (p + 1) * rest, first : first + wide]
                    u_own[i, away + p, low : low + rest, :wide] = piece.astype(BF16)

    def weight_part():
        received(at_ref.at[pl.ds(0, 3), rows_of(PAIRS - 1)], at_recv.at[1])
        last = attention(PAIRS - 1)
        grads = []
        for i in range(mine):
            block = (job * mine + i) * 2 + step_b
            value = other_ref[i] + nn(wt_ref[PAIRS - 1, block], last)
            grads.append((2.0 * value).astype(BF16))

        def send(shift):
            away = far(shift)
            for i in range(mine):
                for to in (0, 1):
                    copy(
                        u_own.at[i, away * 2 + to],
                        y_all.at[i, to, chip],
                        y_send.at[0],
                        y_recv.at[i, to],
                        (dp, away * 2 + (job + away) % 2),
                    ).start()

        if share % 16 == 0 and features % 16 == 0:
            every = jnp.concatenate(grads, axis=0)
            for shift in [*range(1, chips), 0]:
                low = pl.multiple_of(far(shift) * 2 * features, 16)
                attn = jnp.concatenate([at_ref[s, pl.ds(low, 2 * features), :] for s in range(4)], axis=1)
                weight_blocks(far(shift) * 2, range(mine), every, attn, 2)
                if shift:
                    send(shift)
        else:
            attn = jnp.concatenate([at_ref[s] for s in range(4)], axis=1)
            for i in range(mine):
                weight_blocks(0, [i], grads[i], attn, members)
            for shift in range(1, chips):
                send(shift)

    def weight_sum(i, to):
        received(y_all.at[i, to, pl.ds(0, chips - 1)], y_recv.at[i, to])
        value = u_own[i, chip * 2 + to].astype(F32)
        for shift in range(1, chips):
            value = value + y_all[i, to, far(shift)].astype(F32)
        z_own[i, to] = value.astype(BF16)
        owner = job * mine + i
        stays = jnp.logical_and(owner == step_a, core == to)

        @pl.when(stays)
        def _():
            z_all[step_a] = z_own[i, to]

        @pl.when(jnp.logical_not(stays))
        def _():
            copy(
                z_own.at[i, to],
                z_all.at[step_a],
                z_send.at[0],
                z_recv.at[0],
                (owner * 2 + step_b, chip * 2 + to),
            ).start()

    for hops in range(4, outer + 1):
        wave_wait()
        if hops < outer:
            wave_start()
    kvq_relay(QUERY)
    query_pass(0)
    weight_start()
    query_pass(1)
    received(tile_all.at[pl.ds(0, members - 1)], small_recv.at[1])
    pack_loss = tile_all[0]
    for j in range(1, members):
        pack_loss = pack_loss + tile_all[j]
    tile_lane = lax.broadcasted_iota(jnp.int32, pack_loss.shape, 1)
    pair_own[...] = jnp.where(tile_lane == 0, pack_loss, length.astype(F32))
    copy(pair_own, pair_all, small_send.at[3], small_recv.at[3], (across, me)).start()
    weight_part()
    g_relay(0)
    g_relay(1)
    query_pass(2)
    g_relay(2)
    query_pass(3)
    g_relay(3)
    kvq_finish(QUERY)
    units = [(i, to) for i in range(mine) for to in (0, 1)]
    quarter = len(units) // PAIRS
    for pair in range(PAIRS):
        key_pass(pair)
        for i, to in units[pair * quarter : (pair + 1) * quarter]:
            weight_sum(i, to)
        if pair == 0:
            received(pair_all, small_recv.at[3])
            sum_own[...] = pair_own[...] + pair_all[...]
            for shift in range(1, outer):
                to = outer_peer(shift) * 2 + step_b
                copy(sum_own, sum_all.at[step_a], small_send.at[2], small_recv.at[2], (to, me)).start()
            sum_all[step_a] = sum_own[...]

    received(sum_all.at[pl.ds(0, outer - 1)], small_recv.at[2])
    totals = sum_all[0]
    for j in range(1, outer):
        totals = totals + sum_all[j]
    sum_ref[...] = totals

    sent(kvq_ref.at[:, pl.ds(0, members - 1)], kvq_send.at[0])
    sent(g_ref.at[pl.ds(0, members - 1)], g_send.at[0])
    sent(at_ref.at[pl.ds(0, 3)], at_send.at[0])
    sent(tt_all.at[pl.ds(0, 3)], tt_send.at[0])
    sent(y_all.at[:, :, pl.ds(0, chips - 1)], y_send.at[0])
    sent(seg_all.at[pl.ds(0, members - 1)], small_send.at[0])
    sent(tile_all.at[pl.ds(0, members - 1)], small_send.at[1])
    sent(sum_all.at[pl.ds(0, outer - 1)], small_send.at[2])
    sent(pair_all, small_send.at[3])

    collects = job == step_a // mine

    @pl.when(collects)
    def _():
        sent(z_all.at[pl.ds(0, outer - 1)], z_send.at[0])
        received(z_all.at[pl.ds(0, outer - 1)], z_recv.at[0])

    @pl.when(jnp.logical_not(collects))
    def _():
        sent(z_all, z_send.at[0])
        received(z_all, z_recv.at[0])

    summed = z_all[0].astype(F32)
    for j in range(1, outer):
        summed = summed + z_all[j].astype(F32)
    if main:
        dw_ref[:main, :] = summed[:share].T
    for t in range(tiles):
        wide = min(share - t * LANES, LANES)
        low = main_rows + t * rest_rows
        dw_ref[main:, t * LANES : t * LANES + wide] = summed[low : low + rest, :wide]


def scale_kernel(slots, total, sum_ref, dq_ref, dk_ref, dv_ref, dw_ref, query_ref, key_ref, value_ref, weight_ref, loss_ref):
    count = sum_ref[0:1, 1:2]
    ratio = slots / count
    query_ref[...] = dq_ref[...] * ratio
    key_ref[...] = dk_ref[...] * ratio
    value_ref[...] = dv_ref[...] * ratio
    weight_ref[...] = dw_ref[...] * (ratio / total)
    loss_ref[...] = sum_ref[0:1, 0:1] / (count * WIDTH)


def solution(mesh):
    members, groups = mesh.shape["patch"], mesh.shape["dp"]

    def local(query_rows, key_rows, value_rows, out_weight, target, lengths, segments):
        rows = query_rows.shape[1]
        total = rows * members
        chips = members // 2
        outer = groups // 2
        mine = outer // 2
        share, features, main, rest, main_rows, tiles, unit_rows = unit_layout(members, groups)
        vmem = pl.BlockSpec(memory_space=pltpu.VMEM)
        hbm = pl.BlockSpec(memory_space=pltpu.HBM)
        dma = pltpu.SemaphoreType.DMA
        operands = (
            segments,
            query_rows[0].T,
            key_rows[0].T,
            value_rows[0].T,
            out_weight,
            target[0],
        )
        outs = pl.pallas_call(
            functools.partial(kernel, members, groups),
            out_shape=(
                jax.ShapeDtypeStruct((FEAT, rows), F32),
                jax.ShapeDtypeStruct((FEAT, rows), F32),
                jax.ShapeDtypeStruct((FEAT, rows), F32),
                jax.ShapeDtypeStruct((features, share), F32),
                jax.ShapeDtypeStruct((8, 128), F32),
            ),
            in_specs=[pl.BlockSpec(memory_space=pltpu.SMEM)] + [hbm] * 6,
            out_specs=(vmem,) * 5,
            scratch_shapes=[
                pltpu.VMEM((FEAT, WIDTH), BF16),
                pltpu.VMEM((rows, WIDTH), BF16),
                pltpu.VMEM((PAIRS, groups, share, PAIR_ROWS), BF16),
                pltpu.VMEM((WIDTH, rows), F32),
                pltpu.VMEM((WIDTH, rows), BF16),
                pltpu.VMEM((3, members, FEAT, rows), BF16),
                pltpu.VMEM((members, PAIRS, AUG_ROWS, rows), BF16),
                pltpu.VMEM((1, rows), jnp.int32),
                pltpu.VMEM((members, 1, rows), jnp.int32),
                pltpu.VMEM((2 * HEADS, rows), F32),
                pltpu.VMEM((total, rows), F32),
                pltpu.VMEM((PAIRS, total, 2 * rows), F32),
                pltpu.VMEM((4, FEAT, rows), BF16),
                pltpu.VMEM((2, outer, share, rows), BF16),
                pltpu.VMEM((4, mine, share, rows), BF16),
                pltpu.VMEM((mine, share, 4 * rows), F32),
                pltpu.VMEM((mine, members, unit_rows, LANES), BF16),
                pltpu.VMEM((mine, 2, chips, unit_rows, LANES), BF16),
                pltpu.VMEM((mine, 2, unit_rows, LANES), BF16),
                pltpu.VMEM((outer, unit_rows, LANES), BF16),
                pltpu.VMEM((8, 128), F32),
                pltpu.VMEM((members, 8, 128), F32),
                pltpu.VMEM((8, 128), F32),
                pltpu.VMEM((8, 128), F32),
                pltpu.VMEM((8, 128), F32),
                pltpu.VMEM((outer, 8, 128), F32),
                dma((6,)),
                dma((2 * PAIRS + 1,)),
                dma((2 * PAIRS + 1,)),
                dma((1,)),
                dma((PAIRS,)),
                dma((PAIRS,)),
                dma((1,)),
                dma((1,)),
                dma((2,)),
                dma((1,)),
                dma((1,)),
                dma((1,)),
                dma((mine, 2)),
                dma((1,)),
                dma((1,)),
                dma((4,)),
                dma((4,)),
                pltpu.SemaphoreType.REGULAR((2,)),
            ],
            compiler_params=pltpu.CompilerParams(collective_id=0, has_side_effects=True, vmem_limit_bytes=48000000),
            name="sublayer",
        )(lengths, *[pltpu.with_memory_space_constraint(operand, pltpu.HBM) for operand in operands])
        final = pl.pallas_call(
            functools.partial(scale_kernel, groups * total, total),
            out_shape=(
                jax.ShapeDtypeStruct((FEAT, rows), F32),
                jax.ShapeDtypeStruct((FEAT, rows), F32),
                jax.ShapeDtypeStruct((FEAT, rows), F32),
                jax.ShapeDtypeStruct((features, share), F32),
                jax.ShapeDtypeStruct((1, 1), F32),
            ),
            in_specs=[vmem] * 5,
            out_specs=(vmem,) * 5,
            compiler_params=pltpu.CompilerParams(vmem_limit_bytes=8000000),
            name="scale",
        )(outs[4], *outs[:4])
        return (final[0].T[None], final[1].T[None], final[2].T[None], final[3], final[4].reshape(()))

    placed = (
        P("dp", "patch", None),
        P("dp", "patch", None),
        P("dp", "patch", None),
        P(),
        P("dp", "patch", None),
        P("dp"),
        P("dp", "patch"),
    )
    return jax.shard_map(
        local,
        mesh=mesh,
        in_specs=placed,
        out_specs=(
            P("dp", "patch", None),
            P("dp", "patch", None),
            P("dp", "patch", None),
            P("patch", "dp"),
            P(),
        ),
        check_vma=False,
    )
```

```python
import functools
import math

import jax
import jax.numpy as jnp
from jax import lax
from jax.experimental import pallas as pl
from jax.experimental.pallas import tpu as pltpu
from jax.sharding import PartitionSpec as P

MESH = pl.DeviceIdType.MESH
WIDTH = 1152
HEADS = 8
HEAD_DIM = 72
FEAT = 576
PAIRS = HEADS // 2
PAIR_ROWS = 2 * HEAD_DIM
STAT_ROWS = 16
AUG_ROWS = PAIR_ROWS + STAT_ROWS
LANES = 128
NEG_LARGE = -1e30
F32 = jnp.float32
BF16 = jnp.bfloat16
KEY, VALUE, QUERY = range(3)


def nt(left, right):
    return lax.dot_general(left, right, (((1,), (1,)), ((), ())), preferred_element_type=F32)


def nn(left, right):
    return lax.dot_general(left, right, (((1,), (0,)), ((), ())), preferred_element_type=F32)


def tn(left, right):
    return lax.dot_general(left, right, (((0,), (0,)), ((), ())), preferred_element_type=F32)


def pad16(size):
    return -(-size // 16) * 16


def unit_layout(members, groups):
    share, features = WIDTH // groups, FEAT // members
    main = features // LANES * LANES
    rest = features - main
    main_rows = pad16(share) if main else 0
    tiles = -(-share // LANES)
    return share, features, main, rest, main_rows, tiles, main_rows + tiles * pad16(rest)


def kernel(
    members,
    groups,
    len_ref,
    seg_hbm,
    q_hbm,
    k_hbm,
    v_hbm,
    w_hbm,
    t_hbm,
    dq_ref,
    dk_ref,
    dv_ref,
    dw_ref,
    sum_ref,
    w_ref,
    t_ref,
    wt_ref,
    acc_ref,
    dout_ref,
    kvq_ref,
    g_ref,
    seg_own,
    seg_all,
    stat_ref,
    bias_ref,
    prob_ref,
    at_ref,
    tt_own,
    tt_all,
    other_ref,
    u_own,
    y_all,
    z_own,
    z_all,
    tile_own,
    tile_all,
    pair_own,
    pair_all,
    sum_own,
    sum_all,
    load_sem,
    far_sem,
    near_sem,
    kvq_send,
    g_far,
    g_near,
    g_send,
    at_send,
    at_recv,
    tt_send,
    tt_recv,
    y_send,
    y_recv,
    z_send,
    z_recv,
    small_send,
    small_recv,
    wave_sem,
):
    rows = q_hbm.shape[1]
    chips = members // 2
    outer = groups // 2
    mine = outer // 2
    share, features, main, rest, main_rows, tiles, unit_rows = unit_layout(members, groups)
    rest_rows = pad16(rest)
    me = lax.axis_index("patch")
    dp = lax.axis_index("dp")
    chip, core = me // 2, me % 2
    step_a, step_b = dp // 2, dp % 2
    partner = chip * 2 + 1 - core
    across = step_a * 2 + 1 - step_b
    slot = step_b * 2 + core
    job = (core + chip) % 2

    def patch_peer(shift):
        return lax.rem(me + shift, members)

    def far(shift):
        return lax.rem(chip + shift, chips)

    def outer_peer(shift):
        return lax.rem(step_a + shift, outer)

    loads = [
        pltpu.make_async_copy(k_hbm, kvq_ref.at[KEY, me], load_sem.at[0]),
        pltpu.make_async_copy(v_hbm, kvq_ref.at[VALUE, me], load_sem.at[1]),
        pltpu.make_async_copy(seg_hbm, seg_own, load_sem.at[2]),
        pltpu.make_async_copy(q_hbm, kvq_ref.at[QUERY, me], load_sem.at[3]),
        pltpu.make_async_copy(w_hbm, w_ref, load_sem.at[4]),
        pltpu.make_async_copy(t_hbm, t_ref, load_sem.at[5]),
    ]
    for load in loads:
        load.start()

    barrier = pltpu.get_barrier_semaphore()

    def greet(dp_index, patch_index):
        pl.semaphore_signal(barrier, inc=1, device_id=(dp_index, patch_index), device_id_type=MESH)

    for shift in range(1, members):
        greet(dp, patch_peer(shift))
    for to in (me, partner):
        greet(across, to)

        @pl.when(step_a > 0)
        def _():
            greet(dp - 2, to)

        @pl.when(step_a < outer - 1)
        def _():
            greet(dp + 2, to)

    edges = (step_a == 0).astype(jnp.int32) + (step_a == outer - 1).astype(jnp.int32)
    greeted = members - 1 + 2 + 2 * (2 - edges)

    def token(device, side):
        pl.semaphore_signal(wave_sem.at[side], inc=1, device_id=(device, me), device_id_type=MESH)

    def wave_start():
        @pl.when(step_a > 0)
        def _():
            token(dp - 2, 1)

        @pl.when(step_a < outer - 1)
        def _():
            token(dp + 2, 0)

    def wave_wait():
        @pl.when(step_a > 0)
        def _():
            pl.semaphore_wait(wave_sem.at[0], 1)

        @pl.when(step_a < outer - 1)
        def _():
            pl.semaphore_wait(wave_sem.at[1], 1)

    def copy(src, dst, send, recv, device):
        return pltpu.make_async_remote_copy(
            src_ref=src, dst_ref=dst, send_sem=send, recv_sem=recv, device_id=device, device_id_type=MESH
        )

    def received(ref, recv):
        copy(ref, ref, small_send.at[0], recv, (dp, partner)).wait_recv()

    def sent(ref, send):
        copy(ref, ref, send, small_recv.at[0], (dp, partner)).wait_send()

    def rows_of(pair):
        return pl.ds(PAIR_ROWS * pair, PAIR_ROWS)

    def kvq_part(array, owner, pair):
        if array == QUERY:
            return kvq_ref.at[array, owner]
        return kvq_ref.at[array, owner, rows_of(pair)]

    def kvq_index(array, pair):
        return 2 * PAIRS if array == QUERY else PAIRS * array + pair

    def spread(part, index, send, away, near):
        for shift in range(1, chips):
            copy(part, part, send, away.at[index], (dp, far(shift) * 2 + 1 - core)).start()
        copy(part, part, send, near.at[index], (dp, partner)).start()

    def relay_parts(part_at, span_at, index, send, away, near):
        received(part_at(far(1) * 2 + 1 - core) if chips == 2 else span_at(chips - 1), away.at[index])
        for shift in range(1, chips):
            part = part_at(far(shift) * 2 + 1 - core)
            copy(part, part, send, near.at[index], (dp, partner)).start()

    def kvq_span(array, pair, count):
        if array == QUERY:
            return kvq_ref.at[array, pl.ds(0, count)]
        return kvq_ref.at[array, pl.ds(0, count), rows_of(pair)]

    def kvq_spread(array, pair=0):
        spread(kvq_part(array, me, pair), kvq_index(array, pair), kvq_send.at[0], far_sem, near_sem)

    def kvq_relay(array, pair=0):
        relay_parts(
            lambda owner: kvq_part(array, owner, pair),
            lambda count: kvq_span(array, pair, count),
            kvq_index(array, pair),
            kvq_send.at[0],
            far_sem,
            near_sem,
        )

    def kvq_finish(array, pair=0):
        received(kvq_span(array, pair, chips), near_sem.at[kvq_index(array, pair)])

    def g_part(owner, part):
        return g_ref.at[owner, pl.ds(2 * part, 2)]

    def g_span(part, count):
        return g_ref.at[pl.ds(0, count), pl.ds(2 * part, 2)]

    def g_spread(part):
        spread(g_part(me, part), part, g_send.at[0], g_far, g_near)

    def g_relay(part):
        relay_parts(
            lambda owner: g_part(owner, part),
            lambda count: g_span(part, count),
            part,
            g_send.at[0],
            g_far,
            g_near,
        )

    def g_finish(part):
        received(g_span(part, chips), g_near.at[part])

    def small(index, own_ref, everyone):
        for shift in range(1, members):
            copy(own_ref, everyone.at[me], small_send.at[index], small_recv.at[index], (dp, patch_peer(shift))).start()

    loads[0].wait()
    pl.semaphore_wait(barrier, greeted)
    kvq_spread(KEY, 0)
    loads[2].wait()
    small(0, seg_own, seg_all)
    loads[1].wait()
    kvq_spread(VALUE, 0)
    for pair in range(1, PAIRS):
        kvq_spread(KEY, pair)
        kvq_spread(VALUE, pair)
    loads[3].wait()
    kvq_spread(QUERY)
    wave_start()
    seg_all[me] = seg_own[...]

    upper = lax.broadcasted_iota(jnp.int32, (PAIR_ROWS, 1), 0) < HEAD_DIM
    masks = [upper.astype(F32).astype(BF16), jnp.logical_not(upper).astype(F32).astype(BF16)]

    def stacked(value):
        return jnp.concatenate([value * masks[0], value * masks[1]], axis=1)

    def merged(value):
        return jnp.concatenate([value[:HEAD_DIM, :rows], value[HEAD_DIM:, rows:]], axis=0)

    def own(array, pair):
        return kvq_ref[array, me, PAIR_ROWS * pair : PAIR_ROWS * (pair + 1), :]

    def whole(array, pair):
        low = PAIR_ROWS * pair
        return jnp.concatenate([kvq_ref[array, j, low : low + PAIR_ROWS, :] for j in range(members)], axis=1)

    stat_row = lax.broadcasted_iota(jnp.int32, (STAT_ROWS, 2 * rows), 0)
    stat_side = (lax.broadcasted_iota(jnp.int32, (STAT_ROWS, 2 * rows), 1) >= rows).astype(jnp.int32)

    def picker(base):
        low = base + 3 * stat_side
        return jnp.where((stat_row >= low) & (stat_row < low + 3), -1.0, 0.0).astype(BF16)

    norm_picker, delta_picker = picker(0), picker(6)

    loads[5].wait()
    target = t_ref[...].astype(F32).T
    acc_ref[...] = -target
    for z in range(outer):
        for side in (0, 1):
            low = (z * 2 + side) * share
            tt_own[side, z] = target[low : low + share].astype(BF16)
    peers = ((1 - step_b, core), (1 - step_b, 1 - core), (step_b, 1 - core))
    for side, to in peers:
        copy(
            tt_own.at[side, pl.ds((to + chip) % 2 * mine, mine)],
            tt_all.at[slot],
            tt_send.at[0],
            tt_recv.at[0],
            (step_a * 2 + side, chip * 2 + to),
        ).start()
    for i in range(mine):
        tt_all[slot, i] = tt_own[step_b, job * mine + i]
    loads[4].wait()
    for pair in range(PAIRS):
        turned = w_ref[PAIR_ROWS * pair : PAIR_ROWS * (pair + 1), :].astype(F32).T
        for block in range(groups):
            wt_ref[pair, block] = turned[block * share : (block + 1) * share].astype(BF16)
    u_own[:, :, main_rows:, :] = jnp.zeros((mine, members, unit_rows - main_rows, LANES), BF16)

    length = len_ref[0]
    lane_position = lax.broadcasted_iota(jnp.int32, (1, rows), 1)
    own_live = me * rows + lane_position < length
    own_group = jnp.where(own_live, seg_own[...], -1).astype(F32)
    kvq_relay(KEY, 0)
    received(seg_all.at[pl.ds(0, members - 1)], small_recv.at[0])
    for j in range(members):
        group = jnp.where(j * rows + lane_position < length, seg_all[j], -1).astype(F32)
        group = jnp.broadcast_to(group, (rows, rows)).T
        bias_ref[j * rows : (j + 1) * rows, :] = jnp.where(group == own_group, 0.0, NEG_LARGE)

    log_scale = math.log2(math.e) / math.sqrt(HEAD_DIM)
    score_scale = 1.0 / math.sqrt(HEAD_DIM)

    def biased(scores):
        bias = bias_ref[...]
        return scores * log_scale + jnp.concatenate([bias, bias], axis=1)

    def projected(pair):
        attn_pair = at_ref[slot, PAIR_ROWS * pair : PAIR_ROWS * (pair + 1), :]
        if share % 16 == 0:
            return nn(wt_ref[pair].reshape(WIDTH, PAIR_ROWS), attn_pair)
        return jnp.concatenate([nn(wt_ref[pair, block], attn_pair) for block in range(groups)], axis=0)

    inverses = []
    for pair in range(PAIRS):
        kvq_finish(KEY, pair)
        kvq_relay(VALUE, pair)
        scores = biased(tn(whole(KEY, pair), stacked(own(QUERY, pair))))
        row_max = jnp.max(scores, axis=0, keepdims=True)
        probs = jnp.exp2(scores - row_max)
        denom = jnp.sum(probs, axis=0, keepdims=True)
        prob_ref[pair] = probs
        log_norm = (row_max + jnp.log2(denom)) * (1.0 / log_scale)
        for side in (0, 1):
            head = 2 * pair + side
            stat_ref[head : head + 1, :] = log_norm[:, side * rows : (side + 1) * rows]
        inverse = 1.0 / denom
        inverses.append(inverse)
        if pair + 1 < PAIRS:
            kvq_relay(KEY, pair + 1)
        if pair:
            acc_ref[...] += projected(pair - 1)
        kvq_finish(VALUE, pair)
        accum = nn(whole(VALUE, pair), probs.astype(BF16)) * inverse
        attn_pair = jnp.where(own_live, merged(accum), 0.0).astype(BF16)
        at_ref[slot, PAIR_ROWS * pair : PAIR_ROWS * (pair + 1), :] = attn_pair
        part = at_ref.at[slot, rows_of(pair)]
        for side, to in peers:
            arrival = at_recv.at[pair // (PAIRS - 1)]
            copy(part, part, at_send.at[0], arrival, (step_a * 2 + side, chip * 2 + to)).start()
        if pair == 1 and outer > 2:
            wave_wait()
            if outer > 3:
                wave_start()

    error = jnp.where(own_live, acc_ref[...] + projected(PAIRS - 1), 0.0)
    dout = (2.0 * error).astype(BF16)
    dout_ref[...] = dout
    loss_part = jnp.sum(jnp.sum(error * error, axis=0, keepdims=True), axis=1, keepdims=True)
    tile_own[...] = jnp.broadcast_to(loss_part, tile_own.shape)
    small(1, tile_own, tile_all)
    tile_all[me] = tile_own[...]

    def terms(value):
        first = value.astype(BF16).astype(F32)
        second = (value - first).astype(BF16).astype(F32)
        return [first, second, value - first - second]

    for pair in range(PAIRS):
        grad = nn(w_ref[PAIR_ROWS * pair : PAIR_ROWS * (pair + 1), :], dout_ref[...]).astype(BF16)
        g_ref[me, pair, :PAIR_ROWS, :] = grad
        product = grad.astype(F32) * at_ref[slot, PAIR_ROWS * pair : PAIR_ROWS * (pair + 1), :].astype(F32)
        lines = []
        for side in (0, 1):
            lines += terms(stat_ref[2 * pair + side : 2 * pair + side + 1, :])
        for side in (0, 1):
            head = 2 * pair + side
            delta = jnp.sum(product[HEAD_DIM * side : HEAD_DIM * (side + 1)], axis=0, keepdims=True)
            stat_ref[HEADS + head : HEADS + head + 1, :] = delta
            lines += terms(delta)
        lines.append(jnp.zeros((STAT_ROWS - 12, rows), F32))
        g_ref[me, pair, PAIR_ROWS:, :] = jnp.concatenate(lines, axis=0).astype(BF16)
        if pair % 2:
            g_spread(pair // 2)

    def query_pass(pair):
        low = HEADS + 2 * pair
        delta = jnp.concatenate([stat_ref[low : low + 1, :], stat_ref[low + 1 : low + 2, :]], axis=1)
        grad = g_ref[me, pair, :PAIR_ROWS, :]
        dprobs = tn(whole(VALUE, pair), stacked(grad))
        dscores = prob_ref[pair] * inverses[pair] * (dprobs - delta)
        value = nn(whole(KEY, pair), dscores.astype(BF16))
        dq_ref[PAIR_ROWS * pair : PAIR_ROWS * (pair + 1), :] = merged(value) * score_scale

    def key_pass(pair):
        if pair % 2 == 0:
            g_finish(pair // 2)
        queries = whole(QUERY, pair)
        grads = jnp.concatenate([g_ref[j, pair] for j in range(members)], axis=1)
        stats = grads[PAIR_ROWS:]
        scores = tn(
            jnp.concatenate([queries, stats], axis=0),
            jnp.concatenate([stacked(own(KEY, pair)), norm_picker], axis=0),
        )
        probs = jnp.exp2(biased(scores))
        dv_ref[PAIR_ROWS * pair : PAIR_ROWS * (pair + 1), :] = merged(nn(grads[:PAIR_ROWS], probs.astype(BF16)))
        dprobs = tn(grads, jnp.concatenate([stacked(own(VALUE, pair)), delta_picker], axis=0))
        dscores = (probs * dprobs).astype(BF16)
        dk_ref[PAIR_ROWS * pair : PAIR_ROWS * (pair + 1), :] = merged(nn(queries, dscores)) * score_scale

    def attention(pair):
        low = PAIR_ROWS * pair
        return jnp.concatenate([at_ref[s, low : low + PAIR_ROWS, :] for s in range(4)], axis=1)

    def weight_start():
        received(tt_all.at[pl.ds(0, 3)], tt_recv.at[0])
        received(at_ref.at[pl.ds(0, 3), pl.ds(0, FEAT - PAIR_ROWS)], at_recv.at[0])
        for i in range(mine):
            block = (job * mine + i) * 2 + step_b
            value = -jnp.concatenate([tt_all[s, i].astype(F32) for s in range(4)], axis=1)
            for pair in range(PAIRS - 1):
                value = value + nn(wt_ref[pair, block], attention(pair))
            other_ref[i] = value

    def weight_blocks(away, blocks, grads, attn, span):
        if main:
            attn_main = jnp.concatenate([attn[p * features : p * features + main] for p in range(span)], axis=0)
            attn_rest = jnp.concatenate([attn[p * features + main : (p + 1) * features] for p in range(span)], axis=0)
            part_main = nt(grads, attn_main).astype(BF16)
        else:
            attn_rest = attn
        part_rest = nt(attn_rest, grads)
        for place, i in enumerate(blocks):
            for p in range(span):
                if main:
                    u_own[i, away + p, :share, :] = part_main[place * share : (place + 1) * share, p * main : (p + 1) * main]
                for t in range(tiles):
                    wide = min(share - t * LANES, LANES)
                    first = place * share + t * LANES
                    low = main_rows + t * rest_rows
                    piece = part_rest[p * rest : (p + 1) * rest, first : first + wide]
                    u_own[i, away + p, low : low + rest, :wide] = piece.astype(BF16)

    def weight_part():
        received(at_ref.at[pl.ds(0, 3), rows_of(PAIRS - 1)], at_recv.at[1])
        last = attention(PAIRS - 1)

        def grads_of(i):
            block = (job * mine + i) * 2 + step_b
            return (2.0 * (other_ref[i] + nn(wt_ref[PAIRS - 1, block], last))).astype(BF16)

        def send(i, shift):
            away = far(shift)
            for to in (0, 1):
                copy(
                    u_own.at[i, away * 2 + to],
                    y_all.at[i, to, chip],
                    y_send.at[0],
                    y_recv.at[i, to],
                    (dp, away * 2 + (job + away) % 2),
                ).start()

        if share % 16 == 0 and features % 16 == 0:

            def attn_of(shift):
                low = pl.multiple_of(far(shift) * 2 * features, 16)
                return jnp.concatenate([at_ref[s, pl.ds(low, 2 * features), :] for s in range(4)], axis=1)

            grads = []
            for i in range(mine):
                grads.append(grads_of(i))
                for shift in range(1, chips):
                    weight_blocks(far(shift) * 2, [i], grads[i], attn_of(shift), 2)
                    send(i, shift)
            weight_blocks(chip * 2, range(mine), jnp.concatenate(grads, axis=0), attn_of(0), 2)
        else:
            attn = jnp.concatenate([at_ref[s] for s in range(4)], axis=1)
            for i in range(mine):
                weight_blocks(0, [i], grads_of(i), attn, members)
                for shift in range(1, chips):
                    send(i, shift)

    def weight_sum(i, to):
        received(y_all.at[i, to, pl.ds(0, chips - 1)], y_recv.at[i, to])
        value = u_own[i, chip * 2 + to].astype(F32)
        for shift in range(1, chips):
            value = value + y_all[i, to, far(shift)].astype(F32)
        z_own[i, to] = value.astype(BF16)
        owner = job * mine + i
        stays = jnp.logical_and(owner == step_a, core == to)

        @pl.when(stays)
        def _():
            z_all[step_a] = z_own[i, to]

        @pl.when(jnp.logical_not(stays))
        def _():
            copy(
                z_own.at[i, to],
                z_all.at[step_a],
                z_send.at[0],
                z_recv.at[0],
                (owner * 2 + step_b, chip * 2 + to),
            ).start()

    for hops in range(4, outer + 1):
        wave_wait()
        if hops < outer:
            wave_start()
    kvq_relay(QUERY)
    query_pass(0)
    weight_start()
    query_pass(1)
    received(tile_all.at[pl.ds(0, members - 1)], small_recv.at[1])
    pack_loss = tile_all[0]
    for j in range(1, members):
        pack_loss = pack_loss + tile_all[j]
    tile_lane = lax.broadcasted_iota(jnp.int32, pack_loss.shape, 1)
    pair_own[...] = jnp.where(tile_lane == 0, pack_loss, length.astype(F32))
    copy(pair_own, pair_all, small_send.at[3], small_recv.at[3], (across, me)).start()
    weight_part()
    g_relay(0)
    query_pass(2)
    query_pass(3)
    g_relay(1)
    received(pair_all, small_recv.at[3])
    sum_own[...] = pair_own[...] + pair_all[...]
    for shift in range(1, outer):
        to = outer_peer(shift) * 2 + step_b
        copy(sum_own, sum_all.at[step_a], small_send.at[2], small_recv.at[2], (to, me)).start()
    sum_all[step_a] = sum_own[...]
    kvq_finish(QUERY)
    units = [(i, to) for i in range(mine) for to in (0, 1)]
    quarter = len(units) // PAIRS
    for pair in range(PAIRS):
        key_pass(pair)
        for i, to in units[pair * quarter : (pair + 1) * quarter]:
            weight_sum(i, to)

    received(sum_all.at[pl.ds(0, outer - 1)], small_recv.at[2])
    totals = sum_all[0]
    for j in range(1, outer):
        totals = totals + sum_all[j]
    sum_ref[...] = totals

    sent(kvq_ref.at[:, pl.ds(0, members - 1)], kvq_send.at[0])
    sent(g_ref.at[pl.ds(0, members - 1)], g_send.at[0])
    sent(at_ref.at[pl.ds(0, 3)], at_send.at[0])
    sent(tt_all.at[pl.ds(0, 3)], tt_send.at[0])
    sent(y_all.at[:, :, pl.ds(0, chips - 1)], y_send.at[0])
    sent(seg_all.at[pl.ds(0, members - 1)], small_send.at[0])
    sent(tile_all.at[pl.ds(0, members - 1)], small_send.at[1])
    sent(sum_all.at[pl.ds(0, outer - 1)], small_send.at[2])
    sent(pair_all, small_send.at[3])

    collects = job == step_a // mine

    @pl.when(collects)
    def _():
        sent(z_all.at[pl.ds(0, outer - 1)], z_send.at[0])
        received(z_all.at[pl.ds(0, outer - 1)], z_recv.at[0])

    @pl.when(jnp.logical_not(collects))
    def _():
        sent(z_all, z_send.at[0])
        received(z_all, z_recv.at[0])

    summed = z_all[0].astype(F32)
    for j in range(1, outer):
        summed = summed + z_all[j].astype(F32)
    if main:
        dw_ref[:main, :] = summed[:share].T
    for t in range(tiles):
        wide = min(share - t * LANES, LANES)
        low = main_rows + t * rest_rows
        dw_ref[main:, t * LANES : t * LANES + wide] = summed[low : low + rest, :wide]


def scale_kernel(slots, total, sum_ref, dq_ref, dk_ref, dv_ref, dw_ref, query_ref, key_ref, value_ref, weight_ref, loss_ref):
    count = sum_ref[0:1, 1:2]
    ratio = slots / count
    query_ref[...] = dq_ref[...] * ratio
    key_ref[...] = dk_ref[...] * ratio
    value_ref[...] = dv_ref[...] * ratio
    weight_ref[...] = dw_ref[...] * (ratio / total)
    loss_ref[...] = sum_ref[0:1, 0:1] / (count * WIDTH)


def solution(mesh):
    members, groups = mesh.shape["patch"], mesh.shape["dp"]

    def local(query_rows, key_rows, value_rows, out_weight, target, lengths, segments):
        rows = query_rows.shape[1]
        total = rows * members
        chips = members // 2
        outer = groups // 2
        mine = outer // 2
        share, features, main, rest, main_rows, tiles, unit_rows = unit_layout(members, groups)
        vmem = pl.BlockSpec(memory_space=pltpu.VMEM)
        hbm = pl.BlockSpec(memory_space=pltpu.HBM)
        dma = pltpu.SemaphoreType.DMA
        operands = (
            segments,
            query_rows[0].T,
            key_rows[0].T,
            value_rows[0].T,
            out_weight,
            target[0],
        )
        outs = pl.pallas_call(
            functools.partial(kernel, members, groups),
            out_shape=(
                jax.ShapeDtypeStruct((FEAT, rows), F32),
                jax.ShapeDtypeStruct((FEAT, rows), F32),
                jax.ShapeDtypeStruct((FEAT, rows), F32),
                jax.ShapeDtypeStruct((features, share), F32),
                jax.ShapeDtypeStruct((8, 128), F32),
            ),
            in_specs=[pl.BlockSpec(memory_space=pltpu.SMEM)] + [hbm] * 6,
            out_specs=(vmem,) * 5,
            scratch_shapes=[
                pltpu.VMEM((FEAT, WIDTH), BF16),
                pltpu.VMEM((rows, WIDTH), BF16),
                pltpu.VMEM((PAIRS, groups, share, PAIR_ROWS), BF16),
                pltpu.VMEM((WIDTH, rows), F32),
                pltpu.VMEM((WIDTH, rows), BF16),
                pltpu.VMEM((3, members, FEAT, rows), BF16),
                pltpu.VMEM((members, PAIRS, AUG_ROWS, rows), BF16),
                pltpu.VMEM((1, rows), jnp.int32),
                pltpu.VMEM((members, 1, rows), jnp.int32),
                pltpu.VMEM((2 * HEADS, rows), F32),
                pltpu.VMEM((total, rows), F32),
                pltpu.VMEM((PAIRS, total, 2 * rows), F32),
                pltpu.VMEM((4, FEAT, rows), BF16),
                pltpu.VMEM((2, outer, share, rows), BF16),
                pltpu.VMEM((4, mine, share, rows), BF16),
                pltpu.VMEM((mine, share, 4 * rows), F32),
                pltpu.VMEM((mine, members, unit_rows, LANES), BF16),
                pltpu.VMEM((mine, 2, chips, unit_rows, LANES), BF16),
                pltpu.VMEM((mine, 2, unit_rows, LANES), BF16),
                pltpu.VMEM((outer, unit_rows, LANES), BF16),
                pltpu.VMEM((8, 128), F32),
                pltpu.VMEM((members, 8, 128), F32),
                pltpu.VMEM((8, 128), F32),
                pltpu.VMEM((8, 128), F32),
                pltpu.VMEM((8, 128), F32),
                pltpu.VMEM((outer, 8, 128), F32),
                dma((6,)),
                dma((2 * PAIRS + 1,)),
                dma((2 * PAIRS + 1,)),
                dma((1,)),
                dma((PAIRS // 2,)),
                dma((PAIRS // 2,)),
                dma((1,)),
                dma((1,)),
                dma((2,)),
                dma((1,)),
                dma((1,)),
                dma((1,)),
                dma((mine, 2)),
                dma((1,)),
                dma((1,)),
                dma((4,)),
                dma((4,)),
                pltpu.SemaphoreType.REGULAR((2,)),
            ],
            compiler_params=pltpu.CompilerParams(collective_id=0, has_side_effects=True, vmem_limit_bytes=48000000),
            name="sublayer",
        )(lengths, *[pltpu.with_memory_space_constraint(operand, pltpu.HBM) for operand in operands])
        final = pl.pallas_call(
            functools.partial(scale_kernel, groups * total, total),
            out_shape=(
                jax.ShapeDtypeStruct((FEAT, rows), F32),
                jax.ShapeDtypeStruct((FEAT, rows), F32),
                jax.ShapeDtypeStruct((FEAT, rows), F32),
                jax.ShapeDtypeStruct((features, share), F32),
                jax.ShapeDtypeStruct((1, 1), F32),
            ),
            in_specs=[vmem] * 5,
            out_specs=(vmem,) * 5,
            compiler_params=pltpu.CompilerParams(vmem_limit_bytes=8000000),
            name="scale",
        )(outs[4], *outs[:4])
        return (final[0].T[None], final[1].T[None], final[2].T[None], final[3], final[4].reshape(()))

    placed = (
        P("dp", "patch", None),
        P("dp", "patch", None),
        P("dp", "patch", None),
        P(),
        P("dp", "patch", None),
        P("dp"),
        P("dp", "patch"),
    )
    return jax.shard_map(
        local,
        mesh=mesh,
        in_specs=placed,
        out_specs=(
            P("dp", "patch", None),
            P("dp", "patch", None),
            P("dp", "patch", None),
            P("patch", "dp"),
            P(),
        ),
        check_vma=False,
    )
```

```python
import functools
import math

import jax
import jax.numpy as jnp
from jax import lax
from jax.experimental import pallas as pl
from jax.experimental.pallas import tpu as pltpu
from jax.sharding import PartitionSpec as P

MESH = pl.DeviceIdType.MESH
WIDTH = 1152
HEADS = 8
HEAD_DIM = 72
FEAT = 576
PAIRS = HEADS // 2
PAIR_ROWS = 2 * HEAD_DIM
STAT_ROWS = 16
AUG_ROWS = PAIR_ROWS + STAT_ROWS
LANES = 128
NEG_LARGE = -1e30
F32 = jnp.float32
BF16 = jnp.bfloat16
KEY, VALUE, QUERY = range(3)
G_PARTS = ((0, 3), (3, 1))


def nt(left, right):
    return lax.dot_general(left, right, (((1,), (1,)), ((), ())), preferred_element_type=F32)


def nn(left, right):
    return lax.dot_general(left, right, (((1,), (0,)), ((), ())), preferred_element_type=F32)


def tn(left, right):
    return lax.dot_general(left, right, (((0,), (0,)), ((), ())), preferred_element_type=F32)


def pad16(size):
    return -(-size // 16) * 16


def unit_layout(members, groups):
    share, features = WIDTH // groups, FEAT // members
    main = features // LANES * LANES
    rest = features - main
    main_rows = pad16(share) if main else 0
    tiles = -(-share // LANES)
    return share, features, main, rest, main_rows, tiles, main_rows + tiles * pad16(rest)


def kernel(
    members,
    groups,
    len_ref,
    seg_hbm,
    q_hbm,
    k_hbm,
    v_hbm,
    w_hbm,
    t_hbm,
    dq_ref,
    dk_ref,
    dv_ref,
    dw_ref,
    sum_ref,
    w_ref,
    t_ref,
    wt_ref,
    acc_ref,
    kvq_ref,
    g_ref,
    seg_own,
    seg_all,
    stat_ref,
    bias_ref,
    prob_ref,
    at_ref,
    tt_own,
    tt_all,
    other_ref,
    u_own,
    y_all,
    z_own,
    z_all,
    tile_own,
    tile_all,
    pair_own,
    pair_all,
    sum_own,
    sum_all,
    load_sem,
    far_sem,
    near_sem,
    kvq_send,
    g_far,
    g_near,
    g_send,
    at_send,
    at_recv,
    tt_send,
    tt_recv,
    y_send,
    y_recv,
    z_send,
    z_recv,
    small_send,
    small_recv,
    wave_sem,
):
    rows = q_hbm.shape[1]
    chips = members // 2
    outer = groups // 2
    mine = outer // 2
    share, features, main, rest, main_rows, tiles, unit_rows = unit_layout(members, groups)
    rest_rows = pad16(rest)
    me = lax.axis_index("patch")
    dp = lax.axis_index("dp")
    chip, core = me // 2, me % 2
    step_a, step_b = dp // 2, dp % 2
    partner = chip * 2 + 1 - core
    across = step_a * 2 + 1 - step_b
    slot = step_b * 2 + core
    job = (core + chip) % 2

    def patch_peer(shift):
        return lax.rem(me + shift, members)

    def far(shift):
        return lax.rem(chip + shift, chips)

    def outer_peer(shift):
        return lax.rem(step_a + shift, outer)

    loads = [
        pltpu.make_async_copy(k_hbm, kvq_ref.at[KEY, me], load_sem.at[0]),
        pltpu.make_async_copy(v_hbm, kvq_ref.at[VALUE, me], load_sem.at[1]),
        pltpu.make_async_copy(seg_hbm, seg_own, load_sem.at[2]),
        pltpu.make_async_copy(q_hbm, kvq_ref.at[QUERY, me], load_sem.at[3]),
        pltpu.make_async_copy(w_hbm, w_ref, load_sem.at[4]),
        pltpu.make_async_copy(t_hbm, t_ref, load_sem.at[5]),
    ]
    for load in loads:
        load.start()

    barrier = pltpu.get_barrier_semaphore()

    def greet(dp_index, patch_index):
        pl.semaphore_signal(barrier, inc=1, device_id=(dp_index, patch_index), device_id_type=MESH)

    for shift in range(1, members):
        greet(dp, patch_peer(shift))
    for to in (me, partner):
        greet(across, to)

        @pl.when(step_a > 0)
        def _():
            greet(dp - 2, to)

        @pl.when(step_a < outer - 1)
        def _():
            greet(dp + 2, to)

    edges = (step_a == 0).astype(jnp.int32) + (step_a == outer - 1).astype(jnp.int32)
    greeted = members - 1 + 2 + 2 * (2 - edges)

    def token(device, side):
        pl.semaphore_signal(wave_sem.at[side], inc=1, device_id=(device, me), device_id_type=MESH)

    def wave_start():
        @pl.when(step_a > 0)
        def _():
            token(dp - 2, 1)

        @pl.when(step_a < outer - 1)
        def _():
            token(dp + 2, 0)

    def wave_wait():
        @pl.when(step_a > 0)
        def _():
            pl.semaphore_wait(wave_sem.at[0], 1)

        @pl.when(step_a < outer - 1)
        def _():
            pl.semaphore_wait(wave_sem.at[1], 1)

    def copy(src, dst, send, recv, device):
        return pltpu.make_async_remote_copy(
            src_ref=src, dst_ref=dst, send_sem=send, recv_sem=recv, device_id=device, device_id_type=MESH
        )

    def received(ref, recv):
        copy(ref, ref, small_send.at[0], recv, (dp, partner)).wait_recv()

    def sent(ref, send):
        copy(ref, ref, send, small_recv.at[0], (dp, partner)).wait_send()

    def rows_of(pair):
        return pl.ds(PAIR_ROWS * pair, PAIR_ROWS)

    def kvq_part(array, owner, pair):
        if array == QUERY:
            return kvq_ref.at[array, owner]
        return kvq_ref.at[array, owner, rows_of(pair)]

    def kvq_index(array, pair):
        return 2 * PAIRS if array == QUERY else PAIRS * array + pair

    def spread(part, index, send, away, near):
        for shift in range(1, chips):
            copy(part, part, send, away.at[index], (dp, far(shift) * 2 + 1 - core)).start()
        copy(part, part, send, near.at[index], (dp, partner)).start()

    def relay_parts(part_at, span_at, index, send, away, near):
        received(part_at(far(1) * 2 + 1 - core) if chips == 2 else span_at(chips - 1), away.at[index])
        for shift in range(1, chips):
            part = part_at(far(shift) * 2 + 1 - core)
            copy(part, part, send, near.at[index], (dp, partner)).start()

    def kvq_span(array, pair, count):
        if array == QUERY:
            return kvq_ref.at[array, pl.ds(0, count)]
        return kvq_ref.at[array, pl.ds(0, count), rows_of(pair)]

    def kvq_spread(array, pair=0):
        spread(kvq_part(array, me, pair), kvq_index(array, pair), kvq_send.at[0], far_sem, near_sem)

    def kvq_relay(array, pair=0):
        relay_parts(
            lambda owner: kvq_part(array, owner, pair),
            lambda count: kvq_span(array, pair, count),
            kvq_index(array, pair),
            kvq_send.at[0],
            far_sem,
            near_sem,
        )

    def kvq_finish(array, pair=0):
        received(kvq_span(array, pair, chips), near_sem.at[kvq_index(array, pair)])

    def g_part(owner, part):
        return g_ref.at[owner, pl.ds(*G_PARTS[part])]

    def g_span(part, count):
        return g_ref.at[pl.ds(0, count), pl.ds(*G_PARTS[part])]

    def g_spread(part):
        spread(g_part(me, part), part, g_send.at[0], g_far, g_near)

    def g_relay(part):
        relay_parts(
            lambda owner: g_part(owner, part),
            lambda count: g_span(part, count),
            part,
            g_send.at[0],
            g_far,
            g_near,
        )

    def g_finish(part):
        received(g_span(part, chips), g_near.at[part])

    def small(index, own_ref, everyone):
        for shift in range(1, members):
            copy(own_ref, everyone.at[me], small_send.at[index], small_recv.at[index], (dp, patch_peer(shift))).start()

    loads[0].wait()
    pl.semaphore_wait(barrier, greeted)
    kvq_spread(KEY, 0)
    loads[2].wait()
    small(0, seg_own, seg_all)
    loads[1].wait()
    kvq_spread(VALUE, 0)
    for pair in range(1, PAIRS):
        kvq_spread(KEY, pair)
        kvq_spread(VALUE, pair)
    loads[3].wait()
    kvq_spread(QUERY)
    wave_start()
    seg_all[me] = seg_own[...]

    upper = lax.broadcasted_iota(jnp.int32, (PAIR_ROWS, 1), 0) < HEAD_DIM
    masks = [upper.astype(F32).astype(BF16), jnp.logical_not(upper).astype(F32).astype(BF16)]

    def stacked(value):
        return jnp.concatenate([value * masks[0], value * masks[1]], axis=1)

    def merged(value):
        return jnp.concatenate([value[:HEAD_DIM, :rows], value[HEAD_DIM:, rows:]], axis=0)

    def own(array, pair):
        return kvq_ref[array, me, PAIR_ROWS * pair : PAIR_ROWS * (pair + 1), :]

    def whole(array, pair):
        low = PAIR_ROWS * pair
        return jnp.concatenate([kvq_ref[array, j, low : low + PAIR_ROWS, :] for j in range(members)], axis=1)

    stat_row = lax.broadcasted_iota(jnp.int32, (STAT_ROWS, 2 * rows), 0)
    stat_side = (lax.broadcasted_iota(jnp.int32, (STAT_ROWS, 2 * rows), 1) >= rows).astype(jnp.int32)

    def picker(base):
        low = base + 3 * stat_side
        return jnp.where((stat_row >= low) & (stat_row < low + 3), -1.0, 0.0).astype(BF16)

    norm_picker, delta_picker = picker(0), picker(6)

    loads[5].wait()
    target = t_ref[...].astype(F32).T
    acc_ref[...] = -target
    for z in range(outer):
        for side in (0, 1):
            low = (z * 2 + side) * share
            tt_own[side, z] = target[low : low + share].astype(BF16)
    peers = ((1 - step_b, core), (1 - step_b, 1 - core), (step_b, 1 - core))
    for side, to in peers:
        copy(
            tt_own.at[side, pl.ds((to + chip) % 2 * mine, mine)],
            tt_all.at[slot],
            tt_send.at[0],
            tt_recv.at[0],
            (step_a * 2 + side, chip * 2 + to),
        ).start()
    for i in range(mine):
        tt_all[slot, i] = tt_own[step_b, job * mine + i]
    loads[4].wait()
    for pair in range(PAIRS):
        turned = w_ref[PAIR_ROWS * pair : PAIR_ROWS * (pair + 1), :].astype(F32).T
        for block in range(groups):
            wt_ref[pair, block] = turned[block * share : (block + 1) * share].astype(BF16)
    u_own[:, :, main_rows:, :] = jnp.zeros((mine, members, unit_rows - main_rows, LANES), BF16)

    length = len_ref[0]
    lane_position = lax.broadcasted_iota(jnp.int32, (1, rows), 1)
    own_live = me * rows + lane_position < length
    own_group = jnp.where(own_live, seg_own[...], -1).astype(F32)
    kvq_relay(KEY, 0)
    received(seg_all.at[pl.ds(0, members - 1)], small_recv.at[0])
    for j in range(members):
        group = jnp.where(j * rows + lane_position < length, seg_all[j], -1).astype(F32)
        group = jnp.broadcast_to(group, (rows, rows)).T
        bias_ref[j * rows : (j + 1) * rows, :] = jnp.where(group == own_group, 0.0, NEG_LARGE)

    log_scale = math.log2(math.e) / math.sqrt(HEAD_DIM)
    score_scale = 1.0 / math.sqrt(HEAD_DIM)

    def biased(scores):
        bias = bias_ref[...]
        return scores * log_scale + jnp.concatenate([bias, bias], axis=1)

    def projected(pair):
        attn_pair = at_ref[slot, PAIR_ROWS * pair : PAIR_ROWS * (pair + 1), :]
        if share % 16 == 0:
            return nn(wt_ref[pair].reshape(WIDTH, PAIR_ROWS), attn_pair)
        return jnp.concatenate([nn(wt_ref[pair, block], attn_pair) for block in range(groups)], axis=0)

    inverses = []
    for pair in range(PAIRS):
        kvq_relay(VALUE, pair)
        kvq_finish(KEY, pair)
        scores = biased(tn(whole(KEY, pair), stacked(own(QUERY, pair))))
        row_max = jnp.max(scores, axis=0, keepdims=True)
        probs = jnp.exp2(scores - row_max)
        denom = jnp.sum(probs, axis=0, keepdims=True)
        prob_ref[pair] = probs
        log_norm = (row_max + jnp.log2(denom)) * (1.0 / log_scale)
        for side in (0, 1):
            head = 2 * pair + side
            stat_ref[head : head + 1, :] = log_norm[:, side * rows : (side + 1) * rows]
        inverse = 1.0 / denom
        inverses.append(inverse)
        if pair + 1 < PAIRS:
            kvq_relay(KEY, pair + 1)
        if pair:
            acc_ref[...] += projected(pair - 1)
        kvq_finish(VALUE, pair)
        accum = nn(whole(VALUE, pair), probs.astype(BF16)) * inverse
        attn_pair = jnp.where(own_live, merged(accum), 0.0).astype(BF16)
        at_ref[slot, PAIR_ROWS * pair : PAIR_ROWS * (pair + 1), :] = attn_pair
        part = at_ref.at[slot, rows_of(pair)]
        arrival = at_recv.at[pair // (PAIRS - 1)]
        for to in (chip * 2 + chip % 2, chip * 2 + 1 - chip % 2):
            copy(part, part, at_send.at[0], arrival, (across, to)).start()
        copy(part, part, at_send.at[0], arrival, (dp, partner)).start()
        if pair == 1 and outer > 2:
            wave_wait()
            if outer > 3:
                wave_start()

    error = jnp.where(own_live, acc_ref[...] + projected(PAIRS - 1), 0.0)
    dout = (2.0 * error).astype(BF16)
    loss_part = jnp.sum(jnp.sum(error * error, axis=0, keepdims=True), axis=1, keepdims=True)
    tile_own[...] = jnp.broadcast_to(loss_part, tile_own.shape)
    small(1, tile_own, tile_all)
    tile_all[me] = tile_own[...]

    def terms(value):
        first = value.astype(BF16).astype(F32)
        second = (value - first).astype(BF16).astype(F32)
        return [first, second, value - first - second]

    for pair in range(PAIRS):
        grad = nn(w_ref[PAIR_ROWS * pair : PAIR_ROWS * (pair + 1), :], dout).astype(BF16)
        g_ref[me, pair, :PAIR_ROWS, :] = grad
        product = grad.astype(F32) * at_ref[slot, PAIR_ROWS * pair : PAIR_ROWS * (pair + 1), :].astype(F32)
        lines = []
        for side in (0, 1):
            lines += terms(stat_ref[2 * pair + side : 2 * pair + side + 1, :])
        for side in (0, 1):
            head = 2 * pair + side
            delta = jnp.sum(product[HEAD_DIM * side : HEAD_DIM * (side + 1)], axis=0, keepdims=True)
            stat_ref[HEADS + head : HEADS + head + 1, :] = delta
            lines += terms(delta)
        lines.append(jnp.zeros((STAT_ROWS - 12, rows), F32))
        g_ref[me, pair, PAIR_ROWS:, :] = jnp.concatenate(lines, axis=0).astype(BF16)
    g_spread(0)

    def query_pass(pair):
        low = HEADS + 2 * pair
        delta = jnp.concatenate([stat_ref[low : low + 1, :], stat_ref[low + 1 : low + 2, :]], axis=1)
        grad = g_ref[me, pair, :PAIR_ROWS, :]
        dprobs = tn(whole(VALUE, pair), stacked(grad))
        dscores = prob_ref[pair] * inverses[pair] * (dprobs - delta)
        value = nn(whole(KEY, pair), dscores.astype(BF16))
        dq_ref[PAIR_ROWS * pair : PAIR_ROWS * (pair + 1), :] = merged(value) * score_scale

    def key_pass(pair):
        if pair in (0, 3):
            g_finish(pair // 3)
        queries = whole(QUERY, pair)
        grads = jnp.concatenate([g_ref[j, pair] for j in range(members)], axis=1)
        stats = grads[PAIR_ROWS:]
        scores = tn(
            jnp.concatenate([queries, stats], axis=0),
            jnp.concatenate([stacked(own(KEY, pair)), norm_picker], axis=0),
        )
        probs = jnp.exp2(biased(scores))
        dv_ref[PAIR_ROWS * pair : PAIR_ROWS * (pair + 1), :] = merged(nn(grads[:PAIR_ROWS], probs.astype(BF16)))
        dprobs = tn(grads, jnp.concatenate([stacked(own(VALUE, pair)), delta_picker], axis=0))
        dscores = (probs * dprobs).astype(BF16)
        dk_ref[PAIR_ROWS * pair : PAIR_ROWS * (pair + 1), :] = merged(nn(queries, dscores)) * score_scale

    def attention(pair):
        low = PAIR_ROWS * pair
        return jnp.concatenate([at_ref[s, low : low + PAIR_ROWS, :] for s in range(4)], axis=1)

    def weight_start():
        received(tt_all.at[pl.ds(0, 3)], tt_recv.at[0])
        received(at_ref.at[pl.ds(0, 3), pl.ds(0, FEAT - PAIR_ROWS)], at_recv.at[0])
        for i in range(mine):
            block = (job * mine + i) * 2 + step_b
            value = -jnp.concatenate([tt_all[s, i].astype(F32) for s in range(4)], axis=1)
            for pair in range(PAIRS - 1):
                value = value + nn(wt_ref[pair, block], attention(pair))
            other_ref[i] = value

    def weight_blocks(away, blocks, grads, attn, span):
        if main:
            attn_main = jnp.concatenate([attn[p * features : p * features + main] for p in range(span)], axis=0)
            attn_rest = jnp.concatenate([attn[p * features + main : (p + 1) * features] for p in range(span)], axis=0)
            part_main = nt(grads, attn_main).astype(BF16)
        else:
            attn_rest = attn
        part_rest = nt(attn_rest, grads)
        for place, i in enumerate(blocks):
            for p in range(span):
                if main:
                    u_own[i, away + p, :share, :] = part_main[place * share : (place + 1) * share, p * main : (p + 1) * main]
                for t in range(tiles):
                    wide = min(share - t * LANES, LANES)
                    first = place * share + t * LANES
                    low = main_rows + t * rest_rows
                    piece = part_rest[p * rest : (p + 1) * rest, first : first + wide]
                    u_own[i, away + p, low : low + rest, :wide] = piece.astype(BF16)

    def weight_part():
        received(at_ref.at[pl.ds(0, 3), rows_of(PAIRS - 1)], at_recv.at[1])
        last = attention(PAIRS - 1)

        def grads_of(i):
            block = (job * mine + i) * 2 + step_b
            return (2.0 * (other_ref[i] + nn(wt_ref[PAIRS - 1, block], last))).astype(BF16)

        def send(i, shift):
            away = far(shift)
            for to in (0, 1):
                copy(
                    u_own.at[i, away * 2 + to],
                    y_all.at[i, to, chip],
                    y_send.at[0],
                    y_recv.at[i, to],
                    (dp, away * 2 + (job + away) % 2),
                ).start()

        if share % 16 == 0 and features % 16 == 0:

            def attn_of(shift):
                low = pl.multiple_of(far(shift) * 2 * features, 16)
                return jnp.concatenate([at_ref[s, pl.ds(low, 2 * features), :] for s in range(4)], axis=1)

            grads = []
            for i in range(mine):
                grads.append(grads_of(i))
                for shift in range(1, chips):
                    weight_blocks(far(shift) * 2, [i], grads[i], attn_of(shift), 2)
                    send(i, shift)
            weight_blocks(chip * 2, range(mine), jnp.concatenate(grads, axis=0), attn_of(0), 2)
        else:
            attn = jnp.concatenate([at_ref[s] for s in range(4)], axis=1)
            for i in range(mine):
                weight_blocks(0, [i], grads_of(i), attn, members)
                for shift in range(1, chips):
                    send(i, shift)

    def weight_sum(i, to):
        received(y_all.at[i, to, pl.ds(0, chips - 1)], y_recv.at[i, to])
        value = u_own[i, chip * 2 + to].astype(F32)
        for shift in range(1, chips):
            value = value + y_all[i, to, far(shift)].astype(F32)
        z_own[i, to] = value.astype(BF16)
        owner = job * mine + i
        stays = jnp.logical_and(owner == step_a, core == to)

        @pl.when(stays)
        def _():
            z_all[step_a] = z_own[i, to]

        @pl.when(jnp.logical_not(stays))
        def _():
            copy(
                z_own.at[i, to],
                z_all.at[step_a],
                z_send.at[0],
                z_recv.at[0],
                (owner * 2 + step_b, chip * 2 + to),
            ).start()

    for hops in range(4, outer + 1):
        wave_wait()
        if hops < outer:
            wave_start()
    kvq_relay(QUERY)
    query_pass(0)
    weight_start()
    query_pass(1)
    received(tile_all.at[pl.ds(0, members - 1)], small_recv.at[1])
    pack_loss = tile_all[0]
    for j in range(1, members):
        pack_loss = pack_loss + tile_all[j]
    tile_lane = lax.broadcasted_iota(jnp.int32, pack_loss.shape, 1)
    pair_own[...] = jnp.where(tile_lane == 0, pack_loss, length.astype(F32))
    copy(pair_own, pair_all, small_send.at[3], small_recv.at[3], (across, me)).start()
    pl.when(job == 1)(functools.partial(g_spread, 1))
    weight_part()
    pl.when(job == 0)(functools.partial(g_spread, 1))
    query_pass(2)
    query_pass(3)
    g_relay(0)
    received(pair_all, small_recv.at[3])
    sum_own[...] = pair_own[...] + pair_all[...]
    for shift in range(1, outer):
        to = outer_peer(shift) * 2 + step_b
        copy(sum_own, sum_all.at[step_a], small_send.at[2], small_recv.at[2], (to, me)).start()
    sum_all[step_a] = sum_own[...]
    kvq_finish(QUERY)
    units = [(i, to) for i in range(mine) for to in (0, 1)]
    quarter = len(units) // 4
    parts = [units[quarter * k : quarter * (k + 1)] for k in range(4)]

    def weight_sums(early, late):
        for which, chosen in ((0, early), (1, late)):
            if chosen:

                @pl.when(job == which)
                def _():
                    for i, to in chosen:
                        weight_sum(i, to)

    weight_sums(parts[0] + parts[1], [])
    key_pass(0)
    weight_sums(parts[2], [])
    pl.when(job == 1)(functools.partial(g_relay, 1))
    key_pass(1)
    weight_sums(parts[3], parts[0])
    pl.when(job == 0)(functools.partial(g_relay, 1))
    key_pass(2)
    weight_sums([], parts[1] + parts[2] + parts[3])
    key_pass(3)

    received(sum_all.at[pl.ds(0, outer - 1)], small_recv.at[2])
    totals = sum_all[0]
    for j in range(1, outer):
        totals = totals + sum_all[j]
    sum_ref[...] = totals

    sent(kvq_ref.at[:, pl.ds(0, members - 1)], kvq_send.at[0])
    sent(g_ref.at[pl.ds(0, members - 1)], g_send.at[0])
    sent(at_ref.at[pl.ds(0, 3)], at_send.at[0])
    sent(tt_all.at[pl.ds(0, 3)], tt_send.at[0])
    sent(y_all.at[:, :, pl.ds(0, chips - 1)], y_send.at[0])
    sent(seg_all.at[pl.ds(0, members - 1)], small_send.at[0])
    sent(tile_all.at[pl.ds(0, members - 1)], small_send.at[1])
    sent(sum_all.at[pl.ds(0, outer - 1)], small_send.at[2])
    sent(pair_all, small_send.at[3])

    collects = job == step_a // mine

    @pl.when(collects)
    def _():
        sent(z_all.at[pl.ds(0, outer - 1)], z_send.at[0])
        received(z_all.at[pl.ds(0, outer - 1)], z_recv.at[0])

    @pl.when(jnp.logical_not(collects))
    def _():
        sent(z_all, z_send.at[0])
        received(z_all, z_recv.at[0])

    summed = z_all[0].astype(F32)
    for j in range(1, outer):
        summed = summed + z_all[j].astype(F32)
    if main:
        dw_ref[:main, :] = summed[:share].T
    for t in range(tiles):
        wide = min(share - t * LANES, LANES)
        low = main_rows + t * rest_rows
        dw_ref[main:, t * LANES : t * LANES + wide] = summed[low : low + rest, :wide]


def scale_kernel(slots, total, sum_ref, dq_ref, dk_ref, dv_ref, dw_ref, query_ref, key_ref, value_ref, weight_ref, loss_ref):
    count = sum_ref[0:1, 1:2]
    ratio = slots / count
    query_ref[...] = dq_ref[...] * ratio
    key_ref[...] = dk_ref[...] * ratio
    value_ref[...] = dv_ref[...] * ratio
    weight_ref[...] = dw_ref[...] * (ratio / total)
    loss_ref[...] = sum_ref[0:1, 0:1] / (count * WIDTH)


def solution(mesh):
    members, groups = mesh.shape["patch"], mesh.shape["dp"]

    def local(query_rows, key_rows, value_rows, out_weight, target, lengths, segments):
        rows = query_rows.shape[1]
        total = rows * members
        chips = members // 2
        outer = groups // 2
        mine = outer // 2
        share, features, main, rest, main_rows, tiles, unit_rows = unit_layout(members, groups)
        vmem = pl.BlockSpec(memory_space=pltpu.VMEM)
        hbm = pl.BlockSpec(memory_space=pltpu.HBM)
        dma = pltpu.SemaphoreType.DMA
        operands = (
            segments,
            query_rows[0].T,
            key_rows[0].T,
            value_rows[0].T,
            out_weight,
            target[0],
        )
        outs = pl.pallas_call(
            functools.partial(kernel, members, groups),
            out_shape=(
                jax.ShapeDtypeStruct((FEAT, rows), F32),
                jax.ShapeDtypeStruct((FEAT, rows), F32),
                jax.ShapeDtypeStruct((FEAT, rows), F32),
                jax.ShapeDtypeStruct((features, share), F32),
                jax.ShapeDtypeStruct((8, 128), F32),
            ),
            in_specs=[pl.BlockSpec(memory_space=pltpu.SMEM)] + [hbm] * 6,
            out_specs=(vmem,) * 5,
            scratch_shapes=[
                pltpu.VMEM((FEAT, WIDTH), BF16),
                pltpu.VMEM((rows, WIDTH), BF16),
                pltpu.VMEM((PAIRS, groups, share, PAIR_ROWS), BF16),
                pltpu.VMEM((WIDTH, rows), F32),
                pltpu.VMEM((3, members, FEAT, rows), BF16),
                pltpu.VMEM((members, PAIRS, AUG_ROWS, rows), BF16),
                pltpu.VMEM((1, rows), jnp.int32),
                pltpu.VMEM((members, 1, rows), jnp.int32),
                pltpu.VMEM((2 * HEADS, rows), F32),
                pltpu.VMEM((total, rows), F32),
                pltpu.VMEM((PAIRS, total, 2 * rows), F32),
                pltpu.VMEM((4, FEAT, rows), BF16),
                pltpu.VMEM((2, outer, share, rows), BF16),
                pltpu.VMEM((4, mine, share, rows), BF16),
                pltpu.VMEM((mine, share, 4 * rows), F32),
                pltpu.VMEM((mine, members, unit_rows, LANES), BF16),
                pltpu.VMEM((mine, 2, chips, unit_rows, LANES), BF16),
                pltpu.VMEM((mine, 2, unit_rows, LANES), BF16),
                pltpu.VMEM((outer, unit_rows, LANES), BF16),
                pltpu.VMEM((8, 128), F32),
                pltpu.VMEM((members, 8, 128), F32),
                pltpu.VMEM((8, 128), F32),
                pltpu.VMEM((8, 128), F32),
                pltpu.VMEM((8, 128), F32),
                pltpu.VMEM((outer, 8, 128), F32),
                dma((6,)),
                dma((2 * PAIRS + 1,)),
                dma((2 * PAIRS + 1,)),
                dma((1,)),
                dma((PAIRS // 2,)),
                dma((PAIRS // 2,)),
                dma((1,)),
                dma((1,)),
                dma((2,)),
                dma((1,)),
                dma((1,)),
                dma((1,)),
                dma((mine, 2)),
                dma((1,)),
                dma((1,)),
                dma((4,)),
                dma((4,)),
                pltpu.SemaphoreType.REGULAR((2,)),
            ],
            compiler_params=pltpu.CompilerParams(collective_id=0, has_side_effects=True, vmem_limit_bytes=48000000),
            name="sublayer",
        )(lengths, *[pltpu.with_memory_space_constraint(operand, pltpu.HBM) for operand in operands])
        final = pl.pallas_call(
            functools.partial(scale_kernel, groups * total, total),
            out_shape=(
                jax.ShapeDtypeStruct((FEAT, rows), F32),
                jax.ShapeDtypeStruct((FEAT, rows), F32),
                jax.ShapeDtypeStruct((FEAT, rows), F32),
                jax.ShapeDtypeStruct((features, share), F32),
                jax.ShapeDtypeStruct((1, 1), F32),
            ),
            in_specs=[vmem] * 5,
            out_specs=(vmem,) * 5,
            compiler_params=pltpu.CompilerParams(vmem_limit_bytes=8000000),
            name="scale",
        )(outs[4], *outs[:4])
        return (final[0].T[None], final[1].T[None], final[2].T[None], final[3], final[4].reshape(()))

    placed = (
        P("dp", "patch", None),
        P("dp", "patch", None),
        P("dp", "patch", None),
        P(),
        P("dp", "patch", None),
        P("dp"),
        P("dp", "patch"),
    )
    return jax.shard_map(
        local,
        mesh=mesh,
        in_specs=placed,
        out_specs=(
            P("dp", "patch", None),
            P("dp", "patch", None),
            P("dp", "patch", None),
            P("patch", "dp"),
            P(),
        ),
        check_vma=False,
    )
```

```python
import functools
import math

import jax
import jax.numpy as jnp
from jax import lax
from jax.experimental import pallas as pl
from jax.experimental.pallas import tpu as pltpu
from jax.sharding import PartitionSpec as P

MESH = pl.DeviceIdType.MESH
WIDTH = 1152
HEADS = 8
HEAD_DIM = 72
FEAT = 576
PAIRS = HEADS // 2
PAIR_ROWS = 2 * HEAD_DIM
STAT_ROWS = 16
AUG_ROWS = PAIR_ROWS + STAT_ROWS
LANES = 128
NEG_LARGE = -1e30
F32 = jnp.float32
BF16 = jnp.bfloat16
KEY, VALUE, QUERY = range(3)
G_PARTS = ((0, 3), (3, 1))


def nt(left, right):
    return lax.dot_general(left, right, (((1,), (1,)), ((), ())), preferred_element_type=F32)


def nn(left, right):
    return lax.dot_general(left, right, (((1,), (0,)), ((), ())), preferred_element_type=F32)


def tn(left, right):
    return lax.dot_general(left, right, (((0,), (0,)), ((), ())), preferred_element_type=F32)


def pad16(size):
    return -(-size // 16) * 16


def unit_layout(members, groups):
    share, features = WIDTH // groups, FEAT // members
    main = features // LANES * LANES
    rest = features - main
    main_rows = pad16(share) if main else 0
    tiles = -(-share // LANES)
    return share, features, main, rest, main_rows, tiles, main_rows + tiles * pad16(rest)


def kernel(
    members,
    groups,
    len_ref,
    seg_hbm,
    q_hbm,
    k_hbm,
    v_hbm,
    w_hbm,
    t_hbm,
    dq_ref,
    dk_ref,
    dv_ref,
    dw_ref,
    sum_ref,
    w_ref,
    t_ref,
    wt_ref,
    acc_ref,
    kvq_ref,
    g_ref,
    seg_own,
    seg_all,
    stat_ref,
    bias_ref,
    prob_ref,
    at_ref,
    tt_own,
    tt_all,
    other_ref,
    u_own,
    y_all,
    z_own,
    z_all,
    zb_all,
    yb_own,
    yb_all,
    tile_own,
    tile_all,
    pair_own,
    pair_all,
    sum_own,
    sum_all,
    load_sem,
    far_sem,
    near_sem,
    kvq_send,
    g_far,
    g_near,
    g_send,
    at_send,
    at_recv,
    tt_send,
    tt_recv,
    y_send,
    y_recv,
    z_send,
    z_recv,
    small_send,
    small_recv,
    wave_sem,
    turn_send,
    turn_recv,
):
    rows = q_hbm.shape[1]
    chips = members // 2
    outer = groups // 2
    mine = outer // 2
    share, features, main, rest, main_rows, tiles, unit_rows = unit_layout(members, groups)
    rest_rows = pad16(rest)
    me = lax.axis_index("patch")
    dp = lax.axis_index("dp")
    chip, core = me // 2, me % 2
    step_a, step_b = dp // 2, dp % 2
    partner = chip * 2 + 1 - core
    across = step_a * 2 + 1 - step_b
    slot = step_b * 2 + core
    job = (core + chip) % 2
    detour = chips == 2
    turn_owner = job * mine
    ends_turn = step_a % mine == 0

    def patch_peer(shift):
        return lax.rem(me + shift, members)

    def far(shift):
        return lax.rem(chip + shift, chips)

    def outer_peer(shift):
        return lax.rem(step_a + shift, outer)

    loads = [
        pltpu.make_async_copy(k_hbm, kvq_ref.at[KEY, me], load_sem.at[0]),
        pltpu.make_async_copy(v_hbm, kvq_ref.at[VALUE, me], load_sem.at[1]),
        pltpu.make_async_copy(seg_hbm, seg_own, load_sem.at[2]),
        pltpu.make_async_copy(q_hbm, kvq_ref.at[QUERY, me], load_sem.at[3]),
        pltpu.make_async_copy(w_hbm, w_ref, load_sem.at[4]),
        pltpu.make_async_copy(t_hbm, t_ref, load_sem.at[5]),
    ]
    for load in loads:
        load.start()

    barrier = pltpu.get_barrier_semaphore()

    def greet(dp_index, patch_index):
        pl.semaphore_signal(barrier, inc=1, device_id=(dp_index, patch_index), device_id_type=MESH)

    for shift in range(1, members):
        greet(dp, patch_peer(shift))
    for to in (me, partner):
        greet(across, to)

        @pl.when(step_a > 0)
        def _():
            greet(dp - 2, to)

        @pl.when(step_a < outer - 1)
        def _():
            greet(dp + 2, to)

    edges = (step_a == 0).astype(jnp.int32) + (step_a == outer - 1).astype(jnp.int32)
    greeted = members - 1 + 2 + 2 * (2 - edges)

    def token(device, side):
        pl.semaphore_signal(wave_sem.at[side], inc=1, device_id=(device, me), device_id_type=MESH)

    def wave_start():
        @pl.when(step_a > 0)
        def _():
            token(dp - 2, 1)

        @pl.when(step_a < outer - 1)
        def _():
            token(dp + 2, 0)

    def wave_wait():
        @pl.when(step_a > 0)
        def _():
            pl.semaphore_wait(wave_sem.at[0], 1)

        @pl.when(step_a < outer - 1)
        def _():
            pl.semaphore_wait(wave_sem.at[1], 1)

    def copy(src, dst, send, recv, device):
        return pltpu.make_async_remote_copy(
            src_ref=src, dst_ref=dst, send_sem=send, recv_sem=recv, device_id=device, device_id_type=MESH
        )

    def received(ref, recv):
        copy(ref, ref, small_send.at[0], recv, (dp, partner)).wait_recv()

    def sent(ref, send):
        copy(ref, ref, send, small_recv.at[0], (dp, partner)).wait_send()

    def rows_of(pair):
        return pl.ds(PAIR_ROWS * pair, PAIR_ROWS)

    def kvq_part(array, owner, pair):
        if array == QUERY:
            return kvq_ref.at[array, owner]
        return kvq_ref.at[array, owner, rows_of(pair)]

    def kvq_index(array, pair):
        return 2 * PAIRS if array == QUERY else PAIRS * array + pair

    def spread(part, index, send, away, near):
        for shift in range(1, chips):
            copy(part, part, send, away.at[index], (dp, far(shift) * 2 + 1 - core)).start()
        copy(part, part, send, near.at[index], (dp, partner)).start()

    def relay_parts(part_at, span_at, index, send, away, near):
        received(part_at(far(1) * 2 + 1 - core) if chips == 2 else span_at(chips - 1), away.at[index])
        for shift in range(1, chips):
            part = part_at(far(shift) * 2 + 1 - core)
            copy(part, part, send, near.at[index], (dp, partner)).start()

    def kvq_span(array, pair, count):
        if array == QUERY:
            return kvq_ref.at[array, pl.ds(0, count)]
        return kvq_ref.at[array, pl.ds(0, count), rows_of(pair)]

    def kvq_spread(array, pair=0):
        spread(kvq_part(array, me, pair), kvq_index(array, pair), kvq_send.at[0], far_sem, near_sem)

    def kvq_relay(array, pair=0):
        relay_parts(
            lambda owner: kvq_part(array, owner, pair),
            lambda count: kvq_span(array, pair, count),
            kvq_index(array, pair),
            kvq_send.at[0],
            far_sem,
            near_sem,
        )

    def kvq_finish(array, pair=0):
        received(kvq_span(array, pair, chips), near_sem.at[kvq_index(array, pair)])

    def g_part(owner, part):
        return g_ref.at[owner, pl.ds(*G_PARTS[part])]

    def g_span(part, count):
        return g_ref.at[pl.ds(0, count), pl.ds(*G_PARTS[part])]

    def g_spread(part):
        spread(g_part(me, part), part, g_send.at[0], g_far, g_near)

    def g_relay(part):
        relay_parts(
            lambda owner: g_part(owner, part),
            lambda count: g_span(part, count),
            part,
            g_send.at[0],
            g_far,
            g_near,
        )

    def g_finish(part):
        received(g_span(part, chips), g_near.at[part])

    def small(index, own_ref, everyone):
        for shift in range(1, members):
            copy(own_ref, everyone.at[me], small_send.at[index], small_recv.at[index], (dp, patch_peer(shift))).start()

    loads[0].wait()
    pl.semaphore_wait(barrier, greeted)
    kvq_spread(KEY, 0)
    loads[2].wait()
    small(0, seg_own, seg_all)
    loads[1].wait()
    kvq_spread(VALUE, 0)
    for pair in range(1, PAIRS):
        kvq_spread(KEY, pair)
        kvq_spread(VALUE, pair)
    loads[3].wait()
    kvq_spread(QUERY)
    wave_start()
    seg_all[me] = seg_own[...]

    upper = lax.broadcasted_iota(jnp.int32, (PAIR_ROWS, 1), 0) < HEAD_DIM
    masks = [upper.astype(F32).astype(BF16), jnp.logical_not(upper).astype(F32).astype(BF16)]

    def stacked(value):
        return jnp.concatenate([value * masks[0], value * masks[1]], axis=1)

    def merged(value):
        return jnp.concatenate([value[:HEAD_DIM, :rows], value[HEAD_DIM:, rows:]], axis=0)

    def own(array, pair):
        return kvq_ref[array, me, PAIR_ROWS * pair : PAIR_ROWS * (pair + 1), :]

    def whole(array, pair):
        low = PAIR_ROWS * pair
        return jnp.concatenate([kvq_ref[array, j, low : low + PAIR_ROWS, :] for j in range(members)], axis=1)

    stat_row = lax.broadcasted_iota(jnp.int32, (STAT_ROWS, 2 * rows), 0)
    stat_side = (lax.broadcasted_iota(jnp.int32, (STAT_ROWS, 2 * rows), 1) >= rows).astype(jnp.int32)

    def picker(base):
        low = base + 3 * stat_side
        return jnp.where((stat_row >= low) & (stat_row < low + 3), -1.0, 0.0).astype(BF16)

    norm_picker, delta_picker = picker(0), picker(6)

    loads[5].wait()
    target = t_ref[...].astype(F32).T
    acc_ref[...] = -target
    for z in range(outer):
        for side in (0, 1):
            low = (z * 2 + side) * share
            tt_own[side, z] = target[low : low + share].astype(BF16)
    peers = ((1 - step_b, core), (1 - step_b, 1 - core), (step_b, 1 - core))
    for side, to in peers:
        copy(
            tt_own.at[side, pl.ds((to + chip) % 2 * mine, mine)],
            tt_all.at[slot],
            tt_send.at[0],
            tt_recv.at[0],
            (step_a * 2 + side, chip * 2 + to),
        ).start()
    for i in range(mine):
        tt_all[slot, i] = tt_own[step_b, job * mine + i]
    loads[4].wait()
    for pair in range(PAIRS):
        turned = w_ref[PAIR_ROWS * pair : PAIR_ROWS * (pair + 1), :].astype(F32).T
        for block in range(groups):
            wt_ref[pair, block] = turned[block * share : (block + 1) * share].astype(BF16)
    u_own[:, :, main_rows:, :] = jnp.zeros((mine, members, unit_rows - main_rows, LANES), BF16)

    length = len_ref[0]
    lane_position = lax.broadcasted_iota(jnp.int32, (1, rows), 1)
    own_live = me * rows + lane_position < length
    own_group = jnp.where(own_live, seg_own[...], -1).astype(F32)
    kvq_relay(KEY, 0)
    received(seg_all.at[pl.ds(0, members - 1)], small_recv.at[0])
    for j in range(members):
        group = jnp.where(j * rows + lane_position < length, seg_all[j], -1).astype(F32)
        group = jnp.broadcast_to(group, (rows, rows)).T
        bias_ref[j * rows : (j + 1) * rows, :] = jnp.where(group == own_group, 0.0, NEG_LARGE)

    log_scale = math.log2(math.e) / math.sqrt(HEAD_DIM)
    score_scale = 1.0 / math.sqrt(HEAD_DIM)

    def biased(scores):
        bias = bias_ref[...]
        return scores * log_scale + jnp.concatenate([bias, bias], axis=1)

    def projected(pair):
        attn_pair = at_ref[slot, PAIR_ROWS * pair : PAIR_ROWS * (pair + 1), :]
        if share % 16 == 0:
            return nn(wt_ref[pair].reshape(WIDTH, PAIR_ROWS), attn_pair)
        return jnp.concatenate([nn(wt_ref[pair, block], attn_pair) for block in range(groups)], axis=0)

    inverses = []
    for pair in range(PAIRS):
        kvq_relay(VALUE, pair)
        kvq_finish(KEY, pair)
        scores = biased(tn(whole(KEY, pair), stacked(own(QUERY, pair))))
        row_max = jnp.max(scores, axis=0, keepdims=True)
        probs = jnp.exp2(scores - row_max)
        denom = jnp.sum(probs, axis=0, keepdims=True)
        prob_ref[pair] = probs
        log_norm = (row_max + jnp.log2(denom)) * (1.0 / log_scale)
        for side in (0, 1):
            head = 2 * pair + side
            stat_ref[head : head + 1, :] = log_norm[:, side * rows : (side + 1) * rows]
        inverse = 1.0 / denom
        inverses.append(inverse)
        if pair + 1 < PAIRS:
            kvq_relay(KEY, pair + 1)
        if pair:
            acc_ref[...] += projected(pair - 1)
        kvq_finish(VALUE, pair)
        accum = nn(whole(VALUE, pair), probs.astype(BF16)) * inverse
        attn_pair = jnp.where(own_live, merged(accum), 0.0).astype(BF16)
        at_ref[slot, PAIR_ROWS * pair : PAIR_ROWS * (pair + 1), :] = attn_pair
        part = at_ref.at[slot, rows_of(pair)]
        arrival = at_recv.at[pair // (PAIRS - 1)]
        for to in (chip * 2 + chip % 2, chip * 2 + 1 - chip % 2):
            copy(part, part, at_send.at[0], arrival, (across, to)).start()
        copy(part, part, at_send.at[0], arrival, (dp, partner)).start()
        if pair == 1 and outer > 2:
            wave_wait()
            if outer > 3:
                wave_start()

    error = jnp.where(own_live, acc_ref[...] + projected(PAIRS - 1), 0.0)
    dout = (2.0 * error).astype(BF16)
    loss_part = jnp.sum(jnp.sum(error * error, axis=0, keepdims=True), axis=1, keepdims=True)
    tile_own[...] = jnp.broadcast_to(loss_part, tile_own.shape)
    small(1, tile_own, tile_all)
    tile_all[me] = tile_own[...]

    def terms(value):
        first = value.astype(BF16).astype(F32)
        second = (value - first).astype(BF16).astype(F32)
        return [first, second, value - first - second]

    for pair in range(PAIRS):
        grad = nn(w_ref[PAIR_ROWS * pair : PAIR_ROWS * (pair + 1), :], dout).astype(BF16)
        g_ref[me, pair, :PAIR_ROWS, :] = grad
        product = grad.astype(F32) * at_ref[slot, PAIR_ROWS * pair : PAIR_ROWS * (pair + 1), :].astype(F32)
        lines = []
        for side in (0, 1):
            lines += terms(stat_ref[2 * pair + side : 2 * pair + side + 1, :])
        for side in (0, 1):
            head = 2 * pair + side
            delta = jnp.sum(product[HEAD_DIM * side : HEAD_DIM * (side + 1)], axis=0, keepdims=True)
            stat_ref[HEADS + head : HEADS + head + 1, :] = delta
            lines += terms(delta)
        lines.append(jnp.zeros((STAT_ROWS - 12, rows), F32))
        g_ref[me, pair, PAIR_ROWS:, :] = jnp.concatenate(lines, axis=0).astype(BF16)
    g_spread(0)

    def query_pass(pair):
        low = HEADS + 2 * pair
        delta = jnp.concatenate([stat_ref[low : low + 1, :], stat_ref[low + 1 : low + 2, :]], axis=1)
        grad = g_ref[me, pair, :PAIR_ROWS, :]
        dprobs = tn(whole(VALUE, pair), stacked(grad))
        dscores = prob_ref[pair] * inverses[pair] * (dprobs - delta)
        value = nn(whole(KEY, pair), dscores.astype(BF16))
        dq_ref[PAIR_ROWS * pair : PAIR_ROWS * (pair + 1), :] = merged(value) * score_scale

    def key_pass(pair):
        if pair in (0, 3):
            g_finish(pair // 3)
        queries = whole(QUERY, pair)
        grads = jnp.concatenate([g_ref[j, pair] for j in range(members)], axis=1)
        stats = grads[PAIR_ROWS:]
        scores = tn(
            jnp.concatenate([queries, stats], axis=0),
            jnp.concatenate([stacked(own(KEY, pair)), norm_picker], axis=0),
        )
        probs = jnp.exp2(biased(scores))
        dv_ref[PAIR_ROWS * pair : PAIR_ROWS * (pair + 1), :] = merged(nn(grads[:PAIR_ROWS], probs.astype(BF16)))
        dprobs = tn(grads, jnp.concatenate([stacked(own(VALUE, pair)), delta_picker], axis=0))
        dscores = (probs * dprobs).astype(BF16)
        dk_ref[PAIR_ROWS * pair : PAIR_ROWS * (pair + 1), :] = merged(nn(queries, dscores)) * score_scale

    def attention(pair):
        low = PAIR_ROWS * pair
        return jnp.concatenate([at_ref[s, low : low + PAIR_ROWS, :] for s in range(4)], axis=1)

    def weight_start():
        received(tt_all.at[pl.ds(0, 3)], tt_recv.at[0])
        received(at_ref.at[pl.ds(0, 3), pl.ds(0, FEAT - PAIR_ROWS)], at_recv.at[0])
        for i in range(mine):
            block = (job * mine + i) * 2 + step_b
            value = -jnp.concatenate([tt_all[s, i].astype(F32) for s in range(4)], axis=1)
            for pair in range(PAIRS - 1):
                value = value + nn(wt_ref[pair, block], attention(pair))
            other_ref[i] = value

    def deliver(block, everyone, to, send, recv, owner):
        stays = jnp.logical_and(owner == step_a, core == to)

        @pl.when(stays)
        def _():
            everyone[step_a] = block[...]

        @pl.when(jnp.logical_not(stays))
        def _():
            copy(block, everyone.at[step_a], send, recv, (owner * 2 + step_b, chip * 2 + to)).start()

    def weight_blocks(away, blocks, grads, attn, span):
        if main:
            attn_main = jnp.concatenate([attn[p * features : p * features + main] for p in range(span)], axis=0)
            attn_rest = jnp.concatenate([attn[p * features + main : (p + 1) * features] for p in range(span)], axis=0)
            part_main = nt(grads, attn_main).astype(BF16)
        else:
            attn_rest = attn
        part_rest = nt(attn_rest, grads)
        for place, i in enumerate(blocks):
            for p in range(span):
                if main:
                    u_own[i, away + p, :share, :] = part_main[place * share : (place + 1) * share, p * main : (p + 1) * main]
                for t in range(tiles):
                    wide = min(share - t * LANES, LANES)
                    first = place * share + t * LANES
                    low = main_rows + t * rest_rows
                    piece = part_rest[p * rest : (p + 1) * rest, first : first + wide]
                    u_own[i, away + p, low : low + rest, :wide] = piece.astype(BF16)

    def weight_part():
        received(at_ref.at[pl.ds(0, 3), rows_of(PAIRS - 1)], at_recv.at[1])
        last = attention(PAIRS - 1)

        def grads_of(i):
            block = (job * mine + i) * 2 + step_b
            return (2.0 * (other_ref[i] + nn(wt_ref[PAIRS - 1, block], last))).astype(BF16)

        def send(i, shift):
            away = far(shift)
            for to in (0, 1):
                if detour and (i, to) == (0, 1):
                    deliver(u_own.at[i, away * 2 + to], zb_all, 0, turn_send.at[0], turn_recv.at[0], turn_owner)
                    continue
                copy(
                    u_own.at[i, away * 2 + to],
                    y_all.at[i, to, chip],
                    y_send.at[0],
                    y_recv.at[i, to],
                    (dp, away * 2 + (job + away) % 2),
                ).start()

        if share % 16 == 0 and features % 16 == 0:

            def attn_of(shift):
                low = pl.multiple_of(far(shift) * 2 * features, 16)
                return jnp.concatenate([at_ref[s, pl.ds(low, 2 * features), :] for s in range(4)], axis=1)

            grads = []
            for i in range(mine):
                grads.append(grads_of(i))
                for shift in range(1, chips):
                    weight_blocks(far(shift) * 2, [i], grads[i], attn_of(shift), 2)
                    send(i, shift)
            weight_blocks(chip * 2, range(mine), jnp.concatenate(grads, axis=0), attn_of(0), 2)
            if detour:
                deliver(u_own.at[0, chip * 2 + 1], z_all, 1, z_send.at[0], z_recv.at[0], turn_owner)
        else:
            attn = jnp.concatenate([at_ref[s] for s in range(4)], axis=1)
            for i in range(mine):
                weight_blocks(0, [i], grads_of(i), attn, members)
                for shift in range(1, chips):
                    send(i, shift)

    def weight_sum(i, to):
        if detour and (i, to) == (0, 1):
            return
        received(y_all.at[i, to, pl.ds(0, chips - 1)], y_recv.at[i, to])
        value = u_own[i, chip * 2 + to].astype(F32)
        for shift in range(1, chips):
            value = value + y_all[i, to, far(shift)].astype(F32)
        z_own[i, to] = value.astype(BF16)
        deliver(z_own.at[i, to], z_all, to, z_send.at[0], z_recv.at[0], job * mine + i)

    def turn():
        @pl.when(jnp.logical_and(ends_turn, core == 0))
        def _():
            @pl.when(job == step_a // mine)
            def _():
                received(zb_all.at[pl.ds(0, outer - 1)], turn_recv.at[0])

            @pl.when(job != step_a // mine)
            def _():
                received(zb_all, turn_recv.at[0])

            value = zb_all[0].astype(F32)
            for j in range(1, outer):
                value = value + zb_all[j].astype(F32)
            yb_own[...] = value.astype(BF16)
            copy(yb_own, yb_all, turn_send.at[1], turn_recv.at[1], (dp, far(1) * 2 + 1)).start()

    def turn_end():
        @pl.when(jnp.logical_not(jnp.logical_and(turn_owner == step_a, core == 0)))
        def _():
            sent(yb_own, turn_send.at[0])

        @pl.when(jnp.logical_and(ends_turn, core == 0))
        def _():
            sent(yb_own, turn_send.at[1])

        @pl.when(jnp.logical_and(ends_turn, core == 1))
        def _():
            received(yb_all, turn_recv.at[1])

    for hops in range(4, outer + 1):
        wave_wait()
        if hops < outer:
            wave_start()
    kvq_relay(QUERY)
    query_pass(0)
    weight_start()
    query_pass(1)
    received(tile_all.at[pl.ds(0, members - 1)], small_recv.at[1])
    pack_loss = tile_all[0]
    for j in range(1, members):
        pack_loss = pack_loss + tile_all[j]
    tile_lane = lax.broadcasted_iota(jnp.int32, pack_loss.shape, 1)
    pair_own[...] = jnp.where(tile_lane == 0, pack_loss, length.astype(F32))
    copy(pair_own, pair_all, small_send.at[3], small_recv.at[3], (across, me)).start()
    pl.when(job == 1)(functools.partial(g_spread, 1))
    weight_part()
    pl.when(job == 0)(functools.partial(g_spread, 1))
    query_pass(2)
    query_pass(3)
    g_relay(0)
    received(pair_all, small_recv.at[3])
    sum_own[...] = pair_own[...] + pair_all[...]
    for shift in range(1, outer):
        to = outer_peer(shift) * 2 + step_b
        copy(sum_own, sum_all.at[step_a], small_send.at[2], small_recv.at[2], (to, me)).start()
    sum_all[step_a] = sum_own[...]
    kvq_finish(QUERY)
    units = [(i, to) for i in range(mine) for to in (0, 1)]
    quarter = len(units) // 4
    parts = [units[quarter * k : quarter * (k + 1)] for k in range(4)]

    def weight_sums(early, late):
        for which, chosen in ((0, early), (1, late)):
            if chosen:

                @pl.when(job == which)
                def _():
                    for i, to in chosen:
                        weight_sum(i, to)

    weight_sums(parts[0] + parts[1], [])
    key_pass(0)
    weight_sums(parts[2], [])
    pl.when(job == 1)(functools.partial(g_relay, 1))
    key_pass(1)
    weight_sums(parts[3], parts[0])
    pl.when(job == 0)(functools.partial(g_relay, 1))
    if detour:
        turn()
    key_pass(2)
    weight_sums([], parts[1] + parts[2] + parts[3])
    key_pass(3)

    received(sum_all.at[pl.ds(0, outer - 1)], small_recv.at[2])
    totals = sum_all[0]
    for j in range(1, outer):
        totals = totals + sum_all[j]
    sum_ref[...] = totals

    sent(kvq_ref.at[:, pl.ds(0, members - 1)], kvq_send.at[0])
    sent(g_ref.at[pl.ds(0, members - 1)], g_send.at[0])
    sent(at_ref.at[pl.ds(0, 3)], at_send.at[0])
    sent(tt_all.at[pl.ds(0, 3)], tt_send.at[0])
    if detour:
        sent(z_all.at[pl.ds(0, 2 * mine - 1)], y_send.at[0])
        turn_end()
    else:
        sent(y_all.at[:, :, pl.ds(0, chips - 1)], y_send.at[0])
    sent(seg_all.at[pl.ds(0, members - 1)], small_send.at[0])
    sent(tile_all.at[pl.ds(0, members - 1)], small_send.at[1])
    sent(sum_all.at[pl.ds(0, outer - 1)], small_send.at[2])
    sent(pair_all, small_send.at[3])

    collects = job == step_a // mine

    @pl.when(collects)
    def _():
        sent(z_all.at[pl.ds(0, outer - 1)], z_send.at[0])
        received(z_all.at[pl.ds(0, outer - 1)], z_recv.at[0])

    @pl.when(jnp.logical_not(collects))
    def _():
        sent(z_all, z_send.at[0])
        received(z_all, z_recv.at[0])

    summed = z_all[0].astype(F32)
    for j in range(1, outer):
        summed = summed + z_all[j].astype(F32)
    if detour:
        summed = summed + jnp.where(jnp.logical_and(ends_turn, core == 1), yb_all[...].astype(F32), 0.0)
    if main:
        dw_ref[:main, :] = summed[:share].T
    for t in range(tiles):
        wide = min(share - t * LANES, LANES)
        low = main_rows + t * rest_rows
        dw_ref[main:, t * LANES : t * LANES + wide] = summed[low : low + rest, :wide]


def scale_kernel(slots, total, sum_ref, dq_ref, dk_ref, dv_ref, dw_ref, query_ref, key_ref, value_ref, weight_ref, loss_ref):
    count = sum_ref[0:1, 1:2]
    ratio = slots / count
    query_ref[...] = dq_ref[...] * ratio
    key_ref[...] = dk_ref[...] * ratio
    value_ref[...] = dv_ref[...] * ratio
    weight_ref[...] = dw_ref[...] * (ratio / total)
    loss_ref[...] = sum_ref[0:1, 0:1] / (count * WIDTH)


def solution(mesh):
    members, groups = mesh.shape["patch"], mesh.shape["dp"]

    def local(query_rows, key_rows, value_rows, out_weight, target, lengths, segments):
        rows = query_rows.shape[1]
        total = rows * members
        chips = members // 2
        outer = groups // 2
        mine = outer // 2
        share, features, main, rest, main_rows, tiles, unit_rows = unit_layout(members, groups)
        vmem = pl.BlockSpec(memory_space=pltpu.VMEM)
        hbm = pl.BlockSpec(memory_space=pltpu.HBM)
        dma = pltpu.SemaphoreType.DMA
        operands = (
            segments,
            query_rows[0].T,
            key_rows[0].T,
            value_rows[0].T,
            out_weight,
            target[0],
        )
        outs = pl.pallas_call(
            functools.partial(kernel, members, groups),
            out_shape=(
                jax.ShapeDtypeStruct((FEAT, rows), F32),
                jax.ShapeDtypeStruct((FEAT, rows), F32),
                jax.ShapeDtypeStruct((FEAT, rows), F32),
                jax.ShapeDtypeStruct((features, share), F32),
                jax.ShapeDtypeStruct((8, 128), F32),
            ),
            in_specs=[pl.BlockSpec(memory_space=pltpu.SMEM)] + [hbm] * 6,
            out_specs=(vmem,) * 5,
            scratch_shapes=[
                pltpu.VMEM((FEAT, WIDTH), BF16),
                pltpu.VMEM((rows, WIDTH), BF16),
                pltpu.VMEM((PAIRS, groups, share, PAIR_ROWS), BF16),
                pltpu.VMEM((WIDTH, rows), F32),
                pltpu.VMEM((3, members, FEAT, rows), BF16),
                pltpu.VMEM((members, PAIRS, AUG_ROWS, rows), BF16),
                pltpu.VMEM((1, rows), jnp.int32),
                pltpu.VMEM((members, 1, rows), jnp.int32),
                pltpu.VMEM((2 * HEADS, rows), F32),
                pltpu.VMEM((total, rows), F32),
                pltpu.VMEM((PAIRS, total, 2 * rows), F32),
                pltpu.VMEM((4, FEAT, rows), BF16),
                pltpu.VMEM((2, outer, share, rows), BF16),
                pltpu.VMEM((4, mine, share, rows), BF16),
                pltpu.VMEM((mine, share, 4 * rows), F32),
                pltpu.VMEM((mine, members, unit_rows, LANES), BF16),
                pltpu.VMEM((mine, 2, chips, unit_rows, LANES), BF16),
                pltpu.VMEM((mine, 2, unit_rows, LANES), BF16),
                pltpu.VMEM((outer, unit_rows, LANES), BF16),
                pltpu.VMEM((outer, unit_rows, LANES), BF16),
                pltpu.VMEM((unit_rows, LANES), BF16),
                pltpu.VMEM((unit_rows, LANES), BF16),
                pltpu.VMEM((8, 128), F32),
                pltpu.VMEM((members, 8, 128), F32),
                pltpu.VMEM((8, 128), F32),
                pltpu.VMEM((8, 128), F32),
                pltpu.VMEM((8, 128), F32),
                pltpu.VMEM((outer, 8, 128), F32),
                dma((6,)),
                dma((2 * PAIRS + 1,)),
                dma((2 * PAIRS + 1,)),
                dma((1,)),
                dma((PAIRS // 2,)),
                dma((PAIRS // 2,)),
                dma((1,)),
                dma((1,)),
                dma((2,)),
                dma((1,)),
                dma((1,)),
                dma((1,)),
                dma((mine, 2)),
                dma((1,)),
                dma((1,)),
                dma((4,)),
                dma((4,)),
                pltpu.SemaphoreType.REGULAR((2,)),
                dma((2,)),
                dma((2,)),
            ],
            compiler_params=pltpu.CompilerParams(collective_id=0, has_side_effects=True, vmem_limit_bytes=48000000),
            name="sublayer",
        )(lengths, *[pltpu.with_memory_space_constraint(operand, pltpu.HBM) for operand in operands])
        final = pl.pallas_call(
            functools.partial(scale_kernel, groups * total, total),
            out_shape=(
                jax.ShapeDtypeStruct((FEAT, rows), F32),
                jax.ShapeDtypeStruct((FEAT, rows), F32),
                jax.ShapeDtypeStruct((FEAT, rows), F32),
                jax.ShapeDtypeStruct((features, share), F32),
                jax.ShapeDtypeStruct((1, 1), F32),
            ),
            in_specs=[vmem] * 5,
            out_specs=(vmem,) * 5,
            compiler_params=pltpu.CompilerParams(vmem_limit_bytes=8000000),
            name="scale",
        )(outs[4], *outs[:4])
        return (final[0].T[None], final[1].T[None], final[2].T[None], final[3], final[4].reshape(()))

    placed = (
        P("dp", "patch", None),
        P("dp", "patch", None),
        P("dp", "patch", None),
        P(),
        P("dp", "patch", None),
        P("dp"),
        P("dp", "patch"),
    )
    return jax.shard_map(
        local,
        mesh=mesh,
        in_specs=placed,
        out_specs=(
            P("dp", "patch", None),
            P("dp", "patch", None),
            P("dp", "patch", None),
            P("patch", "dp"),
            P(),
        ),
        check_vma=False,
    )
```
